8 devices in a mesh: data: 2 (over z, y), stage: 4 (over x, core).
Axes of the slice: x: 2, y: 2, z: 1, core: 2. Of those that a mesh axis runs over, the one named last changes fastest.
Arguments:
- w_in: float32 [4, 512, 2048], P('stage')
- w_out: float32 [4, 2048, 512], P('stage')
- mom_in: float32 [4, 512, 2048], P('stage')
- mom_out: float32 [4, 2048, 512], P('stage')
- var_in: float32 [4, 512, 2048], P('stage')
- var_out: float32 [4, 2048, 512], P('stage')
- acc_in: float32 [2, 4, 512, 2048], P('data', 'stage')
- acc_out: float32 [2, 4, 2048, 512], P('data', 'stage')
- stage_acts: bfloat16 [4, 4096, 512], P('stage', 'data')
- d_out: bfloat16 [4096, 512], P('data')
- next_x: bfloat16 [16, 4096, 512], P(None, 'data')
- learn_rate: float32 [1], replicated
- max_norm: float32 [1], replicated
Outputs:
- output 1: float32 [4, 512, 2048], P('stage')
- output 2: float32 [4, 2048, 512], P('stage')
- output 3: float32 [4, 512, 2048], P('stage')
- output 4: float32 [4, 2048, 512], P('stage')
- output 5: float32 [4, 512, 2048], P('stage')
- output 6: float32 [4, 2048, 512], P('stage')
- output 7: bfloat16 [16, 4096, 512], P(None, 'data')
All inputs are finite; a program needn't handle non-finite values.
Results may differ from the reference program's by a relative error of at most 0.0070407.
Values are sent between devices in bfloat16 or wider.
A program may use at most 1 GiB of HBM per device.

```python
import jax
import jax.numpy as jnp
from jax import lax

STAGES = 4
REPLICAS = 2
MODEL_DIM = 512
FFN_DIM = 2048
MICRO_TOKENS = 2048
NEXT_MICRO = 16
STEP_COUNT = 10

BETA_ONE = 0.9
BETA_TWO = 0.95
ADAM_EPS = 1e-8
WEIGHT_DECAY = 0.1
NORM_EPS = 1e-6
TOTAL_ROWS = REPLICAS * MICRO_TOKENS


def gelu_tanh(gelu_in):
    return jax.nn.gelu(gelu_in, approximate=True)


def block_forward(row_block, w_first, w_second):
    hidden = jnp.dot(row_block, w_first, preferred_element_type=jnp.float32)
    act_h = gelu_tanh(hidden).astype(jnp.bfloat16)
    branch = jnp.dot(act_h, w_second, preferred_element_type=jnp.float32)
    return (row_block.astype(jnp.float32) + branch).astype(jnp.bfloat16)


def block_backward(grad_val, w_first, w_second, stage_in):
    pre_act = jnp.dot(stage_in, w_first, preferred_element_type=jnp.float32)
    act_h, gelu_vjp = jax.vjp(gelu_tanh, pre_act)
    act_h = act_h.astype(jnp.bfloat16)
    dw_second = jnp.dot(act_h.T, grad_val, preferred_element_type=jnp.float32)
    d_hid = jnp.dot(grad_val, w_second.T, preferred_element_type=jnp.float32)
    d_pre = gelu_vjp(d_hid)[0].astype(jnp.bfloat16)
    dw_first = jnp.dot(stage_in.T, d_pre, preferred_element_type=jnp.float32)
    d_in = grad_val.astype(jnp.float32) + jnp.dot(d_pre, w_first.T, preferred_element_type=jnp.float32)
    return d_in.astype(jnp.bfloat16), dw_first, dw_second


def micro_grads(w_in, w_out, stage_acts, d_out):
    w_first = w_in.astype(jnp.bfloat16)
    w_second = w_out.astype(jnp.bfloat16)
    acts_rep = jnp.transpose(stage_acts.reshape(STAGES, REPLICAS, MICRO_TOKENS, MODEL_DIM), (1, 0, 2, 3))
    grad_rep = d_out.reshape(REPLICAS, MICRO_TOKENS, MODEL_DIM)

    def one_replica(operands):
        acts_one, grad_top = operands

        def layer_step(grad_val, layer_ws):
            d_in, dw_first, dw_second = block_backward(grad_val, layer_ws[0], layer_ws[1], layer_ws[2])
            return d_in, (dw_first, dw_second)

        _, grad_pair = lax.scan(layer_step, grad_top, (w_first, w_second, acts_one), reverse=True)
        return grad_pair

    return lax.map(one_replica, (acts_rep, grad_rep))


def summed_grads(acc_in, acc_out, micro_first, micro_second):
    grad_first = jnp.sum(acc_in + micro_first, axis=0) / REPLICAS
    grad_second = jnp.sum(acc_out + micro_second, axis=0) / REPLICAS
    total_norm = jnp.sqrt(jnp.sum(grad_first * grad_first) + jnp.sum(grad_second * grad_second))
    return grad_first, grad_second, total_norm


def adamw_update(param_old, moment, second, grad_val, clip_coef, lr_value):
    scaled = clip_coef * grad_val
    mom_new = BETA_ONE * moment + (1.0 - BETA_ONE) * scaled
    sec_new = BETA_TWO * second + (1.0 - BETA_TWO) * scaled * scaled
    mom_hat = mom_new / (1.0 - BETA_ONE ** STEP_COUNT)
    sec_hat = sec_new / (1.0 - BETA_TWO ** STEP_COUNT)
    param_new = param_old - lr_value * (mom_hat / (jnp.sqrt(sec_hat) + ADAM_EPS) + WEIGHT_DECAY * param_old)
    return param_new, mom_new, sec_new


def forward_all(w_first, w_second, next_x):
    blocks = next_x.reshape(NEXT_MICRO * REPLICAS, MICRO_TOKENS, MODEL_DIM)

    def one_block(row_block):
        def layer_step(carry_rows, layer_ws):
            return block_forward(carry_rows, layer_ws[0], layer_ws[1]), None

        out_rows, _ = lax.scan(layer_step, row_block, (w_first, w_second))
        return out_rows

    return lax.map(one_block, blocks).reshape(NEXT_MICRO, TOTAL_ROWS, MODEL_DIM)


def setup_inputs(seed: int = 0) -> dict:
    key_list = jax.random.split(jax.random.key(seed), 14)
    w_in = jax.random.normal(key_list[0], (STAGES, MODEL_DIM, FFN_DIM), jnp.float32) * MODEL_DIM ** -0.5
    w_out = jax.random.normal(key_list[1], (STAGES, FFN_DIM, MODEL_DIM), jnp.float32) * (FFN_DIM * STAGES) ** -0.5
    stage_acts = jax.random.normal(key_list[2], (STAGES, TOTAL_ROWS, MODEL_DIM), jnp.float32).astype(jnp.bfloat16)
    d_out = jax.random.normal(key_list[3], (TOTAL_ROWS, MODEL_DIM), jnp.float32).astype(jnp.bfloat16)
    next_x = jax.random.normal(key_list[4], (NEXT_MICRO, TOTAL_ROWS, MODEL_DIM), jnp.float32).astype(jnp.bfloat16)
    micro_first, micro_second = micro_grads(w_in, w_out, stage_acts, d_out)
    rms_first = jnp.sqrt(jnp.mean(micro_first * micro_first, axis=(0, 2, 3)))[None, :, None, None]
    rms_second = jnp.sqrt(jnp.mean(micro_second * micro_second, axis=(0, 2, 3)))[None, :, None, None]
    acc_in = jax.random.normal(key_list[5], micro_first.shape, jnp.float32) * rms_first
    acc_out = jax.random.normal(key_list[6], micro_second.shape, jnp.float32) * rms_second
    grad_first, grad_second, total_norm = summed_grads(acc_in, acc_out, micro_first, micro_second)
    max_norm = total_norm * jax.random.uniform(key_list[7], (1,), jnp.float32, 0.35, 0.65)
    clip_coef = max_norm[0] / (total_norm + NORM_EPS)
    q_first = jnp.sqrt(jnp.mean((clip_coef * grad_first) ** 2, axis=(1, 2)))[:, None, None]
    q_second = jnp.sqrt(jnp.mean((clip_coef * grad_second) ** 2, axis=(1, 2)))[:, None, None]
    mom_in = jax.random.normal(key_list[8], w_in.shape, jnp.float32) * 0.1 * q_first
    mom_out = jax.random.normal(key_list[9], w_out.shape, jnp.float32) * 0.1 * q_second
    var_in = jax.random.uniform(key_list[10], w_in.shape, jnp.float32, 0.5, 1.5) * 0.05 * q_first ** 2
    var_out = jax.random.uniform(key_list[11], w_out.shape, jnp.float32, 0.5, 1.5) * 0.05 * q_second ** 2
    learn_rate = jax.random.uniform(key_list[12], (1,), jnp.float32, 0.6, 1.4) * 0.25 * MODEL_DIM ** -0.5
    return {'w_in': w_in, 'w_out': w_out, 'mom_in': mom_in, 'mom_out': mom_out, 'var_in': var_in, 'var_out': var_out, 'acc_in': acc_in, 'acc_out': acc_out, 'stage_acts': stage_acts, 'd_out': d_out, 'next_x': next_x, 'learn_rate': learn_rate, 'max_norm': max_norm}


def reference(w_in, w_out, mom_in, mom_out, var_in, var_out, acc_in, acc_out, stage_acts, d_out, next_x, learn_rate, max_norm):
    micro_first, micro_second = micro_grads(w_in, w_out, stage_acts, d_out)
    grad_first, grad_second, total_norm = summed_grads(acc_in, acc_out, micro_first, micro_second)
    clip_coef = jnp.minimum(1.0, max_norm[0] / (total_norm + NORM_EPS))
    new_first, mom_first, sec_first = adamw_update(w_in, mom_in, var_in, grad_first, clip_coef, learn_rate[0])
    new_second, mom_second, sec_second = adamw_update(w_out, mom_out, var_out, grad_second, clip_coef, learn_rate[0])
    next_y = forward_all(new_first.astype(jnp.bfloat16), new_second.astype(jnp.bfloat16), next_x)
    return (new_first, new_second, mom_first, mom_second, sec_first, sec_second, next_y)
```

```python
import functools

import jax
import jax.numpy as jnp
from jax import lax
from jax.experimental import pallas as pl
from jax.experimental.pallas import tpu as pltpu
from jax.sharding import PartitionSpec as P

BETA_ONE = 0.9
BETA_TWO = 0.95
ADAM_EPS = 1e-8
WEIGHT_DECAY = 0.1
STEP_COUNT = 10
NORM_EPS = 1e-6
TRANS_DIMS = (((1,), (1,)), ((), ()))
FIRST_DIMS = (((0,), (0,)), ((), ()))
TILE = 512
CHUNK = 512
SLOTS = 8
LAG = 6


def gelu_tanh(gelu_in):
    return jax.nn.gelu(gelu_in, approximate=True)


def fast_gelu(z):
    inner = z * (0.7978845608028654 + 0.035677408136300125 * (z * z))
    half = 0.5 * z
    return half + half * jnp.tanh(inner)


def adamw_update(param_old, moment, second, grad_val, clip_coef, lr_value):
    scaled = clip_coef * grad_val
    mom_new = BETA_ONE * moment + (1.0 - BETA_ONE) * scaled
    sec_new = BETA_TWO * second + (1.0 - BETA_TWO) * scaled * scaled
    mom_hat = mom_new / (1.0 - BETA_ONE ** STEP_COUNT)
    sec_hat = sec_new / (1.0 - BETA_TWO ** STEP_COUNT)
    param_new = param_old - lr_value * (mom_hat / (jnp.sqrt(sec_hat) + ADAM_EPS) + WEIGHT_DECAY * param_old)
    return param_new, mom_new, sec_new


def forward_kernel(n_tiles, x_ref, w1_ref, w2_ref, y_ref, xv, yv, w1v, w2v, xsem, wsem, osem, psend, nsend, fsend, precv, nrecv, frecv):
    stage = lax.axis_index('stage')
    partner = stage + 1 - 2 * (stage % 2)
    across = (stage + 2) % 4
    n_blocks = w1v.shape[0]
    width = w1v.shape[2]

    def rows(owner, tile):
        return pl.ds(pl.multiple_of((owner * n_tiles + tile) * TILE, TILE), TILE)

    def load_x(tile):
        return pltpu.make_async_copy(x_ref.at[rows(stage, tile)], xv.at[tile % 2], xsem.at[tile % 2])

    def load_w(block):
        return (pltpu.make_async_copy(w1_ref.at[block], w1v.at[block], wsem.at[block, 0]),
                pltpu.make_async_copy(w2_ref.at[block], w2v.at[block], wsem.at[block, 1]))

    def store_own(tile):
        return pltpu.make_async_copy(yv.at[tile % SLOTS], y_ref.at[rows(stage, tile)], osem.at[tile % SLOTS])

    def remote(src, owner, tile, send, recv, target):
        return pltpu.make_async_remote_copy(src_ref=src, dst_ref=y_ref.at[rows(owner, tile)], send_sem=send, recv_sem=recv,
                                            device_id={'stage': target}, device_id_type=pl.DeviceIdType.MESH)

    def to_partner(tile):
        return remote(yv.at[tile % SLOTS], stage, tile, psend.at[tile % SLOTS], precv.at[tile], partner)

    def to_across(tile):
        return remote(yv.at[tile % SLOTS], stage, tile, nsend.at[tile % SLOTS], nrecv.at[tile], across)

    def pass_on(tile):
        return remote(y_ref.at[rows(across, tile)], across, tile, fsend.at[tile], frecv.at[tile], partner)

    load_x(0).start()
    for block in range(n_blocks):
        for copy in load_w(block):
            copy.start()
    barrier = pltpu.get_barrier_semaphore()
    for peer in (partner, across):
        pl.semaphore_signal(barrier, inc=1, device_id={'stage': peer}, device_id_type=pl.DeviceIdType.MESH)
    pl.semaphore_wait(barrier, 2)

    def relay(tile):
        remote(y_ref.at[rows(across, tile)], across, tile, nsend.at[0], nrecv.at[tile], across).wait_recv()
        pass_on(tile).start()

    def free_slot(tile):
        store_own(tile).wait()
        to_partner(tile).wait_send()
        to_across(tile).wait_send()

    @pl.loop(0, n_tiles)
    def _(tile):
        load_x(tile).wait()

        @pl.when(tile + 1 < n_tiles)
        def _():
            load_x(tile + 1).start()

        @pl.when(tile >= SLOTS)
        def _():
            free_slot(tile - SLOTS)

        @pl.loop(0, n_blocks)
        def _(block):
            @pl.when(tile == 0)
            def _():
                for copy in load_w(block):
                    copy.wait()

            x_rows = xv[tile % 2]
            total = x_rows.astype(jnp.float32)
            for first in range(0, width, CHUNK):
                hidden = jnp.dot(x_rows, w1v[block, :, first:first + CHUNK], preferred_element_type=jnp.float32)
                act_h = fast_gelu(hidden).astype(jnp.bfloat16)
                part = jnp.dot(act_h, w2v[block, first:first + CHUNK, :], preferred_element_type=jnp.float32)
                total = part if first == 0 else total + part
            total = x_rows.astype(jnp.float32) + total
            xv[tile % 2] = total.astype(jnp.bfloat16)

            @pl.when(block == n_blocks - 1)
            def _():
                yv[tile % SLOTS] = total.astype(jnp.bfloat16)

        store_own(tile).start()
        to_across(tile).start()
        to_partner(tile).start()

        @pl.when(tile >= LAG)
        def _():
            relay(tile - LAG)

    for tile in range(n_tiles - LAG, n_tiles):
        relay(tile)
    for tile in range(n_tiles - SLOTS, n_tiles):
        free_slot(tile)

    @pl.loop(0, n_tiles)
    def _(tile):
        remote(y_ref.at[rows(partner, tile)], partner, tile, psend.at[0], precv.at[tile], partner).wait_recv()
        other = (partner + 2) % 4
        remote(y_ref.at[rows(other, tile)], other, tile, fsend.at[0], frecv.at[tile], partner).wait_recv()
        pass_on(tile).wait_send()


def forward_all(x_rows, w_first, w_second, n_stage):
    n_rows, dim = x_rows.shape
    n_blocks, _, width = w_first.shape
    n_tiles = n_rows // (n_stage * TILE)
    dma = pltpu.SemaphoreType.DMA
    flops = 4 * n_tiles * TILE * dim * width * n_blocks
    return pl.pallas_call(
        functools.partial(forward_kernel, n_tiles),
        out_shape=jax.ShapeDtypeStruct((n_rows, dim), jnp.bfloat16),
        in_specs=[pl.BlockSpec(memory_space=pl.ANY)] * 3,
        out_specs=pl.BlockSpec(memory_space=pl.ANY),
        scratch_shapes=[
            pltpu.VMEM((2, TILE, dim), jnp.bfloat16),
            pltpu.VMEM((SLOTS, TILE, dim), jnp.bfloat16),
            pltpu.VMEM((n_blocks, dim, width), jnp.bfloat16),
            pltpu.VMEM((n_blocks, width, dim), jnp.bfloat16),
            dma((2,)), dma((n_blocks, 2)), dma((SLOTS,)), dma((SLOTS,)), dma((SLOTS,)),
            dma((n_tiles,)), dma((n_tiles,)), dma((n_tiles,)), dma((n_tiles,)),
        ],
        compiler_params=pltpu.CompilerParams(collective_id=0, has_side_effects=True, vmem_limit_bytes=48 * 2 ** 20),
        cost_estimate=pl.CostEstimate(flops=flops, bytes_accessed=2 * n_rows * dim * 2, transcendentals=0),
        name='forward_all',
    )(x_rows, w_first, w_second)


def solution(mesh):
    n_stage = mesh.shape['stage']
    n_rep = mesh.shape['data']
    last_stage = n_stage - 1
    back_perm = [(src, src - 1) for src in range(1, n_stage)]
    swap = [(0, 1), (1, 0)]
    w_spec = P('stage', None, None)
    acc_spec = P('data', 'stage', None, None)
    row_spec = P(None, 'data', None)

    def stage_program(w_in, w_out, mom_in, mom_out, var_in, var_out, acc_in, acc_out, stage_acts, d_out, next_x, learn_rate, max_norm):
        stage_idx = lax.axis_index('stage')
        rep_idx = lax.axis_index('data')
        w_first = w_in[0].astype(jnp.bfloat16)
        w_second = w_out[0].astype(jnp.bfloat16)
        stage_in = stage_acts[0]
        pre_act = jnp.dot(stage_in, w_first, preferred_element_type=jnp.float32)
        act_h, gelu_vjp = jax.vjp(gelu_tanh, pre_act)
        act_h = act_h.astype(jnp.bfloat16)

        def run_active(operands):
            grad_val = operands[0]
            d_hid = lax.dot_general(grad_val, w_second, TRANS_DIMS, preferred_element_type=jnp.float32)
            d_pre = gelu_vjp(d_hid)[0].astype(jnp.bfloat16)
            d_in = grad_val.astype(jnp.float32) + lax.dot_general(d_pre, w_first, TRANS_DIMS, preferred_element_type=jnp.float32)
            return d_in.astype(jnp.bfloat16), grad_val, d_pre

        def back_step(step_idx, loop_carry):
            return lax.cond(stage_idx == last_stage - step_idx, run_active, lambda operands: operands, loop_carry)

        def back_body(step_idx, loop_carry):
            sent_buf, grad_keep, pre_keep = back_step(step_idx, loop_carry)
            return lax.ppermute(sent_buf, 'stage', back_perm), grad_keep, pre_keep

        init_carry = (d_out, jnp.zeros_like(d_out), jnp.zeros((stage_in.shape[0], w_first.shape[1]), jnp.bfloat16))
        back_carry = lax.fori_loop(0, last_stage, back_body, init_carry)
        _, grad_keep, pre_keep = back_step(last_stage, back_carry)
        dw_first = lax.dot_general(stage_in, pre_keep, FIRST_DIMS, preferred_element_type=jnp.float32)
        dw_second = lax.dot_general(act_h, grad_keep, FIRST_DIMS, preferred_element_type=jnp.float32)
        loc_first = acc_in[0, 0] + dw_first
        loc_second = acc_out[0, 0] + dw_second

        def half_of(arr, idx):
            size = arr.shape[0] // n_rep
            return lax.dynamic_slice_in_dim(arr, idx * size, size, 0)

        other_idx = 1 - rep_idx
        half_first = (half_of(loc_first, rep_idx) + lax.ppermute(half_of(loc_first, other_idx), 'data', swap)) / n_rep
        half_second = (half_of(loc_second, rep_idx) + lax.ppermute(half_of(loc_second, other_idx), 'data', swap)) / n_rep
        far_first = lax.ppermute(half_first, 'data', swap)
        far_second = lax.ppermute(half_second, 'data', swap)
        part_sq = jnp.sum(half_first * half_first) + jnp.sum(half_second * half_second)
        total_norm = jnp.sqrt(lax.psum(part_sq, ('data', 'stage')))
        clip_coef = jnp.minimum(1.0, max_norm[0] / (total_norm + NORM_EPS))

        def early(param, moment, second, grad_val):
            new_w, _, _ = adamw_update(half_of(param, rep_idx), half_of(moment, rep_idx), half_of(second, rep_idx), grad_val, clip_coef, learn_rate[0])
            gathered = lax.all_gather(new_w.astype(jnp.bfloat16), ('stage', 'data'), axis=0, tiled=True)
            return gathered.reshape((n_stage,) + param.shape)

        fw_first = early(w_in[0], mom_in[0], var_in[0], half_first)
        fw_second = early(w_out[0], mom_out[0], var_out[0], half_second)
        n_micro, n_rows, dim = next_x.shape
        next_y = forward_all(next_x.reshape(n_micro * n_rows, dim), fw_first, fw_second, n_stage).reshape(next_x.shape)

        def whole(near, far):
            is_low = rep_idx == 0
            return jnp.concatenate([jnp.where(is_low, near, far), jnp.where(is_low, far, near)], axis=0)

        new_first, mom_first, sec_first = adamw_update(w_in[0], mom_in[0], var_in[0], whole(half_first, far_first), clip_coef, learn_rate[0])
        new_second, mom_second, sec_second = adamw_update(w_out[0], mom_out[0], var_out[0], whole(half_second, far_second), clip_coef, learn_rate[0])
        return (new_first[None], new_second[None], mom_first[None], mom_second[None], sec_first[None], sec_second[None], next_y)

    return jax.shard_map(stage_program, mesh=mesh, in_specs=(w_spec, w_spec, w_spec, w_spec, w_spec, w_spec, acc_spec, acc_spec, P('stage', 'data', None), P('data', None), row_spec, P(None), P(None)), out_specs=(w_spec, w_spec, w_spec, w_spec, w_spec, w_spec, row_spec), check_vma=False)
```

```python
import functools

import jax
import jax.numpy as jnp
from jax import lax
from jax.experimental import pallas as pl
from jax.experimental.pallas import tpu as pltpu
from jax.sharding import PartitionSpec as P

BETA_ONE = 0.9
BETA_TWO = 0.95
ADAM_EPS = 1e-8
WEIGHT_DECAY = 0.1
STEP_COUNT = 10
NORM_EPS = 1e-6
TRANS_DIMS = (((1,), (1,)), ((), ()))
FIRST_DIMS = (((0,), (0,)), ((), ()))
TILE = 512
CHUNK = 512
SLOTS = 8
LAG = 6
ROWS = 256
PART = 512


def fast_gelu(z):
    inner = z * (0.7978845608028654 + 0.035677408136300125 * (z * z))
    half = 0.5 * z
    return half + half * jnp.tanh(inner)


def adamw_update(param_old, moment, second, grad_val, clip_coef, lr_value):
    scaled = clip_coef * grad_val
    mom_new = BETA_ONE * moment + (1.0 - BETA_ONE) * scaled
    sec_new = BETA_TWO * second + (1.0 - BETA_TWO) * scaled * scaled
    mom_hat = mom_new / (1.0 - BETA_ONE ** STEP_COUNT)
    sec_hat = sec_new / (1.0 - BETA_TWO ** STEP_COUNT)
    param_new = param_old - lr_value * (mom_hat / (jnp.sqrt(sec_hat) + ADAM_EPS) + WEIGHT_DECAY * param_old)
    return param_new, mom_new, sec_new


def forward_kernel(n_tiles, x_ref, w1_ref, w2_ref, y_ref, xv, yv, w1v, w2v, xsem, wsem, osem, psend, nsend, fsend, precv, nrecv, frecv):
    stage = lax.axis_index('stage')
    partner = stage + 1 - 2 * (stage % 2)
    across = (stage + 2) % 4
    n_blocks = w1v.shape[0]
    width = w1v.shape[2]

    def rows(owner, tile):
        return pl.ds(pl.multiple_of((owner * n_tiles + tile) * TILE, TILE), TILE)

    def load_x(tile):
        return pltpu.make_async_copy(x_ref.at[rows(stage, tile)], xv.at[tile % 2], xsem.at[tile % 2])

    def load_w(block):
        return (pltpu.make_async_copy(w1_ref.at[block], w1v.at[block], wsem.at[block, 0]),
                pltpu.make_async_copy(w2_ref.at[block], w2v.at[block], wsem.at[block, 1]))

    def store_own(tile):
        return pltpu.make_async_copy(yv.at[tile % SLOTS], y_ref.at[rows(stage, tile)], osem.at[tile % SLOTS])

    def remote(src, owner, tile, send, recv, target):
        return pltpu.make_async_remote_copy(src_ref=src, dst_ref=y_ref.at[rows(owner, tile)], send_sem=send, recv_sem=recv,
                                            device_id={'stage': target}, device_id_type=pl.DeviceIdType.MESH)

    def to_partner(tile):
        return remote(yv.at[tile % SLOTS], stage, tile, psend.at[tile % SLOTS], precv.at[tile], partner)

    def to_across(tile):
        return remote(yv.at[tile % SLOTS], stage, tile, nsend.at[tile % SLOTS], nrecv.at[tile], across)

    def pass_on(tile):
        return remote(y_ref.at[rows(across, tile)], across, tile, fsend.at[tile], frecv.at[tile], partner)

    load_x(0).start()
    for block in range(n_blocks):
        for copy in load_w(block):
            copy.start()
    barrier = pltpu.get_barrier_semaphore()
    for peer in (partner, across):
        pl.semaphore_signal(barrier, inc=1, device_id={'stage': peer}, device_id_type=pl.DeviceIdType.MESH)
    pl.semaphore_wait(barrier, 2)

    def relay(tile):
        remote(y_ref.at[rows(across, tile)], across, tile, nsend.at[0], nrecv.at[tile], across).wait_recv()
        pass_on(tile).start()

    def free_slot(tile):
        store_own(tile).wait()
        to_partner(tile).wait_send()
        to_across(tile).wait_send()

    @pl.loop(0, n_tiles)
    def _(tile):
        load_x(tile).wait()

        @pl.when(tile + 1 < n_tiles)
        def _():
            load_x(tile + 1).start()

        @pl.when(tile >= SLOTS)
        def _():
            free_slot(tile - SLOTS)

        @pl.loop(0, n_blocks)
        def _(block):
            @pl.when(tile == 0)
            def _():
                for copy in load_w(block):
                    copy.wait()

            x_rows = xv[tile % 2]
            total = x_rows.astype(jnp.float32)
            for first in range(0, width, CHUNK):
                hidden = jnp.dot(x_rows, w1v[block, :, first:first + CHUNK], preferred_element_type=jnp.float32)
                act_h = fast_gelu(hidden).astype(jnp.bfloat16)
                part = jnp.dot(act_h, w2v[block, first:first + CHUNK, :], preferred_element_type=jnp.float32)
                total = part if first == 0 else total + part
            total = x_rows.astype(jnp.float32) + total
            xv[tile % 2] = total.astype(jnp.bfloat16)

            @pl.when(block == n_blocks - 1)
            def _():
                yv[tile % SLOTS] = total.astype(jnp.bfloat16)

        store_own(tile).start()
        to_across(tile).start()
        to_partner(tile).start()

        @pl.when(tile >= LAG)
        def _():
            relay(tile - LAG)

    for tile in range(n_tiles - LAG, n_tiles):
        relay(tile)
    for tile in range(n_tiles - SLOTS, n_tiles):
        free_slot(tile)

    @pl.loop(0, n_tiles)
    def _(tile):
        remote(y_ref.at[rows(partner, tile)], partner, tile, psend.at[0], precv.at[tile], partner).wait_recv()
        other = (partner + 2) % 4
        remote(y_ref.at[rows(other, tile)], other, tile, fsend.at[0], frecv.at[tile], partner).wait_recv()
        pass_on(tile).wait_send()


def forward_all(x_rows, w_first, w_second, n_stage):
    n_rows, dim = x_rows.shape
    n_blocks, _, width = w_first.shape
    n_tiles = n_rows // (n_stage * TILE)
    dma = pltpu.SemaphoreType.DMA
    flops = 4 * n_tiles * TILE * dim * width * n_blocks
    return pl.pallas_call(
        functools.partial(forward_kernel, n_tiles),
        out_shape=jax.ShapeDtypeStruct((n_rows, dim), jnp.bfloat16),
        in_specs=[pl.BlockSpec(memory_space=pl.ANY)] * 3,
        out_specs=pl.BlockSpec(memory_space=pl.ANY),
        scratch_shapes=[
            pltpu.VMEM((2, TILE, dim), jnp.bfloat16),
            pltpu.VMEM((SLOTS, TILE, dim), jnp.bfloat16),
            pltpu.VMEM((n_blocks, dim, width), jnp.bfloat16),
            pltpu.VMEM((n_blocks, width, dim), jnp.bfloat16),
            dma((2,)), dma((n_blocks, 2)), dma((SLOTS,)), dma((SLOTS,)), dma((SLOTS,)),
            dma((n_tiles,)), dma((n_tiles,)), dma((n_tiles,)), dma((n_tiles,)),
        ],
        compiler_params=pltpu.CompilerParams(collective_id=0, has_side_effects=True, vmem_limit_bytes=48 * 2 ** 20),
        cost_estimate=pl.CostEstimate(flops=flops, bytes_accessed=2 * n_rows * dim * 2, transcendentals=0),
        name='forward_all',
    )(x_rows, w_first, w_second)


def backward_kernel(act_ref, dout_ref, w1_ref, w2_ref, acc1_ref, acc2_ref, g1_ref, g2_ref, sq_ref,
                    actv, grad, w1v, w2v, hid, slope, dpre, sent, accv, inbox,
                    lsem, asem, csend, crecv, rsend, rrecv):
    stage = lax.axis_index('stage')
    rep = lax.axis_index('data')
    far = 1 - rep
    n_rows, dim = actv.shape
    width = w1v.shape[1]
    n_chunks = n_rows // ROWS
    last = 3
    half1 = dim // 2
    half2 = width // 2
    n_parts = inbox.shape[0]
    n_cols = width // PART

    def chunk(idx):
        return pl.ds(pl.multiple_of(idx * ROWS, ROWS), ROWS)

    def peer(**where):
        return dict(device_id=where, device_id_type=pl.DeviceIdType.MESH)

    loads = [pltpu.make_async_copy(act_ref, actv, lsem.at[0]), pltpu.make_async_copy(w1_ref, w1v, lsem.at[1]), pltpu.make_async_copy(w2_ref, w2v, lsem.at[2])]
    for copy in loads:
        copy.start()
    top = pltpu.make_async_copy(dout_ref, grad, lsem.at[3])

    @pl.when(stage == last)
    def _():
        top.start()

    def load_acc(idx, side, step):
        slot = step % accv.shape[0]
        if idx < n_cols:
            src = acc1_ref.at[pl.ds(pl.multiple_of(side * half1, half1), half1), pl.ds(idx * PART, PART)]
        else:
            src = acc2_ref.at[pl.ds(pl.multiple_of(side * half2 + (idx - n_cols) * half1, half1), half1), :]
        return pltpu.make_async_copy(src, accv.at[slot], asem.at[slot])

    steps = [(idx, far) for idx in range(n_parts)] + [(idx, rep) for idx in range(n_parts)]
    ahead = accv.shape[0]
    for step in range(ahead):
        load_acc(*steps[step], step).start()

    barrier = pltpu.get_barrier_semaphore()
    pl.semaphore_signal(barrier, inc=1, **peer(stage=(stage + 1) % 4))
    pl.semaphore_signal(barrier, inc=1, **peer(stage=(stage + 3) % 4))
    pl.semaphore_signal(barrier, inc=1, **peer(data=far))
    pl.semaphore_wait(barrier, 3)

    def hop(idx):
        return pltpu.make_async_remote_copy(src_ref=sent.at[chunk(idx)], dst_ref=grad.at[chunk(idx)], send_sem=csend.at[idx], recv_sem=crecv.at[idx],
                                            **peer(stage=(stage + 3) % 4))

    def prepare(idx):
        act = actv[chunk(idx), :]
        for first in range(0, width, CHUNK):
            cols = slice(first, first + CHUNK)
            z = jnp.dot(act, w1v[:, cols], preferred_element_type=jnp.float32)
            sq = z * z
            th = jnp.tanh(z * (0.7978845608028654 + 0.035677408136300125 * sq))
            gate = 0.5 + 0.5 * th
            hid[chunk(idx), cols] = (z * gate).astype(jnp.bfloat16)
            slope[chunk(idx), cols] = gate + (0.5 * z) * (1.0 - th * th) * (0.7978845608028654 + 0.10703222440890037 * sq)

    def descend(idx):
        grad_rows = grad[chunk(idx), :]
        total = None
        for first in range(0, width, CHUNK):
            cols = slice(first, first + CHUNK)
            d_hid = lax.dot_general(grad_rows, w2v[cols, :], TRANS_DIMS, preferred_element_type=jnp.float32)
            d_pre = (slope[chunk(idx), cols] * d_hid).astype(jnp.bfloat16)
            dpre[chunk(idx), cols] = d_pre
            part = lax.dot_general(d_pre, w1v[:, cols], TRANS_DIMS, preferred_element_type=jnp.float32)
            total = part if first == 0 else total + part
        sent[chunk(idx), :] = (grad_rows.astype(jnp.float32) + total).astype(jnp.bfloat16)

    for copy in loads:
        copy.wait()
    prepare(0)

    @pl.when(stage == last)
    def _():
        top.wait()

    @pl.loop(0, n_chunks)
    def _(idx):
        @pl.when(stage < last)
        def _():
            hop(idx).wait_recv()

        descend(idx)

        @pl.when(stage > 0)
        def _():
            hop(idx).start()

        @pl.when(idx + 1 < n_chunks)
        def _():
            prepare(idx + 1)

    def weight_grad(idx, side):
        if idx < n_cols:
            left = actv[:, pl.ds(pl.multiple_of(side * half1, half1), half1)]
            right = dpre[:, idx * PART:(idx + 1) * PART]
        else:
            left = hid[:, pl.ds(pl.multiple_of(side * half2 + (idx - n_cols) * half1, half1), half1)]
            right = grad[...]
        return lax.dot_general(left, right, FIRST_DIMS, preferred_element_type=jnp.float32)

    def own_part(idx):
        if idx < n_cols:
            return g1_ref, (slice(None), slice(idx * PART, (idx + 1) * PART))
        return g2_ref, (slice((idx - n_cols) * half1, (idx - n_cols + 1) * half1), slice(None))

    def outbox(idx):
        return slope.at[pl.ds((idx // n_cols) * half1, half1), pl.ds((idx % n_cols) * PART, PART)]

    def post(idx):
        return pltpu.make_async_remote_copy(src_ref=outbox(idx), dst_ref=inbox.at[idx], send_sem=rsend.at[idx], recv_sem=rrecv.at[idx], **peer(data=far))

    for step, (idx, side) in enumerate(steps):
        load_acc(idx, side, step).wait()
        value = accv[step % ahead] + weight_grad(idx, side)
        if step < n_parts:
            outbox(idx)[...] = value
            post(idx).start()
        else:
            ref, where = own_part(idx)
            ref[where] = value
        if step + ahead < len(steps):
            load_acc(*steps[step + ahead], step + ahead).start()

    squares = jnp.zeros(sq_ref.shape, jnp.float32)
    for idx in range(n_parts):
        post(idx).wait_recv()
        ref, where = own_part(idx)
        mean = 0.5 * (ref[where] + inbox[idx])
        ref[where] = mean
        squares = squares + jnp.sum((mean * mean).reshape(half1 // 8, 8, PART), axis=0)
    sq_ref[...] = squares
    for idx in range(n_parts):
        post(idx).wait_send()

    @pl.when(stage > 0)
    def _():
        @pl.loop(0, n_chunks)
        def _(idx):
            hop(idx).wait_send()


def backward_all(act, d_out, w_first, w_second, acc_first, acc_second):
    n_rows, dim = act.shape
    width = w_first.shape[1]
    half1 = dim // 2
    n_chunks = n_rows // ROWS
    n_parts = 2 * (width // PART)
    dma = pltpu.SemaphoreType.DMA
    bf16, f32 = jnp.bfloat16, jnp.float32
    vmem = pl.BlockSpec(memory_space=pltpu.VMEM)
    return pl.pallas_call(
        backward_kernel,
        out_shape=(jax.ShapeDtypeStruct((half1, width), f32), jax.ShapeDtypeStruct((width // 2, dim), f32), jax.ShapeDtypeStruct((8, PART), f32)),
        in_specs=[pl.BlockSpec(memory_space=pl.ANY)] * 6,
        out_specs=(vmem, vmem, vmem),
        scratch_shapes=[
            pltpu.VMEM((n_rows, dim), bf16), pltpu.VMEM((n_rows, dim), bf16),
            pltpu.VMEM((dim, width), bf16), pltpu.VMEM((width, dim), bf16),
            pltpu.VMEM((n_rows, width), bf16), pltpu.VMEM((n_rows, width), f32), pltpu.VMEM((n_rows, width), bf16),
            pltpu.VMEM((n_rows, dim), bf16), pltpu.VMEM((4, half1, PART), f32), pltpu.VMEM((n_parts, half1, PART), f32),
            dma((4,)), dma((4,)), dma((n_chunks,)), dma((n_chunks,)), dma((n_parts,)), dma((n_parts,)),
        ],
        compiler_params=pltpu.CompilerParams(collective_id=1, has_side_effects=True, vmem_limit_bytes=63 * 2 ** 20),
        cost_estimate=pl.CostEstimate(flops=10 * n_rows * dim * width, bytes_accessed=40 * 2 ** 20, transcendentals=0),
        name='backward_all',
    )(act, d_out, w_first, w_second, acc_first, acc_second)


def solution(mesh):
    n_stage = mesh.shape['stage']
    n_rep = mesh.shape['data']
    swap = [(0, 1), (1, 0)]
    w_spec = P('stage', None, None)
    acc_spec = P('data', 'stage', None, None)
    row_spec = P(None, 'data', None)

    def stage_program(w_in, w_out, mom_in, mom_out, var_in, var_out, acc_in, acc_out, stage_acts, d_out, next_x, learn_rate, max_norm):
        rep_idx = lax.axis_index('data')
        half_first, half_second, squares = backward_all(
            stage_acts[0], d_out, w_in[0].astype(jnp.bfloat16), w_out[0].astype(jnp.bfloat16), acc_in[0, 0], acc_out[0, 0])

        def half_of(arr, idx):
            size = arr.shape[0] // n_rep
            return lax.dynamic_slice_in_dim(arr, idx * size, size, 0)

        far_first = lax.ppermute(half_first, 'data', swap)
        far_second = lax.ppermute(half_second, 'data', swap)
        total_norm = jnp.sqrt(lax.psum(jnp.sum(squares), ('data', 'stage')))
        clip_coef = jnp.minimum(1.0, max_norm[0] / (total_norm + NORM_EPS))

        def early(param, moment, second, grad_val):
            new_w, _, _ = adamw_update(half_of(param, rep_idx), half_of(moment, rep_idx), half_of(second, rep_idx), grad_val, clip_coef, learn_rate[0])
            gathered = lax.all_gather(new_w.astype(jnp.bfloat16), ('stage', 'data'), axis=0, tiled=True)
            return gathered.reshape((n_stage,) + param.shape)

        fw_first = early(w_in[0], mom_in[0], var_in[0], half_first)
        fw_second = early(w_out[0], mom_out[0], var_out[0], half_second)
        n_micro, n_rows, dim = next_x.shape
        next_y = forward_all(next_x.reshape(n_micro * n_rows, dim), fw_first, fw_second, n_stage).reshape(next_x.shape)

        def whole(near, far):
            is_low = rep_idx == 0
            return jnp.concatenate([jnp.where(is_low, near, far), jnp.where(is_low, far, near)], axis=0)

        new_first, mom_first, sec_first = adamw_update(w_in[0], mom_in[0], var_in[0], whole(half_first, far_first), clip_coef, learn_rate[0])
        new_second, mom_second, sec_second = adamw_update(w_out[0], mom_out[0], var_out[0], whole(half_second, far_second), clip_coef, learn_rate[0])
        return (new_first[None], new_second[None], mom_first[None], mom_second[None], sec_first[None], sec_second[None], next_y)

    return jax.shard_map(stage_program, mesh=mesh, in_specs=(w_spec, w_spec, w_spec, w_spec, w_spec, w_spec, acc_spec, acc_spec, P('stage', 'data', None), P('data', None), row_spec, P(None), P(None)), out_specs=(w_spec, w_spec, w_spec, w_spec, w_spec, w_spec, row_spec), check_vma=False)
```

```python
import functools

import jax
import jax.numpy as jnp
from jax import lax
from jax.experimental import pallas as pl
from jax.experimental.pallas import tpu as pltpu
from jax.sharding import PartitionSpec as P

BETA_ONE = 0.9
BETA_TWO = 0.95
ADAM_EPS = 1e-8
WEIGHT_DECAY = 0.1
STEP_COUNT = 10
NORM_EPS = 1e-6
TRANS_DIMS = (((1,), (1,)), ((), ()))
FIRST_DIMS = (((0,), (0,)), ((), ()))
TILE = 512
CHUNK = 512
SLOTS = 8
LAG = 4
PRE = 4
SHARED = 4
UPDATE_STEPS = 8
ROWS = 256
PART = 512


def fast_gelu(z):
    inner = z * (0.7978845608028654 + 0.035677408136300125 * (z * z))
    half = 0.5 * z
    return half + half * jnp.tanh(inner)


def forward_kernel(n_own, n_both, x_ref, w1_ref, w2_ref, g1_ref, g2_ref, y_ref, far1_ref, far2_ref,
                   xv, pv, yv, w1v, w2v, xsem, psem, lsem, osem, csend, asend, rsend, crecv, arecv, rrecv, wsend, wrecv, fsend, frecv):
    stage = lax.axis_index('stage')
    rep = lax.axis_index('data')
    far = 1 - rep
    core = stage % 2
    partner = stage + 1 - 2 * core
    across = (stage + 2) % 4
    corner = (partner + 2) % 4
    early = stage < 2
    n_tiles = n_own + n_both
    n_blocks, dim, width = w1v.shape
    half1, half2 = dim // 2, width // 2
    to_core, to_chip, to_rep = {'stage': partner}, {'stage': across}, {'data': far}

    def rows(owner, tile):
        place = jnp.where(tile < n_own, owner * n_own + tile, 4 * n_own + (owner % 2) * n_both + tile - n_own)
        return pl.ds(pl.multiple_of(place * TILE, TILE), TILE)

    def remote(src, dst, send, recv, target):
        return pltpu.make_async_remote_copy(src_ref=src, dst_ref=dst, send_sem=send, recv_sem=recv, device_id=target, device_id_type=pl.DeviceIdType.MESH)

    def load_x(tile):
        return pltpu.make_async_copy(x_ref.at[rows(stage, tile)], xv.at[tile % 2], xsem.at[tile % 2])

    def load_p(tile):
        return pltpu.make_async_copy(x_ref.at[rows(stage, tile)], pv.at[tile], psem.at[tile])

    def part(owner, block, kind):
        if kind == 0:
            return w1v.at[block, pl.ds(pl.multiple_of(owner * half1, half1), half1), :]
        return w2v.at[block, pl.ds(pl.multiple_of(owner * half2, half2), half2), :]

    def move(owner, block, kind, target, lane):
        ref = part(owner, block, kind)
        return remote(ref, ref, wsend.at[lane], wrecv.at[(owner * n_blocks + block) * 2 + kind], target)

    def arrive(owner, block, kind):
        move(owner, block, kind, to_core, 0).wait_recv()

    own = [pltpu.make_async_copy(ref, part(rep, stage, kind), lsem.at[kind]) for kind, ref in enumerate((w1_ref, w2_ref))]
    for copy in own:
        copy.start()

    @pl.when(early)
    def _():
        for tile in range(PRE):
            load_p(tile).start()

    @pl.when(stage >= 2)
    def _():
        load_x(0).start()

    barrier = pltpu.get_barrier_semaphore()
    for target in (to_core, to_chip, to_rep):
        pl.semaphore_signal(barrier, inc=1, device_id=target, device_id_type=pl.DeviceIdType.MESH)
    pl.semaphore_wait(barrier, 3)

    sends = []

    def send(owner, block, kind, target):
        copy = move(owner, block, kind, target, len(sends))
        sends.append(copy)
        copy.start()

    for kind in (0, 1):
        own[kind].wait()
        for target in (to_chip, to_rep, to_core):
            send(rep, stage, kind, target)
    arrive(far, stage, 0)
    send(far, stage, 0, to_core)
    arrive(rep, across, 0)
    send(rep, across, 0, to_rep)
    send(rep, across, 0, to_core)
    arrive(far, stage, 1)
    send(far, stage, 1, to_chip)
    send(far, stage, 1, to_core)
    arrive(rep, across, 1)
    send(rep, across, 1, to_core)
    for owner in (rep, far):
        for kind in (0, 1):
            arrive(owner, partner, kind)

    def block_step(x_rows, block):
        total = None
        for first in range(0, width, CHUNK):
            hidden = jnp.dot(x_rows, w1v[block, :, first:first + CHUNK], preferred_element_type=jnp.float32)
            act_h = fast_gelu(hidden).astype(jnp.bfloat16)
            piece = jnp.dot(act_h, w2v[block, first:first + CHUNK, :], preferred_element_type=jnp.float32)
            total = piece if first == 0 else total + piece
        return (x_rows.astype(jnp.float32) + total).astype(jnp.bfloat16)

    @pl.when(early)
    def _():
        @pl.loop(0, PRE)
        def _(tile):
            load_p(tile).wait()

            @pl.loop(0, 2)
            def _(block):
                pv[tile] = block_step(pv[tile], block)

    for kind in (0, 1):
        arrive(far, across, kind)
        send(far, across, kind, to_core)
    swaps = [remote(src, dst, fsend.at[idx], frecv.at[idx], to_rep) for idx, (src, dst) in enumerate(((g1_ref, far1_ref), (g2_ref, far2_ref)))]
    for copy in swaps:
        copy.start()
    for owner in (rep, far):
        for kind in (0, 1):
            arrive(owner, corner, kind)

    def store_own(tile):
        return pltpu.make_async_copy(yv.at[tile % SLOTS], y_ref.at[rows(stage, tile)], osem.at[tile % SLOTS])

    def give_core(tile):
        return remote(yv.at[tile % SLOTS], y_ref.at[rows(stage, tile)], csend.at[tile % SLOTS], crecv.at[tile], to_core)

    def give_chip(tile):
        return remote(yv.at[tile % SLOTS], y_ref.at[rows(stage, tile)], asend.at[tile % SLOTS], arecv.at[tile], to_chip)

    def pass_on(tile):
        ref = y_ref.at[rows(across, tile)]
        return remote(ref, ref, rsend.at[tile], rrecv.at[tile], to_core)

    def relay(tile):
        ref = y_ref.at[rows(across, tile)]
        remote(ref, ref, asend.at[0], arecv.at[tile], to_chip).wait_recv()
        pass_on(tile).start()

    def free_slot(tile):
        store_own(tile).wait()
        give_core(tile).wait_send()

        @pl.when(tile < n_own)
        def _():
            give_chip(tile).wait_send()

    @pl.loop(0, n_tiles)
    def _(tile):
        skip = jnp.where(early, PRE, 0)

        @pl.when(tile < skip)
        def _():
            xv[tile % 2] = pv[tile % PRE]

        @pl.when(tile >= skip)
        def _():
            load_x(tile).wait()

        @pl.when((tile + 1 >= skip) & (tile + 1 < n_tiles))
        def _():
            load_x(tile + 1).start()

        @pl.when(tile >= SLOTS)
        def _():
            free_slot(tile - SLOTS)

        @pl.loop(0, n_blocks)
        def _(block):
            @pl.when((block >= 2) | (tile >= skip))
            def _():
                result = block_step(xv[tile % 2], block)

                @pl.when(block < n_blocks - 1)
                def _():
                    xv[tile % 2] = result

                @pl.when(block == n_blocks - 1)
                def _():
                    yv[tile % SLOTS] = result

        store_own(tile).start()
        give_core(tile).start()

        @pl.when(tile < n_own)
        def _():
            give_chip(tile).start()

        @pl.when((tile >= LAG) & (tile < LAG + n_own))
        def _():
            relay(tile - LAG)

    for tile in range(max(n_tiles - LAG, 0), n_own):
        relay(tile)

    @pl.loop(n_tiles - SLOTS, n_tiles)
    def _(tile):
        free_slot(tile)

    @pl.loop(0, n_tiles)
    def _(tile):
        ref = y_ref.at[rows(partner, tile)]
        remote(ref, ref, csend.at[0], crecv.at[tile], to_core).wait_recv()

    @pl.loop(0, n_own)
    def _(tile):
        ref = y_ref.at[rows(corner, tile)]
        remote(ref, ref, rsend.at[0], rrecv.at[tile], to_core).wait_recv()
        pass_on(tile).wait_send()

    for copy in sends:
        copy.wait_send()
    for copy in swaps:
        copy.wait()


def forward_all(x_rows, w_first, w_second, near_first, near_second, n_stage, n_both):
    n_rows, dim = x_rows.shape
    width = w_first.shape[1]
    n_own = (n_rows // TILE - 2 * n_both) // 4
    n_tiles = n_own + n_both
    dma = pltpu.SemaphoreType.DMA
    flops = 4 * n_tiles * TILE * dim * width * n_stage
    return pl.pallas_call(
        functools.partial(forward_kernel, n_own, n_both),
        out_shape=(jax.ShapeDtypeStruct((n_rows, dim), jnp.bfloat16), jax.ShapeDtypeStruct(near_first.shape, jnp.float32), jax.ShapeDtypeStruct(near_second.shape, jnp.float32)),
        in_specs=[pl.BlockSpec(memory_space=pl.ANY)] * 5,
        out_specs=(pl.BlockSpec(memory_space=pl.ANY),) * 3,
        scratch_shapes=[
            pltpu.VMEM((2, TILE, dim), jnp.bfloat16),
            pltpu.VMEM((PRE, TILE, dim), jnp.bfloat16),
            pltpu.VMEM((SLOTS, TILE, dim), jnp.bfloat16),
            pltpu.VMEM((n_stage, dim, width), jnp.bfloat16),
            pltpu.VMEM((n_stage, width, dim), jnp.bfloat16),
            dma((2,)), dma((PRE,)), dma((2,)), dma((SLOTS,)), dma((SLOTS,)), dma((SLOTS,)), dma((n_own,)),
            dma((n_tiles,)), dma((n_own,)), dma((n_own,)), dma((14,)), dma((4 * n_stage,)), dma((2,)), dma((2,)),
        ],
        compiler_params=pltpu.CompilerParams(collective_id=0, has_side_effects=True, vmem_limit_bytes=56 * 2 ** 20),
        cost_estimate=pl.CostEstimate(flops=flops, bytes_accessed=2 * n_rows * dim * 2, transcendentals=0),
        name='forward_all',
    )(x_rows, w_first, w_second, near_first, near_second)


def adamw_rows(coef, rate, param, moment, second, grad_val):
    scaled = coef * grad_val
    mom_new = BETA_ONE * moment + (1.0 - BETA_ONE) * scaled
    sec_new = BETA_TWO * second + (1.0 - BETA_TWO) * scaled * scaled
    mom_hat = mom_new * (1.0 / (1.0 - BETA_ONE ** STEP_COUNT))
    sec_hat = sec_new * (1.0 / (1.0 - BETA_TWO ** STEP_COUNT))
    return param - rate * (mom_hat / (jnp.sqrt(sec_hat) + ADAM_EPS) + WEIGHT_DECAY * param), mom_new, sec_new


def near_kernel(half_ref, rate_ref, clip_ref, *refs):
    for side in (0, 1):
        param, moment, second, grad_val = (ref[...] for ref in refs[4 * side:4 * side + 4])
        outs = refs[8 + 4 * side:12 + 4 * side]
        news = adamw_rows(clip_ref[0:1, 0:1], rate_ref[0], param, moment, second, grad_val)
        for ref, new in zip(outs, news):
            ref[...] = new
        outs[3][...] = news[0].astype(jnp.bfloat16)


def far_kernel(half_ref, rate_ref, clip_ref, *refs):
    for side in (0, 1):
        param, moment, second, grad_val = (ref[...] for ref in refs[4 * side:4 * side + 4])
        news = adamw_rows(clip_ref[0:1, 0:1], rate_ref[0], param, moment, second, grad_val)
        for ref, new in zip(refs[14 + 3 * side:17 + 3 * side], news):
            ref[...] = new


def half_update(half_idx, rate, clip, first, second, grads, made):
    steps = UPDATE_STEPS
    f32, bf16 = jnp.float32, jnp.bfloat16
    full, grad_specs, out_specs, out_shape = [], [], [], []
    for arr, grad in zip((first[0], second[0]), grads):
        block = (grad.shape[0] // steps, grad.shape[1])
        picked = pl.BlockSpec(block, lambda step, half: (half[0] * steps + step, 0))
        plain = pl.BlockSpec(block, lambda step, half: (step, 0))
        full += [picked] * 3 + [plain]
        out_specs += [picked] * 3
        out_shape += [jax.ShapeDtypeStruct(arr.shape, f32)] * 3
        if made is None:
            out_specs.append(plain)
            out_shape.append(jax.ShapeDtypeStruct(grad.shape, bf16))
    in_specs = [pl.BlockSpec(memory_space=pltpu.SMEM), pl.BlockSpec(clip.shape, lambda step, half: (0, 0))] + full
    args = [half_idx, rate, clip, *first, grads[0], *second, grads[1]]
    aliases = {}
    if made is not None:
        aliases = {len(args) + idx: idx for idx in range(6)}
        in_specs += [pl.BlockSpec(memory_space=pl.ANY)] * 6
        args += list(made)
    return pl.pallas_call(
        near_kernel if made is None else far_kernel,
        out_shape=tuple(out_shape),
        grid_spec=pltpu.PrefetchScalarGridSpec(num_scalar_prefetch=1, grid=(steps,), in_specs=in_specs, out_specs=tuple(out_specs)),
        input_output_aliases=aliases,
        compiler_params=pltpu.CompilerParams(vmem_limit_bytes=48 * 2 ** 20),
        cost_estimate=pl.CostEstimate(flops=30 * 2 ** 20, bytes_accessed=30 * 2 ** 20, transcendentals=0),
        name='near_update' if made is None else 'far_update',
    )(*args)


def backward_kernel(limit_ref, act_ref, dout_ref, w1_ref, w2_ref, acc1_ref, acc2_ref, g1_ref, g2_ref, clip_ref,
                    actv, grad, w1v, w2v, hid, slope, dpre, sent, accv, inbox,
                    norms, lsem, asem, csend, crecv, rsend, rrecv, nsend, nrecv):
    stage = lax.axis_index('stage')
    rep = lax.axis_index('data')
    far = 1 - rep
    n_rows, dim = actv.shape
    width = w1v.shape[1]
    n_chunks = n_rows // ROWS
    last = 3
    half1 = dim // 2
    half2 = width // 2
    n_parts = inbox.shape[0]
    n_cols = width // PART

    def chunk(idx):
        return pl.ds(pl.multiple_of(idx * ROWS, ROWS), ROWS)

    def peer(**where):
        return dict(device_id=where, device_id_type=pl.DeviceIdType.MESH)

    loads = [pltpu.make_async_copy(act_ref, actv, lsem.at[0]), pltpu.make_async_copy(w1_ref, w1v, lsem.at[1]), pltpu.make_async_copy(w2_ref, w2v, lsem.at[2])]
    for copy in loads:
        copy.start()
    top = pltpu.make_async_copy(dout_ref, grad, lsem.at[3])

    @pl.when(stage == last)
    def _():
        top.start()

    def load_acc(idx, side, step):
        slot = step % accv.shape[0]
        if idx < n_cols:
            src = acc1_ref.at[pl.ds(pl.multiple_of(side * half1, half1), half1), pl.ds(idx * PART, PART)]
        else:
            src = acc2_ref.at[pl.ds(pl.multiple_of(side * half2 + (idx - n_cols) * half1, half1), half1), :]
        return pltpu.make_async_copy(src, accv.at[slot], asem.at[slot])

    steps = [(idx, far) for idx in range(n_parts)] + [(idx, rep) for idx in range(n_parts)]
    ahead = accv.shape[0]
    for step in range(ahead):
        load_acc(*steps[step], step).start()

    barrier = pltpu.get_barrier_semaphore()
    place = rep * 4 + stage
    others = [(place + hop) % 8 for hop in range(1, 8)]
    for other in others:
        pl.semaphore_signal(barrier, inc=1, **peer(data=other // 4, stage=other % 4))
    pl.semaphore_wait(barrier, 7)

    def hop(idx):
        return pltpu.make_async_remote_copy(src_ref=sent.at[chunk(idx)], dst_ref=grad.at[chunk(idx)], send_sem=csend.at[idx], recv_sem=crecv.at[idx],
                                            **peer(stage=(stage + 3) % 4))

    def prepare(idx):
        act = actv[chunk(idx), :]
        for first in range(0, width, CHUNK):
            cols = slice(first, first + CHUNK)
            z = jnp.dot(act, w1v[:, cols], preferred_element_type=jnp.float32)
            sq = z * z
            th = jnp.tanh(z * (0.7978845608028654 + 0.035677408136300125 * sq))
            gate = 0.5 + 0.5 * th
            hid[chunk(idx), cols] = (z * gate).astype(jnp.bfloat16)
            slope[chunk(idx), cols] = gate + (0.5 * z) * (1.0 - th * th) * (0.7978845608028654 + 0.10703222440890037 * sq)

    def descend(idx):
        grad_rows = grad[chunk(idx), :]
        total = None
        for first in range(0, width, CHUNK):
            cols = slice(first, first + CHUNK)
            d_hid = lax.dot_general(grad_rows, w2v[cols, :], TRANS_DIMS, preferred_element_type=jnp.float32)
            d_pre = (slope[chunk(idx), cols] * d_hid).astype(jnp.bfloat16)
            dpre[chunk(idx), cols] = d_pre
            part = lax.dot_general(d_pre, w1v[:, cols], TRANS_DIMS, preferred_element_type=jnp.float32)
            total = part if first == 0 else total + part
        sent[chunk(idx), :] = (grad_rows.astype(jnp.float32) + total).astype(jnp.bfloat16)

    for copy in loads:
        copy.wait()
    prepare(0)

    @pl.when(stage == last)
    def _():
        top.wait()

    @pl.loop(0, n_chunks)
    def _(idx):
        @pl.when(stage < last)
        def _():
            hop(idx).wait_recv()

        descend(idx)

        @pl.when(stage > 0)
        def _():
            hop(idx).start()

        @pl.when(idx + 1 < n_chunks)
        def _():
            prepare(idx + 1)

    def weight_grad(idx, side):
        if idx < n_cols:
            left = actv[:, pl.ds(pl.multiple_of(side * half1, half1), half1)]
            right = dpre[:, idx * PART:(idx + 1) * PART]
        else:
            left = hid[:, pl.ds(pl.multiple_of(side * half2 + (idx - n_cols) * half1, half1), half1)]
            right = grad[...]
        return lax.dot_general(left, right, FIRST_DIMS, preferred_element_type=jnp.float32)

    def own_part(idx):
        if idx < n_cols:
            return g1_ref, (slice(None), slice(idx * PART, (idx + 1) * PART))
        return g2_ref, (slice((idx - n_cols) * half1, (idx - n_cols + 1) * half1), slice(None))

    def outbox(idx):
        return slope.at[pl.ds((idx // n_cols) * half1, half1), pl.ds((idx % n_cols) * PART, PART)]

    def post(idx):
        return pltpu.make_async_remote_copy(src_ref=outbox(idx), dst_ref=inbox.at[idx], send_sem=rsend.at[idx], recv_sem=rrecv.at[idx], **peer(data=far))

    for step, (idx, side) in enumerate(steps):
        load_acc(idx, side, step).wait()
        value = accv[step % ahead] + weight_grad(idx, side)
        if step < n_parts:
            outbox(idx)[...] = value
            post(idx).start()
        else:
            ref, where = own_part(idx)
            ref[where] = value
        if step + ahead < len(steps):
            load_acc(*steps[step + ahead], step + ahead).start()

    squares = jnp.zeros((8, PART), jnp.float32)
    for idx in range(n_parts):
        post(idx).wait_recv()
        ref, where = own_part(idx)
        mean = 0.5 * (ref[where] + inbox[idx])
        ref[where] = mean
        squares = squares + jnp.sum((mean * mean).reshape(half1 // 8, 8, PART), axis=0)
    norms[place] = squares

    def tell(idx):
        return pltpu.make_async_remote_copy(src_ref=norms.at[place], dst_ref=norms.at[place], send_sem=nsend.at[idx], recv_sem=nrecv.at[place],
                                            **peer(data=others[idx] // 4, stage=others[idx] % 4))

    def hear(idx):
        ref = norms.at[others[idx]]
        return pltpu.make_async_remote_copy(src_ref=ref, dst_ref=ref, send_sem=nsend.at[idx], recv_sem=nrecv.at[others[idx]],
                                            **peer(data=others[idx] // 4, stage=others[idx] % 4))

    for idx in range(7):
        tell(idx).start()
    for idx in range(7):
        hear(idx).wait_recv()
    total = norms[0]
    for idx in range(1, 8):
        total = total + norms[idx]
    total = jnp.sum(jnp.sum(total, axis=0, keepdims=True), axis=1, keepdims=True)
    clip = jnp.minimum(1.0, limit_ref[0] / (jnp.sqrt(total) + NORM_EPS))
    clip_ref[...] = jnp.broadcast_to(clip, clip_ref.shape)
    for idx in range(7):
        tell(idx).wait_send()
    for idx in range(n_parts):
        post(idx).wait_send()

    @pl.when(stage > 0)
    def _():
        @pl.loop(0, n_chunks)
        def _(idx):
            hop(idx).wait_send()


def backward_all(limit, act, d_out, w_first, w_second, acc_first, acc_second):
    n_rows, dim = act.shape
    width = w_first.shape[1]
    half1 = dim // 2
    n_chunks = n_rows // ROWS
    n_parts = 2 * (width // PART)
    dma = pltpu.SemaphoreType.DMA
    bf16, f32 = jnp.bfloat16, jnp.float32
    vmem = pl.BlockSpec(memory_space=pltpu.VMEM)
    return pl.pallas_call(
        backward_kernel,
        out_shape=(jax.ShapeDtypeStruct((half1, width), f32), jax.ShapeDtypeStruct((width // 2, dim), f32), jax.ShapeDtypeStruct((8, 128), f32)),
        in_specs=[pl.BlockSpec(memory_space=pltpu.SMEM)] + [pl.BlockSpec(memory_space=pl.ANY)] * 6,
        out_specs=(vmem, vmem, vmem),
        scratch_shapes=[
            pltpu.VMEM((n_rows, dim), bf16), pltpu.VMEM((n_rows, dim), bf16),
            pltpu.VMEM((dim, width), bf16), pltpu.VMEM((width, dim), bf16),
            pltpu.VMEM((n_rows, width), bf16), pltpu.VMEM((n_rows, width), f32), pltpu.VMEM((n_rows, width), bf16),
            pltpu.VMEM((n_rows, dim), bf16), pltpu.VMEM((4, half1, PART), f32), pltpu.VMEM((n_parts, half1, PART), f32), pltpu.VMEM((8, 8, PART), f32),
            dma((4,)), dma((4,)), dma((n_chunks,)), dma((n_chunks,)), dma((n_parts,)), dma((n_parts,)), dma((7,)), dma((8,)),
        ],
        compiler_params=pltpu.CompilerParams(collective_id=1, has_side_effects=True, vmem_limit_bytes=63 * 2 ** 20),
        cost_estimate=pl.CostEstimate(flops=10 * n_rows * dim * width, bytes_accessed=40 * 2 ** 20, transcendentals=0),
        name='backward_all',
    )(limit, act, d_out, w_first, w_second, acc_first, acc_second)


def solution(mesh):
    n_stage = mesh.shape['stage']
    w_spec = P('stage', None, None)
    acc_spec = P('data', 'stage', None, None)
    row_spec = P(None, 'data', None)

    def stage_program(w_in, w_out, mom_in, mom_out, var_in, var_out, acc_in, acc_out, stage_acts, d_out, next_x, learn_rate, max_norm):
        rep_idx = lax.axis_index('data')
        near_first, near_second, clip = backward_all(
            max_norm, stage_acts[0], d_out, w_in[0].astype(jnp.bfloat16), w_out[0].astype(jnp.bfloat16), acc_in[0, 0], acc_out[0, 0])
        first = (w_in[0], mom_in[0], var_in[0])
        second = (w_out[0], mom_out[0], var_out[0])
        near = half_update(rep_idx.reshape(1), learn_rate, clip, first, second, (near_first, near_second), None)
        n_micro, n_rows, dim = next_x.shape
        next_y, far_first, far_second = forward_all(next_x.reshape(n_micro * n_rows, dim), near[3], near[7], near_first, near_second, n_stage, SHARED)
        news = half_update((1 - rep_idx).reshape(1), learn_rate, clip, first, second, (far_first, far_second), near[:3] + near[4:7])
        return (news[0][None], news[3][None], news[1][None], news[4][None], news[2][None], news[5][None], next_y.reshape(next_x.shape))

    return jax.shard_map(stage_program, mesh=mesh, in_specs=(w_spec, w_spec, w_spec, w_spec, w_spec, w_spec, acc_spec, acc_spec, P('stage', 'data', None), P('data', None), row_spec, P(None), P(None)), out_specs=(w_spec, w_spec, w_spec, w_spec, w_spec, w_spec, row_spec), check_vma=False)
```

```python
import functools

import jax
import jax.numpy as jnp
from jax import lax
from jax.experimental import pallas as pl
from jax.experimental.pallas import tpu as pltpu
from jax.sharding import PartitionSpec as P

BETA_ONE = 0.9
BETA_TWO = 0.95
ADAM_EPS = 1e-8
WEIGHT_DECAY = 0.1
STEP_COUNT = 10
NORM_EPS = 1e-6
TRANS_DIMS = (((1,), (1,)), ((), ()))
FIRST_DIMS = (((0,), (0,)), ((), ()))
TILE = 512
CHUNK = 1024
SLOTS = 8
LAG = 4
PRE = 4
SHARED = 2
UPDATE_STEPS = 8
ROWS = 256
PART = 512
COLS = 512


def gelu_of_half(half):
    return half + half * jnp.tanh(half * (1.5957691216057308 + 0.28541926509040104 * (half * half)))


def forward_kernel(n_own, n_both, x_ref, w1_ref, w2_ref, g1_ref, g2_ref, y_ref, far1_ref, far2_ref,
                   xv, pv, yv, w1v, w2v, xsem, psem, lsem, osem, csend, asend, rsend, crecv, arecv, rrecv, wsend, wrecv, fsend, frecv):
    stage = lax.axis_index('stage')
    rep = lax.axis_index('data')
    far = 1 - rep
    core = stage % 2
    partner = stage + 1 - 2 * core
    across = (stage + 2) % 4
    corner = (partner + 2) % 4
    early = stage < 2
    n_tiles = n_own + n_both
    n_blocks, dim, width = w1v.shape
    half1, half2 = dim // 2, width // 2
    to_core, to_chip, to_rep = {'stage': partner}, {'stage': across}, {'data': far}

    def rows(owner, tile):
        place = jnp.where(tile < n_own, owner * n_own + tile, 4 * n_own + (owner % 2) * n_both + tile - n_own)
        return pl.ds(pl.multiple_of(place * TILE, TILE), TILE)

    def remote(src, dst, send, recv, target):
        return pltpu.make_async_remote_copy(src_ref=src, dst_ref=dst, send_sem=send, recv_sem=recv, device_id=target, device_id_type=pl.DeviceIdType.MESH)

    def load_x(tile):
        return pltpu.make_async_copy(x_ref.at[rows(stage, tile)], xv.at[tile % 2], xsem.at[tile % 2])

    def load_p(tile):
        return pltpu.make_async_copy(x_ref.at[rows(stage, tile)], pv.at[tile], psem.at[tile])

    def part(owner, block, kind):
        if kind == 0:
            return w1v.at[block, pl.ds(pl.multiple_of(owner * half1, half1), half1), :]
        return w2v.at[block, pl.ds(pl.multiple_of(owner * half2, half2), half2), :]

    def move(owner, block, kind, target, lane):
        ref = part(owner, block, kind)
        return remote(ref, ref, wsend.at[lane], wrecv.at[(owner * n_blocks + block) * 2 + kind], target)

    def arrive(owner, block, kind):
        move(owner, block, kind, to_core, 0).wait_recv()

    own = [pltpu.make_async_copy(ref, part(rep, stage, kind), lsem.at[kind]) for kind, ref in enumerate((w1_ref, w2_ref))]
    for copy in own:
        copy.start()

    @pl.when(early)
    def _():
        for tile in range(PRE):
            load_p(tile).start()

    @pl.when(stage >= 2)
    def _():
        load_x(0).start()

    barrier = pltpu.get_barrier_semaphore()
    for target in (to_core, to_chip, to_rep):
        pl.semaphore_signal(barrier, inc=1, device_id=target, device_id_type=pl.DeviceIdType.MESH)
    pl.semaphore_wait(barrier, 3)

    sends = []

    def send(owner, block, kind, target):
        copy = move(owner, block, kind, target, len(sends))
        sends.append(copy)
        copy.start()

    for kind in (0, 1):
        own[kind].wait()
        for target in (to_chip, to_rep, to_core):
            send(rep, stage, kind, target)
    arrive(far, stage, 0)
    send(far, stage, 0, to_core)
    arrive(rep, across, 0)
    send(rep, across, 0, to_rep)
    send(rep, across, 0, to_core)
    arrive(far, stage, 1)
    send(far, stage, 1, to_chip)
    send(far, stage, 1, to_core)
    arrive(rep, across, 1)
    send(rep, across, 1, to_core)
    for owner in (rep, far):
        for kind in (0, 1):
            arrive(owner, partner, kind)

    def block_step(src, block, dst):
        half = TILE // 2
        pieces = [(side, first) for first in range(0, width, CHUNK) for side in (0, 1)]
        x_rows = [src[side * half:(side + 1) * half, :] for side in (0, 1)]
        total = [None, None]
        act_h = {}
        for turn in range(len(pieces) + 2):
            if turn < len(pieces):
                side, first = pieces[turn]
                halved = jnp.dot(x_rows[side], w1v[block, :, first:first + CHUNK], preferred_element_type=jnp.float32)
                act_h[turn] = gelu_of_half(halved).astype(jnp.bfloat16)
            if turn >= 2:
                side, first = pieces[turn - 2]
                piece = jnp.dot(act_h.pop(turn - 2), w2v[block, first:first + CHUNK, :], preferred_element_type=jnp.float32)
                total[side] = piece if first == 0 else total[side] + piece
        for side in (0, 1):
            dst[side * half:(side + 1) * half, :] = (x_rows[side].astype(jnp.float32) + total[side]).astype(jnp.bfloat16)

    @pl.when(early)
    def _():
        @pl.loop(0, PRE)
        def _(tile):
            load_p(tile).wait()

            @pl.loop(0, 2)
            def _(block):
                block_step(pv.at[tile], block, pv.at[tile])

    for kind in (0, 1):
        arrive(far, across, kind)
        send(far, across, kind, to_core)
    swaps = [remote(src, dst, fsend.at[idx], frecv.at[idx], to_rep) for idx, (src, dst) in enumerate(((g1_ref, far1_ref), (g2_ref, far2_ref)))]
    for copy in swaps:
        copy.start()
    for owner in (rep, far):
        for kind in (0, 1):
            arrive(owner, corner, kind)

    def store_own(tile):
        return pltpu.make_async_copy(yv.at[tile % SLOTS], y_ref.at[rows(stage, tile)], osem.at[tile % SLOTS])

    def give_core(tile):
        return remote(yv.at[tile % SLOTS], y_ref.at[rows(stage, tile)], csend.at[tile % SLOTS], crecv.at[tile], to_core)

    def give_chip(tile):
        return remote(yv.at[tile % SLOTS], y_ref.at[rows(stage, tile)], asend.at[tile % SLOTS], arecv.at[tile], to_chip)

    def pass_on(tile):
        ref = y_ref.at[rows(across, tile)]
        return remote(ref, ref, rsend.at[tile], rrecv.at[tile], to_core)

    def relay(tile):
        ref = y_ref.at[rows(across, tile)]
        remote(ref, ref, asend.at[0], arecv.at[tile], to_chip).wait_recv()
        pass_on(tile).start()

    def free_slot(tile):
        store_own(tile).wait()
        give_core(tile).wait_send()

        @pl.when(tile < n_own)
        def _():
            give_chip(tile).wait_send()

    @pl.loop(0, n_tiles)
    def _(tile):
        skip = jnp.where(early, PRE, 0)

        @pl.when(tile < skip)
        def _():
            xv[tile % 2] = pv[tile % PRE]

        @pl.when(tile >= skip)
        def _():
            load_x(tile).wait()

        @pl.when((tile + 1 >= skip) & (tile + 1 < n_tiles))
        def _():
            load_x(tile + 1).start()

        @pl.when(tile >= SLOTS)
        def _():
            free_slot(tile - SLOTS)

        @pl.loop(0, n_blocks)
        def _(block):
            @pl.when((block >= 2) | (tile >= skip))
            def _():
                block_step(xv.at[tile % 2], block, xv.at[tile % 2])

        yv[tile % SLOTS] = xv[tile % 2]
        store_own(tile).start()
        give_core(tile).start()

        @pl.when(tile < n_own)
        def _():
            give_chip(tile).start()

        @pl.when((tile >= LAG) & (tile < LAG + n_own))
        def _():
            relay(tile - LAG)

    for tile in range(max(n_tiles - LAG, 0), n_own):
        relay(tile)

    @pl.loop(n_tiles - SLOTS, n_tiles)
    def _(tile):
        free_slot(tile)

    @pl.loop(0, n_tiles)
    def _(tile):
        ref = y_ref.at[rows(partner, tile)]
        remote(ref, ref, csend.at[0], crecv.at[tile], to_core).wait_recv()

    @pl.loop(0, n_own)
    def _(tile):
        ref = y_ref.at[rows(corner, tile)]
        remote(ref, ref, rsend.at[0], rrecv.at[tile], to_core).wait_recv()
        pass_on(tile).wait_send()

    for copy in sends:
        copy.wait_send()
    for copy in swaps:
        copy.wait()


def forward_all(x_rows, w_first, w_second, near_first, near_second, n_stage, n_both):
    n_rows, dim = x_rows.shape
    width = w_first.shape[1]
    n_own = (n_rows // TILE - 2 * n_both) // 4
    n_tiles = n_own + n_both
    dma = pltpu.SemaphoreType.DMA
    flops = 4 * n_tiles * TILE * dim * width * n_stage
    return pl.pallas_call(
        functools.partial(forward_kernel, n_own, n_both),
        out_shape=(jax.ShapeDtypeStruct((n_rows, dim), jnp.bfloat16), jax.ShapeDtypeStruct(near_first.shape, jnp.float32), jax.ShapeDtypeStruct(near_second.shape, jnp.float32)),
        in_specs=[pl.BlockSpec(memory_space=pl.ANY)] * 5,
        out_specs=(pl.BlockSpec(memory_space=pl.ANY),) * 3,
        scratch_shapes=[
            pltpu.VMEM((2, TILE, dim), jnp.bfloat16),
            pltpu.VMEM((PRE, TILE, dim), jnp.bfloat16),
            pltpu.VMEM((SLOTS, TILE, dim), jnp.bfloat16),
            pltpu.VMEM((n_stage, dim, width), jnp.bfloat16),
            pltpu.VMEM((n_stage, width, dim), jnp.bfloat16),
            dma((2,)), dma((PRE,)), dma((2,)), dma((SLOTS,)), dma((SLOTS,)), dma((SLOTS,)), dma((n_own,)),
            dma((n_tiles,)), dma((n_own,)), dma((n_own,)), dma((14,)), dma((4 * n_stage,)), dma((2,)), dma((2,)),
        ],
        compiler_params=pltpu.CompilerParams(collective_id=0, has_side_effects=True, vmem_limit_bytes=56 * 2 ** 20),
        cost_estimate=pl.CostEstimate(flops=flops, bytes_accessed=2 * n_rows * dim * 2, transcendentals=0),
        name='forward_all',
    )(x_rows, w_first, w_second, near_first, near_second)


def adamw_rows(coef, rate, param, moment, second, grad_val):
    scaled = coef * grad_val
    mom_new = BETA_ONE * moment + (1.0 - BETA_ONE) * scaled
    sec_new = BETA_TWO * second + (1.0 - BETA_TWO) * scaled * scaled
    mom_hat = mom_new * (1.0 / (1.0 - BETA_ONE ** STEP_COUNT))
    sec_hat = sec_new * (1.0 / (1.0 - BETA_TWO ** STEP_COUNT))
    return param - rate * (mom_hat / (jnp.sqrt(sec_hat) + ADAM_EPS) + WEIGHT_DECAY * param), mom_new, sec_new


def near_kernel(half_ref, rate_ref, clip_ref, *refs):
    for side in (0, 1):
        param, moment, second, grad_val = (ref[...] for ref in refs[4 * side:4 * side + 4])
        outs = refs[8 + 4 * side:12 + 4 * side]
        news = adamw_rows(clip_ref[0:1, 0:1], rate_ref[0], param, moment, second, grad_val)
        for ref, new in zip(outs, news):
            ref[...] = new
        outs[3][...] = ((0.5 if side == 0 else 1.0) * news[0]).astype(jnp.bfloat16)


def far_kernel(half_ref, rate_ref, clip_ref, *refs):
    for side in (0, 1):
        param, moment, second, grad_val = (ref[...] for ref in refs[4 * side:4 * side + 4])
        news = adamw_rows(clip_ref[0:1, 0:1], rate_ref[0], param, moment, second, grad_val)
        for ref, new in zip(refs[14 + 3 * side:17 + 3 * side], news):
            ref[...] = new


def half_update(half_idx, rate, clip, first, second, grads, made):
    steps = UPDATE_STEPS
    f32, bf16 = jnp.float32, jnp.bfloat16
    full, grad_specs, out_specs, out_shape = [], [], [], []
    for arr, grad in zip((first[0], second[0]), grads):
        block = (grad.shape[0] // steps, grad.shape[1])
        picked = pl.BlockSpec(block, lambda step, half: (half[0] * steps + step, 0))
        plain = pl.BlockSpec(block, lambda step, half: (step, 0))
        full += [picked] * 3 + [plain]
        out_specs += [picked] * 3
        out_shape += [jax.ShapeDtypeStruct(arr.shape, f32)] * 3
        if made is None:
            out_specs.append(plain)
            out_shape.append(jax.ShapeDtypeStruct(grad.shape, bf16))
    in_specs = [pl.BlockSpec(memory_space=pltpu.SMEM), pl.BlockSpec(clip.shape, lambda step, half: (0, 0))] + full
    args = [half_idx, rate, clip, *first, grads[0], *second, grads[1]]
    aliases = {}
    if made is not None:
        aliases = {len(args) + idx: idx for idx in range(6)}
        in_specs += [pl.BlockSpec(memory_space=pl.ANY)] * 6
        args += list(made)
    return pl.pallas_call(
        near_kernel if made is None else far_kernel,
        out_shape=tuple(out_shape),
        grid_spec=pltpu.PrefetchScalarGridSpec(num_scalar_prefetch=1, grid=(steps,), in_specs=in_specs, out_specs=tuple(out_specs)),
        input_output_aliases=aliases,
        compiler_params=pltpu.CompilerParams(vmem_limit_bytes=48 * 2 ** 20),
        cost_estimate=pl.CostEstimate(flops=30 * 2 ** 20, bytes_accessed=30 * 2 ** 20, transcendentals=0),
        name='near_update' if made is None else 'far_update',
    )(*args)


def backward_kernel(limit_ref, act_ref, dout_ref, w1_ref, w2_ref, acc1_ref, acc2_ref, g1_ref, g2_ref, clip_ref,
                    actv, grad, w1v, w2v, hid, slope, dpre, sent, accv, inbox,
                    norms, lsem, asem, csend, crecv, rsend, rrecv, nsend, nrecv):
    stage = lax.axis_index('stage')
    rep = lax.axis_index('data')
    far = 1 - rep
    n_rows, dim = actv.shape
    width = w1v.shape[1]
    n_chunks = n_rows // ROWS
    last = 3
    half1 = dim // 2
    half2 = width // 2
    n_parts = inbox.shape[0]
    n_cols = width // PART

    def chunk(idx):
        return pl.ds(pl.multiple_of(idx * ROWS, ROWS), ROWS)

    def peer(**where):
        return dict(device_id=where, device_id_type=pl.DeviceIdType.MESH)

    loads = [pltpu.make_async_copy(act_ref, actv, lsem.at[0]), pltpu.make_async_copy(w1_ref, w1v, lsem.at[1]), pltpu.make_async_copy(w2_ref, w2v, lsem.at[2])]
    for copy in loads:
        copy.start()
    top = pltpu.make_async_copy(dout_ref, grad, lsem.at[3])

    @pl.when(stage == last)
    def _():
        top.start()

    def load_acc(idx, side, step):
        slot = step % accv.shape[0]
        if idx < n_cols:
            src = acc1_ref.at[pl.ds(pl.multiple_of(side * half1, half1), half1), pl.ds(idx * PART, PART)]
        else:
            src = acc2_ref.at[pl.ds(pl.multiple_of(side * half2 + (idx - n_cols) * half1, half1), half1), :]
        return pltpu.make_async_copy(src, accv.at[slot], asem.at[slot])

    steps = [(idx, far) for idx in range(n_parts)] + [(idx, rep) for idx in range(n_parts)]
    ahead = accv.shape[0]
    for step in range(ahead):
        load_acc(*steps[step], step).start()

    barrier = pltpu.get_barrier_semaphore()
    place = rep * 4 + stage
    others = [(place + hop) % 8 for hop in range(1, 8)]
    for other in others:
        pl.semaphore_signal(barrier, inc=1, **peer(data=other // 4, stage=other % 4))
    pl.semaphore_wait(barrier, 7)

    def hop(idx):
        return pltpu.make_async_remote_copy(src_ref=sent.at[chunk(idx)], dst_ref=grad.at[chunk(idx)], send_sem=csend.at[idx], recv_sem=crecv.at[idx],
                                            **peer(stage=(stage + 3) % 4))

    def prepare(idx):
        act = actv[chunk(idx), :]
        for first in range(0, width, COLS):
            cols = slice(first, first + COLS)
            z = jnp.dot(act, w1v[:, cols], preferred_element_type=jnp.float32)
            sq = z * z
            th = jnp.tanh(z * (0.7978845608028654 + 0.035677408136300125 * sq))
            gate = 0.5 + 0.5 * th
            hid[chunk(idx), cols] = (z * gate).astype(jnp.bfloat16)
            slope[chunk(idx), cols] = gate + (0.5 * z) * (1.0 - th * th) * (0.7978845608028654 + 0.10703222440890037 * sq)

    def descend(idx):
        grad_rows = grad[chunk(idx), :]
        total = None
        for first in range(0, width, COLS):
            cols = slice(first, first + COLS)
            d_hid = lax.dot_general(grad_rows, w2v[cols, :], TRANS_DIMS, preferred_element_type=jnp.float32)
            d_pre = (slope[chunk(idx), cols] * d_hid).astype(jnp.bfloat16)
            dpre[chunk(idx), cols] = d_pre
            part = lax.dot_general(d_pre, w1v[:, cols], TRANS_DIMS, preferred_element_type=jnp.float32)
            total = part if first == 0 else total + part
        sent[chunk(idx), :] = (grad_rows.astype(jnp.float32) + total).astype(jnp.bfloat16)

    for copy in loads:
        copy.wait()
    prepare(0)

    @pl.when(stage == last)
    def _():
        top.wait()

    @pl.loop(0, n_chunks)
    def _(idx):
        @pl.when(stage < last)
        def _():
            hop(idx).wait_recv()

        descend(idx)

        @pl.when(stage > 0)
        def _():
            hop(idx).start()

        @pl.when(idx + 1 < n_chunks)
        def _():
            prepare(idx + 1)

    def weight_grad(idx, side):
        if idx < n_cols:
            left = actv[:, pl.ds(pl.multiple_of(side * half1, half1), half1)]
            right = dpre[:, idx * PART:(idx + 1) * PART]
        else:
            left = hid[:, pl.ds(pl.multiple_of(side * half2 + (idx - n_cols) * half1, half1), half1)]
            right = grad[...]
        return lax.dot_general(left, right, FIRST_DIMS, preferred_element_type=jnp.float32)

    def own_part(idx):
        if idx < n_cols:
            return g1_ref, (slice(None), slice(idx * PART, (idx + 1) * PART))
        return g2_ref, (slice((idx - n_cols) * half1, (idx - n_cols + 1) * half1), slice(None))

    def outbox(idx):
        return slope.at[pl.ds((idx // n_cols) * half1, half1), pl.ds((idx % n_cols) * PART, PART)]

    def post(idx):
        return pltpu.make_async_remote_copy(src_ref=outbox(idx), dst_ref=inbox.at[idx], send_sem=rsend.at[idx], recv_sem=rrecv.at[idx], **peer(data=far))

    for step, (idx, side) in enumerate(steps):
        load_acc(idx, side, step).wait()
        value = accv[step % ahead] + weight_grad(idx, side)
        if step < n_parts:
            outbox(idx)[...] = value
            post(idx).start()
        else:
            ref, where = own_part(idx)
            ref[where] = value
        if step + ahead < len(steps):
            load_acc(*steps[step + ahead], step + ahead).start()

    squares = jnp.zeros((8, PART), jnp.float32)
    for idx in range(n_parts):
        post(idx).wait_recv()
        ref, where = own_part(idx)
        mean = 0.5 * (ref[where] + inbox[idx])
        ref[where] = mean
        squares = squares + jnp.sum((mean * mean).reshape(half1 // 8, 8, PART), axis=0)
    norms[place] = squares

    def tell(idx):
        return pltpu.make_async_remote_copy(src_ref=norms.at[place], dst_ref=norms.at[place], send_sem=nsend.at[idx], recv_sem=nrecv.at[place],
                                            **peer(data=others[idx] // 4, stage=others[idx] % 4))

    def hear(idx):
        ref = norms.at[others[idx]]
        return pltpu.make_async_remote_copy(src_ref=ref, dst_ref=ref, send_sem=nsend.at[idx], recv_sem=nrecv.at[others[idx]],
                                            **peer(data=others[idx] // 4, stage=others[idx] % 4))

    for idx in range(7):
        tell(idx).start()
    for idx in range(7):
        hear(idx).wait_recv()
    total = norms[0]
    for idx in range(1, 8):
        total = total + norms[idx]
    total = jnp.sum(jnp.sum(total, axis=0, keepdims=True), axis=1, keepdims=True)
    clip = jnp.minimum(1.0, limit_ref[0] / (jnp.sqrt(total) + NORM_EPS))
    clip_ref[...] = jnp.broadcast_to(clip, clip_ref.shape)
    for idx in range(7):
        tell(idx).wait_send()
    for idx in range(n_parts):
        post(idx).wait_send()

    @pl.when(stage > 0)
    def _():
        @pl.loop(0, n_chunks)
        def _(idx):
            hop(idx).wait_send()


def backward_all(limit, act, d_out, w_first, w_second, acc_first, acc_second):
    n_rows, dim = act.shape
    width = w_first.shape[1]
    half1 = dim // 2
    n_chunks = n_rows // ROWS
    n_parts = 2 * (width // PART)
    dma = pltpu.SemaphoreType.DMA
    bf16, f32 = jnp.bfloat16, jnp.float32
    vmem = pl.BlockSpec(memory_space=pltpu.VMEM)
    return pl.pallas_call(
        backward_kernel,
        out_shape=(jax.ShapeDtypeStruct((half1, width), f32), jax.ShapeDtypeStruct((width // 2, dim), f32), jax.ShapeDtypeStruct((8, 128), f32)),
        in_specs=[pl.BlockSpec(memory_space=pltpu.SMEM)] + [pl.BlockSpec(memory_space=pl.ANY)] * 6,
        out_specs=(vmem, vmem, vmem),
        scratch_shapes=[
            pltpu.VMEM((n_rows, dim), bf16), pltpu.VMEM((n_rows, dim), bf16),
            pltpu.VMEM((dim, width), bf16), pltpu.VMEM((width, dim), bf16),
            pltpu.VMEM((n_rows, width), bf16), pltpu.VMEM((n_rows, width), f32), pltpu.VMEM((n_rows, width), bf16),
            pltpu.VMEM((n_rows, dim), bf16), pltpu.VMEM((4, half1, PART), f32), pltpu.VMEM((n_parts, half1, PART), f32), pltpu.VMEM((8, 8, PART), f32),
            dma((4,)), dma((4,)), dma((n_chunks,)), dma((n_chunks,)), dma((n_parts,)), dma((n_parts,)), dma((7,)), dma((8,)),
        ],
        compiler_params=pltpu.CompilerParams(collective_id=1, has_side_effects=True, vmem_limit_bytes=63 * 2 ** 20),
        cost_estimate=pl.CostEstimate(flops=10 * n_rows * dim * width, bytes_accessed=40 * 2 ** 20, transcendentals=0),
        name='backward_all',
    )(limit, act, d_out, w_first, w_second, acc_first, acc_second)


def solution(mesh):
    n_stage = mesh.shape['stage']
    w_spec = P('stage', None, None)
    acc_spec = P('data', 'stage', None, None)
    row_spec = P(None, 'data', None)

    def stage_program(w_in, w_out, mom_in, mom_out, var_in, var_out, acc_in, acc_out, stage_acts, d_out, next_x, learn_rate, max_norm):
        rep_idx = lax.axis_index('data')
        near_first, near_second, clip = backward_all(
            max_norm, stage_acts[0], d_out, w_in[0].astype(jnp.bfloat16), w_out[0].astype(jnp.bfloat16), acc_in[0, 0], acc_out[0, 0])
        first = (w_in[0], mom_in[0], var_in[0])
        second = (w_out[0], mom_out[0], var_out[0])
        near = half_update(rep_idx.reshape(1), learn_rate, clip, first, second, (near_first, near_second), None)
        n_micro, n_rows, dim = next_x.shape
        next_y, far_first, far_second = forward_all(next_x.reshape(n_micro * n_rows, dim), near[3], near[7], near_first, near_second, n_stage, SHARED)
        news = half_update((1 - rep_idx).reshape(1), learn_rate, clip, first, second, (far_first, far_second), near[:3] + near[4:7])
        return (news[0][None], news[3][None], news[1][None], news[4][None], news[2][None], news[5][None], next_y.reshape(next_x.shape))

    return jax.shard_map(stage_program, mesh=mesh, in_specs=(w_spec, w_spec, w_spec, w_spec, w_spec, w_spec, acc_spec, acc_spec, P('stage', 'data', None), P('data', None), row_spec, P(None), P(None)), out_specs=(w_spec, w_spec, w_spec, w_spec, w_spec, w_spec, row_spec), check_vma=False)
```

```python
import functools

import jax
import jax.numpy as jnp
from jax import lax
from jax.experimental import pallas as pl
from jax.experimental.pallas import tpu as pltpu
from jax.sharding import PartitionSpec as P

BETA_ONE = 0.9
BETA_TWO = 0.95
ADAM_EPS = 1e-8
WEIGHT_DECAY = 0.1
STEP_COUNT = 10
NORM_EPS = 1e-6
TRANS_DIMS = (((1,), (1,)), ((), ()))
FIRST_DIMS = (((0,), (0,)), ((), ()))
TILE = 512
CHUNK = 1024
SLOTS = 8
LAG = 4
PRE = 4
SHARED = 4
UPDATE_STEPS = 8
FINAL_STEPS = 16
ADAM_ROWS = 32
ROWS = 256
PART = 512
COLS = 512


def gelu_of_half(half):
    return half + half * jnp.tanh(half * (1.5957691216057308 + 0.28541926509040104 * (half * half)))


def forward_kernel(n_own, n_both, x_ref, w1_ref, w2_ref, xw1_ref, xw2_ref, rw1_ref, rw2_ref, g1_ref, g2_ref, y_ref, far1_ref, far2_ref,
                   xv, pv, yv, w1v, w2v, xsem, psem, lsem, osem, csend, asend, rsend, crecv, arecv, rrecv, wsend, wrecv, fsend, frecv):
    stage = lax.axis_index('stage')
    rep = lax.axis_index('data')
    far = 1 - rep
    core = stage % 2
    partner = stage + 1 - 2 * core
    across = (stage + 2) % 4
    corner = (partner + 2) % 4
    early = stage < 2
    n_tiles = n_own + n_both
    n_blocks, dim, width = w1v.shape
    half1, half2 = dim // 2, width // 2
    to_core, to_chip, to_rep = {'stage': partner}, {'stage': across}, {'data': far}

    def rows(owner, tile):
        place = jnp.where(tile < n_own, owner * n_own + tile, 4 * n_own + (owner % 2) * n_both + tile - n_own)
        return pl.ds(pl.multiple_of(place * TILE, TILE), TILE)

    def remote(src, dst, send, recv, target):
        return pltpu.make_async_remote_copy(src_ref=src, dst_ref=dst, send_sem=send, recv_sem=recv, device_id=target, device_id_type=pl.DeviceIdType.MESH)

    def load_x(tile):
        return pltpu.make_async_copy(x_ref.at[rows(stage, tile)], xv.at[tile % 2], xsem.at[tile % 2])

    def load_p(tile):
        return pltpu.make_async_copy(x_ref.at[rows(stage, tile)], pv.at[tile], psem.at[tile])

    def part(owner, block, kind):
        if kind == 0:
            return w1v.at[block, pl.ds(pl.multiple_of(owner * half1, half1), half1), :]
        return w2v.at[block, pl.ds(pl.multiple_of(owner * half2, half2), half2), :]

    def move(owner, block, kind, target, lane):
        ref = part(owner, block, kind)
        return remote(ref, ref, wsend.at[lane], wrecv.at[(owner * n_blocks + block) * 2 + kind], target)

    def arrive(owner, block, kind):
        move(owner, block, kind, to_core, 0).wait_recv()

    fetched = {}
    for lane, (where, kind, ref) in enumerate((('chip', 0, xw1_ref), ('rep', 1, rw2_ref), ('rep', 0, rw1_ref), ('chip', 1, xw2_ref), ('own', 0, w1_ref), ('own', 1, w2_ref))):
        owner, block = {'own': (rep, stage), 'chip': (rep, across), 'rep': (far, stage)}[where]
        fetched[where, kind] = pltpu.make_async_copy(ref, part(owner, block, kind), lsem.at[lane])
        fetched[where, kind].start()

    @pl.when(early)
    def _():
        for tile in range(PRE):
            load_p(tile).start()

    @pl.when(stage >= 2)
    def _():
        load_x(0).start()

    barrier = pltpu.get_barrier_semaphore()
    for target in (to_core, to_chip, to_rep):
        pl.semaphore_signal(barrier, inc=1, device_id=target, device_id_type=pl.DeviceIdType.MESH)
    pl.semaphore_wait(barrier, 3)

    sends = []

    def send(owner, block, kind, target):
        copy = move(owner, block, kind, target, len(sends))
        sends.append(copy)
        copy.start()

    fetched['chip', 0].wait()
    send(rep, across, 0, to_rep)
    fetched['rep', 1].wait()
    send(far, stage, 1, to_chip)
    for kind in (0, 1):
        fetched['own', kind].wait()
        send(rep, stage, kind, to_core)
    fetched['rep', 0].wait()
    for kind in (0, 1):
        send(far, stage, kind, to_core)
    fetched['chip', 1].wait()
    for kind in (0, 1):
        send(rep, across, kind, to_core)
    for owner in (rep, far):
        for kind in (0, 1):
            arrive(owner, partner, kind)

    def block_step(src, block, dst):
        half = TILE // 2
        pieces = [(side, first) for first in range(0, width, CHUNK) for side in (0, 1)]
        x_rows = [src[side * half:(side + 1) * half, :] for side in (0, 1)]
        total = [None, None]
        act_h = {}
        for turn in range(len(pieces) + 2):
            if turn < len(pieces):
                side, first = pieces[turn]
                halved = jnp.dot(x_rows[side], w1v[block, :, first:first + CHUNK], preferred_element_type=jnp.float32)
                act_h[turn] = gelu_of_half(halved).astype(jnp.bfloat16)
            if turn >= 2:
                side, first = pieces[turn - 2]
                piece = jnp.dot(act_h.pop(turn - 2), w2v[block, first:first + CHUNK, :], preferred_element_type=jnp.float32)
                total[side] = piece if first == 0 else total[side] + piece
        for side in (0, 1):
            dst[side * half:(side + 1) * half, :] = (x_rows[side].astype(jnp.float32) + total[side]).astype(jnp.bfloat16)

    @pl.when(early)
    def _():
        @pl.loop(0, PRE)
        def _(tile):
            load_p(tile).wait()

            @pl.loop(0, 2)
            def _(block):
                block_step(pv.at[tile], block, pv.at[tile])

    for kind in (0, 1):
        arrive(far, across, kind)
        send(far, across, kind, to_core)
    swaps = [remote(src, dst, fsend.at[idx], frecv.at[idx], to_rep) for idx, (src, dst) in enumerate(((g1_ref, far1_ref), (g2_ref, far2_ref)))]
    for copy in swaps:
        copy.start()
    for owner in (rep, far):
        for kind in (0, 1):
            arrive(owner, corner, kind)

    def store_own(tile):
        return pltpu.make_async_copy(yv.at[tile % SLOTS], y_ref.at[rows(stage, tile)], osem.at[tile % SLOTS])

    def give_core(tile):
        return remote(yv.at[tile % SLOTS], y_ref.at[rows(stage, tile)], csend.at[tile % SLOTS], crecv.at[tile], to_core)

    def give_chip(tile):
        return remote(yv.at[tile % SLOTS], y_ref.at[rows(stage, tile)], asend.at[tile % SLOTS], arecv.at[tile], to_chip)

    def pass_on(tile):
        ref = y_ref.at[rows(across, tile)]
        return remote(ref, ref, rsend.at[tile], rrecv.at[tile], to_core)

    def relay(tile):
        ref = y_ref.at[rows(across, tile)]
        remote(ref, ref, asend.at[0], arecv.at[tile], to_chip).wait_recv()
        pass_on(tile).start()

    def free_slot(tile):
        store_own(tile).wait()
        give_core(tile).wait_send()

        @pl.when(tile < n_own)
        def _():
            give_chip(tile).wait_send()

    @pl.loop(0, n_tiles)
    def _(tile):
        skip = jnp.where(early, PRE, 0)

        @pl.when(tile < skip)
        def _():
            xv[tile % 2] = pv[tile % PRE]

        @pl.when(tile >= skip)
        def _():
            load_x(tile).wait()

        @pl.when((tile + 1 >= skip) & (tile + 1 < n_tiles))
        def _():
            load_x(tile + 1).start()

        @pl.when(tile >= SLOTS)
        def _():
            free_slot(tile - SLOTS)

        @pl.loop(0, n_blocks)
        def _(block):
            @pl.when((block >= 2) | (tile >= skip))
            def _():
                block_step(xv.at[tile % 2], block, xv.at[tile % 2])

        yv[tile % SLOTS] = xv[tile % 2]
        store_own(tile).start()
        give_core(tile).start()

        @pl.when(tile < n_own)
        def _():
            give_chip(tile).start()

        @pl.when((tile >= LAG) & (tile < LAG + n_own))
        def _():
            relay(tile - LAG)

    for tile in range(max(n_tiles - LAG, 0), n_own):
        relay(tile)

    @pl.loop(n_tiles - SLOTS, n_tiles)
    def _(tile):
        free_slot(tile)

    @pl.loop(0, n_tiles)
    def _(tile):
        ref = y_ref.at[rows(partner, tile)]
        remote(ref, ref, csend.at[0], crecv.at[tile], to_core).wait_recv()

    @pl.loop(0, n_own)
    def _(tile):
        ref = y_ref.at[rows(corner, tile)]
        remote(ref, ref, rsend.at[0], rrecv.at[tile], to_core).wait_recv()
        pass_on(tile).wait_send()

    for copy in sends:
        copy.wait_send()
    for copy in swaps:
        copy.wait()


def forward_all(x_rows, own, chip, twin, near_first, near_second, n_stage, n_both):
    n_rows, dim = x_rows.shape
    width = own[0].shape[1]
    n_own = (n_rows // TILE - 2 * n_both) // 4
    n_tiles = n_own + n_both
    dma = pltpu.SemaphoreType.DMA
    flops = 4 * n_tiles * TILE * dim * width * n_stage
    return pl.pallas_call(
        functools.partial(forward_kernel, n_own, n_both),
        out_shape=(jax.ShapeDtypeStruct((n_rows, dim), jnp.bfloat16), jax.ShapeDtypeStruct(near_first.shape, jnp.float32), jax.ShapeDtypeStruct(near_second.shape, jnp.float32)),
        in_specs=[pl.BlockSpec(memory_space=pl.ANY)] * 9,
        out_specs=(pl.BlockSpec(memory_space=pl.ANY),) * 3,
        scratch_shapes=[
            pltpu.VMEM((2, TILE, dim), jnp.bfloat16),
            pltpu.VMEM((PRE, TILE, dim), jnp.bfloat16),
            pltpu.VMEM((SLOTS, TILE, dim), jnp.bfloat16),
            pltpu.VMEM((n_stage, dim, width), jnp.bfloat16),
            pltpu.VMEM((n_stage, width, dim), jnp.bfloat16),
            dma((2,)), dma((PRE,)), dma((6,)), dma((SLOTS,)), dma((SLOTS,)), dma((SLOTS,)), dma((n_own,)),
            dma((n_tiles,)), dma((n_own,)), dma((n_own,)), dma((10,)), dma((4 * n_stage,)), dma((2,)), dma((2,)),
        ],
        compiler_params=pltpu.CompilerParams(collective_id=0, has_side_effects=True, vmem_limit_bytes=56 * 2 ** 20),
        cost_estimate=pl.CostEstimate(flops=flops, bytes_accessed=2 * n_rows * dim * 2, transcendentals=0),
        name='forward_all',
    )(x_rows, *own, *chip, *twin, near_first, near_second)


def adamw_rows(coef, rate, param, moment, second, grad_val):
    scaled = coef * grad_val
    mom_new = BETA_ONE * moment + (1.0 - BETA_ONE) * scaled
    sec_new = BETA_TWO * second + (1.0 - BETA_TWO) * scaled * scaled
    mom_hat = mom_new * (1.0 / (1.0 - BETA_ONE ** STEP_COUNT))
    sec_hat = sec_new * (1.0 / (1.0 - BETA_TWO ** STEP_COUNT))
    return param - rate * (mom_hat / (jnp.sqrt(sec_hat) + ADAM_EPS) + WEIGHT_DECAY * param), mom_new, sec_new


def update_kernel(n_ins, half_ref, rate_ref, clip_ref, *refs):
    outs = refs[n_ins:]
    for side in (0, 1):
        param, moment, second, grad_val = (ref[...] for ref in refs[4 * side:4 * side + 4])
        news = adamw_rows(clip_ref[0:1, 0:1], rate_ref[0], param, moment, second, grad_val)
        for ref, new in zip(outs[3 * side:3 * side + 3], news):
            ref[...] = new
    if len(outs) == 7:
        outs[6][...] = refs[8][...]


def half_update(half_idx, rate, clip, first, second, grads, made=(), rows=None):
    steps = FINAL_STEPS if made else UPDATE_STEPS
    full, out_specs, out_shape = [], [], []
    for arr, grad in zip((first[0], second[0]), grads):
        block = (grad.shape[0] // steps, grad.shape[1])
        picked = pl.BlockSpec(block, lambda step, half: (half[0] * steps + step, 0))
        full += [picked] * 3 + [pl.BlockSpec(block, lambda step, half: (step, 0))]
        out_specs += [picked] * 3
        out_shape += [jax.ShapeDtypeStruct(arr.shape, jnp.float32)] * 3
    in_specs = [pl.BlockSpec(memory_space=pltpu.SMEM), pl.BlockSpec(clip.shape, lambda step, half: (0, 0))] + full
    args = [half_idx, rate, clip, *first, grads[0], *second, grads[1]]
    aliases = {}
    if made:
        spec = pl.BlockSpec((rows.shape[0] // steps, rows.shape[1]), lambda step, half: (step, 0))
        in_specs.append(spec)
        args.append(rows)
        out_specs.append(spec)
        out_shape.append(jax.ShapeDtypeStruct(rows.shape, rows.dtype))
        aliases = {len(args) + idx: idx for idx in range(6)}
        in_specs += [pl.BlockSpec(memory_space=pl.ANY)] * 6
        args += list(made)
    return pl.pallas_call(
        functools.partial(update_kernel, len(in_specs) - 2),
        out_shape=tuple(out_shape),
        grid_spec=pltpu.PrefetchScalarGridSpec(num_scalar_prefetch=1, grid=(steps,), in_specs=in_specs, out_specs=tuple(out_specs)),
        input_output_aliases=aliases,
        compiler_params=pltpu.CompilerParams(vmem_limit_bytes=62 * 2 ** 20),
        cost_estimate=pl.CostEstimate(flops=30 * 2 ** 20, bytes_accessed=30 * 2 ** 20, transcendentals=0),
        name='far_update' if made else 'near_update',
    )(*args)


def backward_kernel(limit_ref, rate_ref, act_ref, dout_ref, w1_ref, w2_ref, m1_ref, m2_ref, v1_ref, v2_ref, acc1_ref, acc2_ref,
                    g1_ref, g2_ref, clip_ref, b1_ref, b2_ref,
                    actv, grad, w1v, w2v, hid, slope, dpre, sent, accv, inbox,
                    norms, lsem, hsem, asem, csend, crecv, rsend, rrecv, nsend, nrecv):
    stage = lax.axis_index('stage')
    rep = lax.axis_index('data')
    far = 1 - rep
    n_rows, dim = actv.shape
    width = w1v.shape[1]
    n_chunks = n_rows // ROWS
    last = 3
    half1 = dim // 2
    half2 = width // 2
    n_parts = inbox.shape[0]
    n_cols = width // PART

    def chunk(idx):
        return pl.ds(pl.multiple_of(idx * ROWS, ROWS), ROWS)

    def peer(**where):
        return dict(device_id=where, device_id_type=pl.DeviceIdType.MESH)

    loads = [pltpu.make_async_copy(w1_ref, slope.at[2 * dim:3 * dim, :], lsem.at[0]), pltpu.make_async_copy(act_ref, actv, lsem.at[1])]
    loads += [pltpu.make_async_copy(w2_ref.at[idx * dim:(idx + 1) * dim, :], slope.at[3 * dim:4 * dim, idx * dim:(idx + 1) * dim], lsem.at[2 + idx]) for idx in range(4)]
    for copy in loads:
        copy.start()
    top = pltpu.make_async_copy(dout_ref, grad, lsem.at[6])

    @pl.when(stage == last)
    def _():
        top.start()

    def load_acc(idx, side, step):
        slot = step % accv.shape[0]
        if idx < n_cols:
            src = acc1_ref.at[pl.ds(pl.multiple_of(side * half1, half1), half1), pl.ds(idx * PART, PART)]
        else:
            src = acc2_ref.at[pl.ds(pl.multiple_of(side * half2 + (idx - n_cols) * half1, half1), half1), :]
        return pltpu.make_async_copy(src, accv.at[slot], asem.at[slot])

    steps = [(idx, far) for idx in range(n_parts)] + [(idx, rep) for idx in range(n_parts)]
    ahead = accv.shape[0]
    for step in range(ahead):
        load_acc(*steps[step], step).start()

    barrier = pltpu.get_barrier_semaphore()
    place = rep * 4 + stage
    others = [(place + hop) % 8 for hop in range(1, 8)]
    for other in others:
        pl.semaphore_signal(barrier, inc=1, **peer(data=other // 4, stage=other % 4))
    pl.semaphore_wait(barrier, 7)

    def hop(idx):
        return pltpu.make_async_remote_copy(src_ref=sent.at[chunk(idx)], dst_ref=grad.at[chunk(idx)], send_sem=csend.at[idx], recv_sem=crecv.at[idx],
                                            **peer(stage=(stage + 3) % 4))

    def prepare(idx):
        act = actv[chunk(idx), :]
        for first in range(0, width, COLS):
            cols = slice(first, first + COLS)
            z = jnp.dot(act, w1v[:, cols], preferred_element_type=jnp.float32)
            sq = z * z
            th = jnp.tanh(z * (0.7978845608028654 + 0.035677408136300125 * sq))
            gate = 0.5 + 0.5 * th
            hid[chunk(idx), cols] = (z * gate).astype(jnp.bfloat16)
            slope[chunk(idx), cols] = gate + (0.5 * z) * (1.0 - th * th) * (0.7978845608028654 + 0.10703222440890037 * sq)

    def descend(idx):
        grad_rows = grad[chunk(idx), :]
        total = None
        for first in range(0, width, COLS):
            cols = slice(first, first + COLS)
            d_hid = lax.dot_general(grad_rows, w2v[cols, :], TRANS_DIMS, preferred_element_type=jnp.float32)
            d_pre = (slope[chunk(idx), cols] * d_hid).astype(jnp.bfloat16)
            dpre[chunk(idx), cols] = d_pre
            part = lax.dot_general(d_pre, w1v[:, cols], TRANS_DIMS, preferred_element_type=jnp.float32)
            total = part if first == 0 else total + part
        sent[chunk(idx), :] = (grad_rows.astype(jnp.float32) + total).astype(jnp.bfloat16)

    loads[0].wait()

    @pl.loop(0, dim // 64)
    def _(idx):
        span = pl.ds(pl.multiple_of(idx * 64, 64), 64)
        w1v[span, :] = slope[pl.ds(pl.multiple_of(2 * dim + idx * 64, 64), 64), :].astype(jnp.bfloat16)

    loads[1].wait()
    prepare(0)
    for copy in loads[2:]:
        copy.wait()

    @pl.loop(0, dim // 64)
    def _(idx):
        for group in range(4):
            span = pl.ds(pl.multiple_of(group * dim + idx * 64, 64), 64)
            w2v[span, :] = slope[pl.ds(pl.multiple_of(3 * dim + idx * 64, 64), 64), group * dim:(group + 1) * dim].astype(jnp.bfloat16)

    @pl.when(stage == last)
    def _():
        top.wait()

    @pl.loop(0, n_chunks)
    def _(idx):
        @pl.when(stage < last)
        def _():
            hop(idx).wait_recv()

        descend(idx)

        @pl.when(stage > 0)
        def _():
            hop(idx).start()

        @pl.when(idx + 1 < n_chunks)
        def _():
            prepare(idx + 1)

    near = []
    for idx, ref in enumerate((w1_ref, m1_ref, v1_ref)):
        near.append(pltpu.make_async_copy(ref.at[pl.ds(pl.multiple_of(rep * half1, half1), half1), :], slope.at[dim + idx * half1:dim + (idx + 1) * half1, :], hsem.at[len(near)]))
    for idx, ref in enumerate((w2_ref, m2_ref, v2_ref)):
        for group in range(4):
            near.append(pltpu.make_async_copy(ref.at[pl.ds(pl.multiple_of(rep * half2 + group * half1, half1), half1), :],
                                              slope.at[dim + (3 + idx) * half1:dim + (4 + idx) * half1, group * dim:(group + 1) * dim], hsem.at[len(near)]))
    for copy in near:
        copy.start()

    def weight_grad(idx, side):
        if idx < n_cols:
            left = actv[:, pl.ds(pl.multiple_of(side * half1, half1), half1)]
            right = dpre[:, idx * PART:(idx + 1) * PART]
        else:
            left = hid[:, pl.ds(pl.multiple_of(side * half2 + (idx - n_cols) * half1, half1), half1)]
            right = grad[...]
        return lax.dot_general(left, right, FIRST_DIMS, preferred_element_type=jnp.float32)

    def own_part(idx):
        if idx < n_cols:
            return g1_ref, (slice(None), slice(idx * PART, (idx + 1) * PART))
        return g2_ref, (slice((idx - n_cols) * half1, (idx - n_cols + 1) * half1), slice(None))

    def outbox(idx):
        return slope.at[pl.ds((idx // n_cols) * half1, half1), pl.ds((idx % n_cols) * PART, PART)]

    def post(idx):
        return pltpu.make_async_remote_copy(src_ref=outbox(idx), dst_ref=inbox.at[idx], send_sem=rsend.at[idx], recv_sem=rrecv.at[idx], **peer(data=far))

    for step, (idx, side) in enumerate(steps):
        load_acc(idx, side, step).wait()
        value = accv[step % ahead] + weight_grad(idx, side)
        if step < n_parts:
            outbox(idx)[...] = value
            post(idx).start()
        else:
            ref, where = own_part(idx)
            ref[where] = value
        if step + ahead < len(steps):
            load_acc(*steps[step + ahead], step + ahead).start()

    squares = jnp.zeros((8, PART), jnp.float32)
    for idx in range(n_parts):
        post(idx).wait_recv()
        ref, where = own_part(idx)
        mean = 0.5 * (ref[where] + inbox[idx])
        ref[where] = mean
        squares = squares + jnp.sum((mean * mean).reshape(half1 // 8, 8, PART), axis=0)
    norms[place] = squares

    def tell(idx):
        return pltpu.make_async_remote_copy(src_ref=norms.at[place], dst_ref=norms.at[place], send_sem=nsend.at[idx], recv_sem=nrecv.at[place],
                                            **peer(data=others[idx] // 4, stage=others[idx] % 4))

    def hear(idx):
        ref = norms.at[others[idx]]
        return pltpu.make_async_remote_copy(src_ref=ref, dst_ref=ref, send_sem=nsend.at[idx], recv_sem=nrecv.at[others[idx]],
                                            **peer(data=others[idx] // 4, stage=others[idx] % 4))

    for idx in range(7):
        tell(idx).start()
    for idx in range(7):
        hear(idx).wait_recv()
    total = norms[0]
    for idx in range(1, 8):
        total = total + norms[idx]
    total = jnp.sum(jnp.sum(total, axis=0, keepdims=True), axis=1, keepdims=True)
    clip = jnp.minimum(1.0, limit_ref[0] / (jnp.sqrt(total) + NORM_EPS))
    clip_ref[...] = jnp.broadcast_to(clip, clip_ref.shape)
    for copy in near:
        copy.wait()

    @pl.loop(0, half1 // ADAM_ROWS)
    def _(idx):
        def from_slope(which, cols):
            return slope[pl.ds(pl.multiple_of(dim + which * half1 + idx * ADAM_ROWS, ADAM_ROWS), ADAM_ROWS), cols]

        coef = clip_ref[0:1, 0:1]
        span = pl.ds(pl.multiple_of(idx * ADAM_ROWS, ADAM_ROWS), ADAM_ROWS)
        every = slice(0, width)
        new_w, _, _ = adamw_rows(coef, rate_ref[0], from_slope(0, every), from_slope(1, every), from_slope(2, every), g1_ref[span, :])
        b1_ref[span, :] = (0.5 * new_w).astype(jnp.bfloat16)
        for group in range(4):
            cols = slice(group * dim, (group + 1) * dim)
            span = pl.ds(pl.multiple_of(group * half1 + idx * ADAM_ROWS, ADAM_ROWS), ADAM_ROWS)
            new_w, _, _ = adamw_rows(coef, rate_ref[0], from_slope(3, cols), from_slope(4, cols), from_slope(5, cols), g2_ref[span, :])
            b2_ref[span, :] = new_w.astype(jnp.bfloat16)

    for idx in range(7):
        tell(idx).wait_send()
    for idx in range(n_parts):
        post(idx).wait_send()

    @pl.when(stage > 0)
    def _():
        @pl.loop(0, n_chunks)
        def _(idx):
            hop(idx).wait_send()


def backward_all(limit, rate, act, d_out, first, second, acc_first, acc_second):
    n_rows, dim = act.shape
    width = first[0].shape[1]
    half1 = dim // 2
    n_chunks = n_rows // ROWS
    n_parts = 2 * (width // PART)
    dma = pltpu.SemaphoreType.DMA
    bf16, f32 = jnp.bfloat16, jnp.float32
    vmem = pl.BlockSpec(memory_space=pltpu.VMEM)
    return pl.pallas_call(
        backward_kernel,
        out_shape=(jax.ShapeDtypeStruct((half1, width), f32), jax.ShapeDtypeStruct((width // 2, dim), f32), jax.ShapeDtypeStruct((8, 128), f32),
                   jax.ShapeDtypeStruct((half1, width), bf16), jax.ShapeDtypeStruct((width // 2, dim), bf16)),
        in_specs=[pl.BlockSpec(memory_space=pltpu.SMEM)] * 2 + [pl.BlockSpec(memory_space=pl.ANY)] * 10,
        out_specs=(vmem,) * 5,
        scratch_shapes=[
            pltpu.VMEM((n_rows, dim), bf16), pltpu.VMEM((n_rows, dim), bf16),
            pltpu.VMEM((dim, width), bf16), pltpu.VMEM((width, dim), bf16),
            pltpu.VMEM((n_rows, width), bf16), pltpu.VMEM((n_rows, width), f32), pltpu.VMEM((n_rows, width), bf16),
            pltpu.VMEM((n_rows, dim), bf16), pltpu.VMEM((4, half1, PART), f32), pltpu.VMEM((n_parts, half1, PART), f32), pltpu.VMEM((8, 8, PART), f32),
            dma((7,)), dma((15,)), dma((4,)), dma((n_chunks,)), dma((n_chunks,)), dma((n_parts,)), dma((n_parts,)), dma((7,)), dma((8,)),
        ],
        compiler_params=pltpu.CompilerParams(collective_id=1, has_side_effects=True, vmem_limit_bytes=63 * 2 ** 20),
        cost_estimate=pl.CostEstimate(flops=10 * n_rows * dim * width, bytes_accessed=40 * 2 ** 20, transcendentals=0),
        name='backward_all',
    )(limit, rate, act, d_out, first[0], second[0], first[1], second[1], first[2], second[2], acc_first, acc_second)


def solution(mesh):
    n_stage = mesh.shape['stage']
    w_spec = P('stage', None, None)
    acc_spec = P('data', 'stage', None, None)
    row_spec = P(None, 'data', None)

    def stage_program(w_in, w_out, mom_in, mom_out, var_in, var_out, acc_in, acc_out, stage_acts, d_out, next_x, learn_rate, max_norm):
        rep_idx = lax.axis_index('data')
        first = (w_in[0], mom_in[0], var_in[0])
        second = (w_out[0], mom_out[0], var_out[0])
        near_first, near_second, clip, half_first, half_second = backward_all(
            max_norm, learn_rate, stage_acts[0], d_out, first, second, acc_in[0, 0], acc_out[0, 0])
        own = (half_first, half_second)
        chip = tuple(lax.ppermute(arr, 'stage', [(src, (src + 2) % 4) for src in range(4)]) for arr in own)
        twin = tuple(lax.ppermute(arr, 'data', [(0, 1), (1, 0)]) for arr in own)
        near = half_update(rep_idx.reshape(1), learn_rate, clip, first, second, (near_first, near_second))
        n_micro, n_rows, dim = next_x.shape
        rows, far_first, far_second = forward_all(next_x.reshape(n_micro * n_rows, dim), own, chip, twin, near_first, near_second, n_stage, SHARED)
        *news, next_y = half_update((1 - rep_idx).reshape(1), learn_rate, clip, first, second, (far_first, far_second), near, rows)
        return (news[0][None], news[3][None], news[1][None], news[4][None], news[2][None], news[5][None], next_y.reshape(next_x.shape))

    return jax.shard_map(stage_program, mesh=mesh, in_specs=(w_spec, w_spec, w_spec, w_spec, w_spec, w_spec, acc_spec, acc_spec, P('stage', 'data', None), P('data', None), row_spec, P(None), P(None)), out_specs=(w_spec, w_spec, w_spec, w_spec, w_spec, w_spec, row_spec), check_vma=False)
```

```python
import functools

import jax
import jax.numpy as jnp
from jax import lax
from jax.experimental import pallas as pl
from jax.experimental.pallas import tpu as pltpu
from jax.sharding import PartitionSpec as P

BETA_ONE = 0.9
BETA_TWO = 0.95
ADAM_EPS = 1e-8
WEIGHT_DECAY = 0.1
STEP_COUNT = 10
NORM_EPS = 1e-6
TRANS_DIMS = (((1,), (1,)), ((), ()))
FIRST_DIMS = (((0,), (0,)), ((), ()))
TILE = 512
CHUNK = 1024
FORWARD_VMEM = 30
LAG = 4
PRE = 4
SHARED = 4
UPDATE_STEPS = 8
FINAL_STEPS = 16
ADAM_ROWS = 32
ROWS = 256
PART = 512
COLS = 512


def gelu_of_half(half):
    return half + half * jnp.tanh(half * (1.5957691216057308 + 0.28541926509040104 * (half * half)))


def forward_kernel(n_own, n_both, x_ref, w1_ref, w2_ref, xw1_ref, xw2_ref, rw1_ref, rw2_ref, g1_ref, g2_ref, y_ref, far1_ref, far2_ref,
                   xv, pv, w1v, w2v, xsem, psem, lsem, csend, asend, rsend, crecv, arecv, rrecv, wsend, wrecv, fsend, frecv):
    stage = lax.axis_index('stage')
    rep = lax.axis_index('data')
    far = 1 - rep
    core = stage % 2
    partner = stage + 1 - 2 * core
    across = (stage + 2) % 4
    corner = (partner + 2) % 4
    early = stage < 2
    n_tiles = n_own + n_both
    n_blocks, dim, width = w1v.shape
    half1, half2 = dim // 2, width // 2
    to_core, to_chip, to_rep = {'stage': partner}, {'stage': across}, {'data': far}

    def rows(owner, tile):
        place = jnp.where(tile < n_own, owner * n_own + tile, 4 * n_own + (owner % 2) * n_both + tile - n_own)
        return pl.ds(pl.multiple_of(place * TILE, TILE), TILE)

    def remote(src, dst, send, recv, target):
        return pltpu.make_async_remote_copy(src_ref=src, dst_ref=dst, send_sem=send, recv_sem=recv, device_id=target, device_id_type=pl.DeviceIdType.MESH)

    def load_x(tile):
        return pltpu.make_async_copy(x_ref.at[rows(stage, tile)], xv.at[tile % 2], xsem.at[tile % 2])

    def load_p(tile):
        return pltpu.make_async_copy(x_ref.at[rows(stage, tile)], pv.at[tile], psem.at[tile])

    def part(owner, block, kind):
        if kind == 0:
            return w1v.at[block, pl.ds(pl.multiple_of(owner * half1, half1), half1), :]
        return w2v.at[block, pl.ds(pl.multiple_of(owner * half2, half2), half2), :]

    def move(owner, block, kind, target, lane):
        ref = part(owner, block, kind)
        return remote(ref, ref, wsend.at[lane], wrecv.at[(owner * n_blocks + block) * 2 + kind], target)

    def arrive(owner, block, kind):
        move(owner, block, kind, to_core, 0).wait_recv()

    fetched = {}
    for lane, (where, kind, ref) in enumerate((('chip', 0, xw1_ref), ('rep', 1, rw2_ref), ('rep', 0, rw1_ref), ('chip', 1, xw2_ref), ('own', 0, w1_ref), ('own', 1, w2_ref))):
        owner, block = {'own': (rep, stage), 'chip': (rep, across), 'rep': (far, stage)}[where]
        fetched[where, kind] = pltpu.make_async_copy(ref, part(owner, block, kind), lsem.at[lane])
        fetched[where, kind].start()

    @pl.when(early)
    def _():
        for tile in range(PRE):
            load_p(tile).start()

    @pl.when(stage >= 2)
    def _():
        load_x(0).start()

    barrier = pltpu.get_barrier_semaphore()
    for target in (to_core, to_chip, to_rep):
        pl.semaphore_signal(barrier, inc=1, device_id=target, device_id_type=pl.DeviceIdType.MESH)
    pl.semaphore_wait(barrier, 3)

    sends = []

    def send(owner, block, kind, target):
        copy = move(owner, block, kind, target, len(sends))
        sends.append(copy)
        copy.start()

    fetched['chip', 0].wait()
    send(rep, across, 0, to_rep)
    fetched['rep', 1].wait()
    send(far, stage, 1, to_chip)
    for kind in (0, 1):
        fetched['own', kind].wait()
        send(rep, stage, kind, to_core)
    fetched['rep', 0].wait()
    for kind in (0, 1):
        send(far, stage, kind, to_core)
    fetched['chip', 1].wait()
    for kind in (0, 1):
        send(rep, across, kind, to_core)
    for owner in (rep, far):
        for kind in (0, 1):
            arrive(owner, partner, kind)

    def block_step(src, block, dst):
        half = TILE // 2
        pieces = [(side, first) for first in range(0, width, CHUNK) for side in (0, 1)]
        x_rows = [src[side * half:(side + 1) * half, :] for side in (0, 1)]
        total = [None, None]
        act_h = {}
        for turn in range(len(pieces) + 2):
            if turn < len(pieces):
                side, first = pieces[turn]
                halved = jnp.dot(x_rows[side], w1v[block, :, first:first + CHUNK], preferred_element_type=jnp.float32)
                act_h[turn] = gelu_of_half(halved).astype(jnp.bfloat16)
            if turn >= 2:
                side, first = pieces[turn - 2]
                piece = jnp.dot(act_h.pop(turn - 2), w2v[block, first:first + CHUNK, :], preferred_element_type=jnp.float32)
                total[side] = piece if first == 0 else total[side] + piece
        for side in (0, 1):
            dst[side * half:(side + 1) * half, :] = (x_rows[side].astype(jnp.float32) + total[side]).astype(jnp.bfloat16)

    @pl.when(early)
    def _():
        @pl.loop(0, PRE)
        def _(tile):
            load_p(tile).wait()

            @pl.loop(0, 2)
            def _(block):
                block_step(pv.at[tile], block, pv.at[tile])

    for kind in (0, 1):
        arrive(far, across, kind)
        send(far, across, kind, to_core)
    swaps = [remote(src, dst, fsend.at[idx], frecv.at[idx], to_rep) for idx, (src, dst) in enumerate(((g1_ref, far1_ref), (g2_ref, far2_ref)))]
    for copy in swaps:
        copy.start()
    for owner in (rep, far):
        for kind in (0, 1):
            arrive(owner, corner, kind)

    def give(tile, send, recv, target):
        ref = y_ref.at[rows(stage, tile)]
        return remote(ref, ref, send.at[tile], recv.at[tile], target)

    def give_core(tile):
        return give(tile, csend, crecv, to_core)

    def give_chip(tile):
        return give(tile, asend, arecv, to_chip)

    def pass_on(tile):
        ref = y_ref.at[rows(across, tile)]
        return remote(ref, ref, rsend.at[tile], rrecv.at[tile], to_core)

    def relay(tile):
        ref = y_ref.at[rows(across, tile)]
        remote(ref, ref, asend.at[0], arecv.at[tile], to_chip).wait_recv()
        pass_on(tile).start()

    @pl.loop(0, n_tiles)
    def _(tile):
        skip = jnp.where(early, PRE, 0)

        @pl.when(tile < skip)
        def _():
            xv[tile % 2] = pv[tile % PRE]

        @pl.when(tile >= skip)
        def _():
            load_x(tile).wait()

        @pl.when((tile + 1 >= skip) & (tile + 1 < n_tiles))
        def _():
            load_x(tile + 1).start()

        @pl.loop(0, n_blocks)
        def _(block):
            @pl.when((block >= 2) | (tile >= skip))
            def _():
                block_step(xv.at[tile % 2], block, xv.at[tile % 2])

        y_ref[rows(stage, tile), :] = xv[tile % 2]
        give_core(tile).start()

        @pl.when(tile < n_own)
        def _():
            give_chip(tile).start()

        @pl.when((tile >= LAG) & (tile < LAG + n_own))
        def _():
            relay(tile - LAG)

    for tile in range(max(n_tiles - LAG, 0), n_own):
        relay(tile)

    @pl.loop(0, n_tiles)
    def _(tile):
        ref = y_ref.at[rows(partner, tile)]
        remote(ref, ref, csend.at[0], crecv.at[tile], to_core).wait_recv()
        give_core(tile).wait_send()

    @pl.loop(0, n_own)
    def _(tile):
        ref = y_ref.at[rows(corner, tile)]
        remote(ref, ref, rsend.at[0], rrecv.at[tile], to_core).wait_recv()
        pass_on(tile).wait_send()
        give_chip(tile).wait_send()

    for copy in sends:
        copy.wait_send()
    for copy in swaps:
        copy.wait()


def forward_all(x_rows, own, chip, twin, near_first, near_second, n_stage, n_both):
    n_rows, dim = x_rows.shape
    width = own[0].shape[1]
    n_own = (n_rows // TILE - 2 * n_both) // 4
    n_tiles = n_own + n_both
    dma = pltpu.SemaphoreType.DMA
    flops = 4 * n_tiles * TILE * dim * width * n_stage
    return pl.pallas_call(
        functools.partial(forward_kernel, n_own, n_both),
        out_shape=(pltpu.VMEM((n_rows, dim), jnp.bfloat16), jax.ShapeDtypeStruct(near_first.shape, jnp.float32), jax.ShapeDtypeStruct(near_second.shape, jnp.float32)),
        in_specs=[pl.BlockSpec(memory_space=pl.ANY)] * 9,
        out_specs=(pl.BlockSpec(memory_space=pltpu.VMEM),) + (pl.BlockSpec(memory_space=pl.ANY),) * 2,
        scratch_shapes=[
            pltpu.VMEM((2, TILE, dim), jnp.bfloat16),
            pltpu.VMEM((PRE, TILE, dim), jnp.bfloat16),
            pltpu.VMEM((n_stage, dim, width), jnp.bfloat16),
            pltpu.VMEM((n_stage, width, dim), jnp.bfloat16),
            dma((2,)), dma((PRE,)), dma((6,)), dma((n_tiles,)), dma((n_own,)), dma((n_own,)),
            dma((n_tiles,)), dma((n_own,)), dma((n_own,)), dma((10,)), dma((4 * n_stage,)), dma((2,)), dma((2,)),
        ],
        compiler_params=pltpu.CompilerParams(collective_id=0, has_side_effects=True, vmem_limit_bytes=FORWARD_VMEM * 2 ** 20),
        cost_estimate=pl.CostEstimate(flops=flops, bytes_accessed=2 * n_rows * dim * 2, transcendentals=0),
        name='forward_all',
    )(x_rows, *own, *chip, *twin, near_first, near_second)


def adamw_rows(coef, rate, param, moment, second, grad_val):
    scaled = coef * grad_val
    mom_new = BETA_ONE * moment + (1.0 - BETA_ONE) * scaled
    sec_new = BETA_TWO * second + (1.0 - BETA_TWO) * scaled * scaled
    mom_hat = mom_new * (1.0 / (1.0 - BETA_ONE ** STEP_COUNT))
    sec_hat = sec_new * (1.0 / (1.0 - BETA_TWO ** STEP_COUNT))
    return param - rate * (mom_hat / (jnp.sqrt(sec_hat) + ADAM_EPS) + WEIGHT_DECAY * param), mom_new, sec_new


def update_kernel(n_ins, half_ref, rate_ref, clip_ref, *refs):
    outs = refs[n_ins:]
    if len(outs) == 8:
        step, steps = pl.program_id(0), pl.num_programs(0)

        def drain(idx):
            size = outs[6].shape[0] // FINAL_STEPS
            span = pl.ds(pl.multiple_of(idx * size, size), size)
            return pltpu.make_async_copy(refs[8].at[span], outs[6].at[span], outs[7].at[idx])

        drain(step).start()

    for side in (0, 1):
        param, moment, second, grad_val = (ref[...] for ref in refs[4 * side:4 * side + 4])
        news = adamw_rows(clip_ref[0:1, 0:1], rate_ref[0], param, moment, second, grad_val)
        for ref, new in zip(outs[3 * side:3 * side + 3], news):
            ref[...] = new
    if len(outs) == 8:
        @pl.when(step == steps - 1)
        def _():
            for idx in range(FINAL_STEPS):
                drain(idx).wait()


def half_update(half_idx, rate, clip, first, second, grads, made=(), rows=None):
    steps = FINAL_STEPS if made else UPDATE_STEPS
    full, out_specs, out_shape = [], [], []
    for arr, grad in zip((first[0], second[0]), grads):
        block = (grad.shape[0] // steps, grad.shape[1])
        picked = pl.BlockSpec(block, lambda step, half: (half[0] * steps + step, 0))
        full += [picked] * 3 + [pl.BlockSpec(block, lambda step, half: (step, 0))]
        out_specs += [picked] * 3
        out_shape += [jax.ShapeDtypeStruct(arr.shape, jnp.float32)] * 3
    in_specs = [pl.BlockSpec(memory_space=pltpu.SMEM), pl.BlockSpec(clip.shape, lambda step, half: (0, 0))] + full
    args = [half_idx, rate, clip, *first, grads[0], *second, grads[1]]
    aliases = {}
    if made:
        in_specs.append(pl.BlockSpec(memory_space=pl.ANY))
        args.append(pltpu.with_memory_space_constraint(rows, pltpu.VMEM))
        out_specs.append(pl.BlockSpec(memory_space=pl.ANY))
        out_shape.append(jax.ShapeDtypeStruct(rows.shape, rows.dtype))
        aliases = {len(args) + idx: idx for idx in range(6)}
        in_specs += [pl.BlockSpec(memory_space=pl.ANY)] * 6
        args += list(made)
    return pl.pallas_call(
        functools.partial(update_kernel, len(in_specs) - 2),
        out_shape=tuple(out_shape),
        grid_spec=pltpu.PrefetchScalarGridSpec(num_scalar_prefetch=1, grid=(steps,), in_specs=in_specs, out_specs=tuple(out_specs),
                                              scratch_shapes=[pltpu.SemaphoreType.DMA((FINAL_STEPS,))] if made else []),
        input_output_aliases=aliases,
        compiler_params=pltpu.CompilerParams(vmem_limit_bytes=(28 if made else 62) * 2 ** 20),
        cost_estimate=pl.CostEstimate(flops=30 * 2 ** 20, bytes_accessed=30 * 2 ** 20, transcendentals=0),
        name='far_update' if made else 'near_update',
    )(*args)


def backward_kernel(limit_ref, rate_ref, act_ref, dout_ref, w1_ref, w2_ref, m1_ref, m2_ref, v1_ref, v2_ref, acc1_ref, acc2_ref,
                    g1_ref, g2_ref, clip_ref, b1_ref, b2_ref,
                    actv, grad, w1v, w2v, hid, slope, dpre, sent, accv, inbox,
                    norms, lsem, hsem, asem, csend, crecv, rsend, rrecv, nsend, nrecv):
    stage = lax.axis_index('stage')
    rep = lax.axis_index('data')
    far = 1 - rep
    n_rows, dim = actv.shape
    width = w1v.shape[1]
    n_chunks = n_rows // ROWS
    last = 3
    half1 = dim // 2
    half2 = width // 2
    n_parts = inbox.shape[0]
    n_cols = width // PART

    def chunk(idx):
        return pl.ds(pl.multiple_of(idx * ROWS, ROWS), ROWS)

    def peer(**where):
        return dict(device_id=where, device_id_type=pl.DeviceIdType.MESH)

    loads = [pltpu.make_async_copy(w1_ref, slope.at[2 * dim:3 * dim, :], lsem.at[0]), pltpu.make_async_copy(act_ref, actv, lsem.at[1])]
    loads += [pltpu.make_async_copy(w2_ref.at[idx * dim:(idx + 1) * dim, :], slope.at[3 * dim:4 * dim, idx * dim:(idx + 1) * dim], lsem.at[2 + idx]) for idx in range(4)]
    for copy in loads:
        copy.start()
    top = pltpu.make_async_copy(dout_ref, grad, lsem.at[6])

    @pl.when(stage == last)
    def _():
        top.start()

    def load_acc(idx, side, step):
        slot = step % accv.shape[0]
        if idx < n_cols:
            src = acc1_ref.at[pl.ds(pl.multiple_of(side * half1, half1), half1), pl.ds(idx * PART, PART)]
        else:
            src = acc2_ref.at[pl.ds(pl.multiple_of(side * half2 + (idx - n_cols) * half1, half1), half1), :]
        return pltpu.make_async_copy(src, accv.at[slot], asem.at[slot])

    steps = [(idx, far) for idx in range(n_parts)] + [(idx, rep) for idx in range(n_parts)]
    ahead = accv.shape[0]
    for step in range(ahead):
        load_acc(*steps[step], step).start()

    barrier = pltpu.get_barrier_semaphore()
    place = rep * 4 + stage
    others = [(place + hop) % 8 for hop in range(1, 8)]
    for other in others:
        pl.semaphore_signal(barrier, inc=1, **peer(data=other // 4, stage=other % 4))
    pl.semaphore_wait(barrier, 7)

    def hop(idx):
        return pltpu.make_async_remote_copy(src_ref=sent.at[chunk(idx)], dst_ref=grad.at[chunk(idx)], send_sem=csend.at[idx], recv_sem=crecv.at[idx],
                                            **peer(stage=(stage + 3) % 4))

    def prepare(idx):
        act = actv[chunk(idx), :]
        for first in range(0, width, COLS):
            cols = slice(first, first + COLS)
            z = jnp.dot(act, w1v[:, cols], preferred_element_type=jnp.float32)
            sq = z * z
            th = jnp.tanh(z * (0.7978845608028654 + 0.035677408136300125 * sq))
            gate = 0.5 + 0.5 * th
            hid[chunk(idx), cols] = (z * gate).astype(jnp.bfloat16)
            slope[chunk(idx), cols] = gate + (0.5 * z) * (1.0 - th * th) * (0.7978845608028654 + 0.10703222440890037 * sq)

    def descend(idx):
        grad_rows = grad[chunk(idx), :]
        total = None
        for first in range(0, width, COLS):
            cols = slice(first, first + COLS)
            d_hid = lax.dot_general(grad_rows, w2v[cols, :], TRANS_DIMS, preferred_element_type=jnp.float32)
            d_pre = (slope[chunk(idx), cols] * d_hid).astype(jnp.bfloat16)
            dpre[chunk(idx), cols] = d_pre
            part = lax.dot_general(d_pre, w1v[:, cols], TRANS_DIMS, preferred_element_type=jnp.float32)
            total = part if first == 0 else total + part
        sent[chunk(idx), :] = (grad_rows.astype(jnp.float32) + total).astype(jnp.bfloat16)

    loads[0].wait()

    @pl.loop(0, dim // 64)
    def _(idx):
        span = pl.ds(pl.multiple_of(idx * 64, 64), 64)
        w1v[span, :] = slope[pl.ds(pl.multiple_of(2 * dim + idx * 64, 64), 64), :].astype(jnp.bfloat16)

    loads[1].wait()
    prepare(0)
    for copy in loads[2:]:
        copy.wait()

    @pl.loop(0, dim // 64)
    def _(idx):
        for group in range(4):
            span = pl.ds(pl.multiple_of(group * dim + idx * 64, 64), 64)
            w2v[span, :] = slope[pl.ds(pl.multiple_of(3 * dim + idx * 64, 64), 64), group * dim:(group + 1) * dim].astype(jnp.bfloat16)

    @pl.when(stage == last)
    def _():
        top.wait()

    @pl.loop(0, n_chunks)
    def _(idx):
        @pl.when(stage < last)
        def _():
            hop(idx).wait_recv()

        descend(idx)

        @pl.when(stage > 0)
        def _():
            hop(idx).start()

        @pl.when(idx + 1 < n_chunks)
        def _():
            prepare(idx + 1)

    near = []
    for idx, ref in enumerate((w1_ref, m1_ref, v1_ref)):
        near.append(pltpu.make_async_copy(ref.at[pl.ds(pl.multiple_of(rep * half1, half1), half1), :], slope.at[dim + idx * half1:dim + (idx + 1) * half1, :], hsem.at[len(near)]))
    for idx, ref in enumerate((w2_ref, m2_ref, v2_ref)):
        for group in range(4):
            near.append(pltpu.make_async_copy(ref.at[pl.ds(pl.multiple_of(rep * half2 + group * half1, half1), half1), :],
                                              slope.at[dim + (3 + idx) * half1:dim + (4 + idx) * half1, group * dim:(group + 1) * dim], hsem.at[len(near)]))
    for copy in near:
        copy.start()

    def weight_grad(idx, side):
        if idx < n_cols:
            left = actv[:, pl.ds(pl.multiple_of(side * half1, half1), half1)]
            right = dpre[:, idx * PART:(idx + 1) * PART]
        else:
            left = hid[:, pl.ds(pl.multiple_of(side * half2 + (idx - n_cols) * half1, half1), half1)]
            right = grad[...]
        return lax.dot_general(left, right, FIRST_DIMS, preferred_element_type=jnp.float32)

    def own_part(idx):
        if idx < n_cols:
            return g1_ref, (slice(None), slice(idx * PART, (idx + 1) * PART))
        return g2_ref, (slice((idx - n_cols) * half1, (idx - n_cols + 1) * half1), slice(None))

    def outbox(idx):
        return slope.at[pl.ds((idx // n_cols) * half1, half1), pl.ds((idx % n_cols) * PART, PART)]

    def post(idx):
        return pltpu.make_async_remote_copy(src_ref=outbox(idx), dst_ref=inbox.at[idx], send_sem=rsend.at[idx], recv_sem=rrecv.at[idx], **peer(data=far))

    for step, (idx, side) in enumerate(steps):
        load_acc(idx, side, step).wait()
        value = accv[step % ahead] + weight_grad(idx, side)
        if step < n_parts:
            outbox(idx)[...] = value
            post(idx).start()
        else:
            ref, where = own_part(idx)
            ref[where] = value
        if step + ahead < len(steps):
            load_acc(*steps[step + ahead], step + ahead).start()

    squares = jnp.zeros((8, PART), jnp.float32)
    for idx in range(n_parts):
        post(idx).wait_recv()
        ref, where = own_part(idx)
        mean = 0.5 * (ref[where] + inbox[idx])
        ref[where] = mean
        squares = squares + jnp.sum((mean * mean).reshape(half1 // 8, 8, PART), axis=0)
    norms[place] = squares

    def tell(idx):
        return pltpu.make_async_remote_copy(src_ref=norms.at[place], dst_ref=norms.at[place], send_sem=nsend.at[idx], recv_sem=nrecv.at[place],
                                            **peer(data=others[idx] // 4, stage=others[idx] % 4))

    def hear(idx):
        ref = norms.at[others[idx]]
        return pltpu.make_async_remote_copy(src_ref=ref, dst_ref=ref, send_sem=nsend.at[idx], recv_sem=nrecv.at[others[idx]],
                                            **peer(data=others[idx] // 4, stage=others[idx] % 4))

    for idx in range(7):
        tell(idx).start()
    for idx in range(7):
        hear(idx).wait_recv()
    total = norms[0]
    for idx in range(1, 8):
        total = total + norms[idx]
    total = jnp.sum(jnp.sum(total, axis=0, keepdims=True), axis=1, keepdims=True)
    clip = jnp.minimum(1.0, limit_ref[0] / (jnp.sqrt(total) + NORM_EPS))
    clip_ref[...] = jnp.broadcast_to(clip, clip_ref.shape)
    for copy in near:
        copy.wait()

    @pl.loop(0, half1 // ADAM_ROWS)
    def _(idx):
        def from_slope(which, cols):
            return slope[pl.ds(pl.multiple_of(dim + which * half1 + idx * ADAM_ROWS, ADAM_ROWS), ADAM_ROWS), cols]

        coef = clip_ref[0:1, 0:1]
        span = pl.ds(pl.multiple_of(idx * ADAM_ROWS, ADAM_ROWS), ADAM_ROWS)
        every = slice(0, width)
        new_w, _, _ = adamw_rows(coef, rate_ref[0], from_slope(0, every), from_slope(1, every), from_slope(2, every), g1_ref[span, :])
        b1_ref[span, :] = (0.5 * new_w).astype(jnp.bfloat16)
        for group in range(4):
            cols = slice(group * dim, (group + 1) * dim)
            span = pl.ds(pl.multiple_of(group * half1 + idx * ADAM_ROWS, ADAM_ROWS), ADAM_ROWS)
            new_w, _, _ = adamw_rows(coef, rate_ref[0], from_slope(3, cols), from_slope(4, cols), from_slope(5, cols), g2_ref[span, :])
            b2_ref[span, :] = new_w.astype(jnp.bfloat16)

    for idx in range(7):
        tell(idx).wait_send()
    for idx in range(n_parts):
        post(idx).wait_send()

    @pl.when(stage > 0)
    def _():
        @pl.loop(0, n_chunks)
        def _(idx):
            hop(idx).wait_send()


def backward_all(limit, rate, act, d_out, first, second, acc_first, acc_second):
    n_rows, dim = act.shape
    width = first[0].shape[1]
    half1 = dim // 2
    n_chunks = n_rows // ROWS
    n_parts = 2 * (width // PART)
    dma = pltpu.SemaphoreType.DMA
    bf16, f32 = jnp.bfloat16, jnp.float32
    vmem = pl.BlockSpec(memory_space=pltpu.VMEM)
    return pl.pallas_call(
        backward_kernel,
        out_shape=(jax.ShapeDtypeStruct((half1, width), f32), jax.ShapeDtypeStruct((width // 2, dim), f32), jax.ShapeDtypeStruct((8, 128), f32),
                   jax.ShapeDtypeStruct((half1, width), bf16), jax.ShapeDtypeStruct((width // 2, dim), bf16)),
        in_specs=[pl.BlockSpec(memory_space=pltpu.SMEM)] * 2 + [pl.BlockSpec(memory_space=pl.ANY)] * 10,
        out_specs=(vmem,) * 5,
        scratch_shapes=[
            pltpu.VMEM((n_rows, dim), bf16), pltpu.VMEM((n_rows, dim), bf16),
            pltpu.VMEM((dim, width), bf16), pltpu.VMEM((width, dim), bf16),
            pltpu.VMEM((n_rows, width), bf16), pltpu.VMEM((n_rows, width), f32), pltpu.VMEM((n_rows, width), bf16),
            pltpu.VMEM((n_rows, dim), bf16), pltpu.VMEM((4, half1, PART), f32), pltpu.VMEM((n_parts, half1, PART), f32), pltpu.VMEM((8, 8, PART), f32),
            dma((7,)), dma((15,)), dma((4,)), dma((n_chunks,)), dma((n_chunks,)), dma((n_parts,)), dma((n_parts,)), dma((7,)), dma((8,)),
        ],
        compiler_params=pltpu.CompilerParams(collective_id=1, has_side_effects=True, vmem_limit_bytes=63 * 2 ** 20),
        cost_estimate=pl.CostEstimate(flops=10 * n_rows * dim * width, bytes_accessed=40 * 2 ** 20, transcendentals=0),
        name='backward_all',
    )(limit, rate, act, d_out, first[0], second[0], first[1], second[1], first[2], second[2], acc_first, acc_second)


def solution(mesh):
    n_stage = mesh.shape['stage']
    w_spec = P('stage', None, None)
    acc_spec = P('data', 'stage', None, None)
    row_spec = P(None, 'data', None)

    def stage_program(w_in, w_out, mom_in, mom_out, var_in, var_out, acc_in, acc_out, stage_acts, d_out, next_x, learn_rate, max_norm):
        rep_idx = lax.axis_index('data')
        first = (w_in[0], mom_in[0], var_in[0])
        second = (w_out[0], mom_out[0], var_out[0])
        near_first, near_second, clip, half_first, half_second = backward_all(
            max_norm, learn_rate, stage_acts[0], d_out, first, second, acc_in[0, 0], acc_out[0, 0])
        own = (half_first, half_second)
        chip = tuple(lax.ppermute(arr, 'stage', [(src, (src + 2) % 4) for src in range(4)]) for arr in own)
        twin = tuple(lax.ppermute(arr, 'data', [(0, 1), (1, 0)]) for arr in own)
        near = half_update(rep_idx.reshape(1), learn_rate, clip, first, second, (near_first, near_second))
        n_micro, n_rows, dim = next_x.shape
        rows, far_first, far_second = forward_all(next_x.reshape(n_micro * n_rows, dim), own, chip, twin, near_first, near_second, n_stage, SHARED)
        *news, next_y = half_update((1 - rep_idx).reshape(1), learn_rate, clip, first, second, (far_first, far_second), near, rows)
        return (news[0][None], news[3][None], news[1][None], news[4][None], news[2][None], news[5][None], next_y.reshape(next_x.shape))

    return jax.shard_map(stage_program, mesh=mesh, in_specs=(w_spec, w_spec, w_spec, w_spec, w_spec, w_spec, acc_spec, acc_spec, P('stage', 'data', None), P('data', None), row_spec, P(None), P(None)), out_specs=(w_spec, w_spec, w_spec, w_spec, w_spec, w_spec, row_spec), check_vma=False)
```

```python
import functools

import jax
import jax.numpy as jnp
from jax import lax
from jax.experimental import pallas as pl
from jax.experimental.pallas import tpu as pltpu
from jax.sharding import PartitionSpec as P

BETA_ONE = 0.9
BETA_TWO = 0.95
ADAM_EPS = 1e-8
WEIGHT_DECAY = 0.1
STEP_COUNT = 10
NORM_EPS = 1e-6
TRANS_DIMS = (((1,), (1,)), ((), ()))
FIRST_DIMS = (((0,), (0,)), ((), ()))
TILE = 512
CHUNK = 512
BEHIND = 3
FORWARD_VMEM = 30
LAG = 4
PRE = 4
SHARED = 3
OWN_TILES = (15, 15, 14, 14)
UPDATE_STEPS = 8
FINAL_STEPS = 16
ADAM_ROWS = 32
ROWS = 256
PART = 512
COLS = 512


def gelu_of_half(half):
    return half + half * jnp.tanh(half * (1.5957691216057308 + 0.28541926509040104 * (half * half)))


def forward_kernel(n_low, n_high, n_both, x_ref, w1_ref, w2_ref, xw1_ref, xw2_ref, rw1_ref, rw2_ref, g1_ref, g2_ref, y_ref, far1_ref, far2_ref,
                   xv, pv, w1v, w2v, xsem, psem, lsem, csend, asend, rsend, crecv, arecv, rrecv, wsend, wrecv, fsend, frecv):
    stage = lax.axis_index('stage')
    rep = lax.axis_index('data')
    far = 1 - rep
    core = stage % 2
    partner = stage + 1 - 2 * core
    across = (stage + 2) % 4
    corner = (partner + 2) % 4
    early = stage < 2
    mine, theirs = jnp.where(early, n_low, n_high), jnp.where(early, n_high, n_low)
    n_tiles = mine + n_both
    n_blocks, dim, width = w1v.shape
    half1, half2 = dim // 2, width // 2
    to_core, to_chip, to_rep = {'stage': partner}, {'stage': across}, {'data': far}

    def rows(owner, tile):
        count = jnp.where(owner < 2, n_low, n_high)
        base = jnp.where(owner < 2, owner * n_low, 2 * n_low + (owner - 2) * n_high)
        place = jnp.where(tile < count, base + tile, 2 * (n_low + n_high) + (owner % 2) * n_both + tile - count)
        return pl.ds(pl.multiple_of(place * TILE, TILE), TILE)

    def remote(src, dst, send, recv, target):
        return pltpu.make_async_remote_copy(src_ref=src, dst_ref=dst, send_sem=send, recv_sem=recv, device_id=target, device_id_type=pl.DeviceIdType.MESH)

    def load_x(tile):
        return pltpu.make_async_copy(x_ref.at[rows(stage, tile)], xv.at[tile % 2], xsem.at[tile % 2])

    def load_p(tile):
        return pltpu.make_async_copy(x_ref.at[rows(stage, tile)], pv.at[tile], psem.at[tile])

    def part(owner, block, kind):
        if kind == 0:
            return w1v.at[block, pl.ds(pl.multiple_of(owner * half1, half1), half1), :]
        return w2v.at[block, pl.ds(pl.multiple_of(owner * half2, half2), half2), :]

    def move(owner, block, kind, target, lane):
        ref = part(owner, block, kind)
        return remote(ref, ref, wsend.at[lane], wrecv.at[(owner * n_blocks + block) * 2 + kind], target)

    def arrive(owner, block, kind):
        move(owner, block, kind, to_core, 0).wait_recv()

    fetched = {}
    for lane, (where, kind, ref) in enumerate((('chip', 0, xw1_ref), ('rep', 1, rw2_ref), ('rep', 0, rw1_ref), ('chip', 1, xw2_ref), ('own', 0, w1_ref), ('own', 1, w2_ref))):
        owner, block = {'own': (rep, stage), 'chip': (rep, across), 'rep': (far, stage)}[where]
        fetched[where, kind] = pltpu.make_async_copy(ref, part(owner, block, kind), lsem.at[lane])
        fetched[where, kind].start()

    @pl.when(early)
    def _():
        for tile in range(PRE):
            load_p(tile).start()

    @pl.when(stage >= 2)
    def _():
        load_x(0).start()

    barrier = pltpu.get_barrier_semaphore()
    for target in (to_core, to_chip, to_rep):
        pl.semaphore_signal(barrier, inc=1, device_id=target, device_id_type=pl.DeviceIdType.MESH)
    pl.semaphore_wait(barrier, 3)

    sends = []

    def send(owner, block, kind, target):
        copy = move(owner, block, kind, target, len(sends))
        sends.append(copy)
        copy.start()

    fetched['chip', 0].wait()
    send(rep, across, 0, to_rep)
    fetched['rep', 1].wait()
    send(far, stage, 1, to_chip)
    for kind in (0, 1):
        fetched['own', kind].wait()
        send(rep, stage, kind, to_core)
    fetched['rep', 0].wait()
    for kind in (0, 1):
        send(far, stage, kind, to_core)
    fetched['chip', 1].wait()
    for kind in (0, 1):
        send(rep, across, kind, to_core)
    for owner in (rep, far):
        for kind in (0, 1):
            arrive(owner, partner, kind)

    def block_step(src, block, dst):
        half = TILE // 2
        pieces = [(side, first) for first in range(0, width, CHUNK) for side in (0, 1)]
        x_rows = [src[side * half:(side + 1) * half, :] for side in (0, 1)]
        total = [None, None]
        act_h = {}
        for turn in range(len(pieces) + BEHIND):
            if turn < len(pieces):
                side, first = pieces[turn]
                halved = jnp.dot(x_rows[side], w1v[block, :, first:first + CHUNK], preferred_element_type=jnp.float32)
                act_h[turn] = gelu_of_half(halved).astype(jnp.bfloat16)
            if turn >= BEHIND:
                side, first = pieces[turn - BEHIND]
                piece = jnp.dot(act_h.pop(turn - BEHIND), w2v[block, first:first + CHUNK, :], preferred_element_type=jnp.float32)
                total[side] = piece if first == 0 else total[side] + piece
        for side in (0, 1):
            dst[side * half:(side + 1) * half, :] = (x_rows[side].astype(jnp.float32) + total[side]).astype(jnp.bfloat16)

    @pl.when(early)
    def _():
        @pl.loop(0, PRE)
        def _(tile):
            load_p(tile).wait()

            @pl.loop(0, 2)
            def _(block):
                block_step(pv.at[tile], block, pv.at[tile])

    for kind in (0, 1):
        arrive(far, across, kind)
        send(far, across, kind, to_core)
    swaps = [remote(src, dst, fsend.at[idx], frecv.at[idx], to_rep) for idx, (src, dst) in enumerate(((g1_ref, far1_ref), (g2_ref, far2_ref)))]
    for copy in swaps:
        copy.start()
    for owner in (rep, far):
        for kind in (0, 1):
            arrive(owner, corner, kind)

    def give(tile, send, recv, target):
        ref = y_ref.at[rows(stage, tile)]
        return remote(ref, ref, send.at[tile], recv.at[tile], target)

    def give_core(tile):
        return give(tile, csend, crecv, to_core)

    def give_chip(tile):
        return give(tile, asend, arecv, to_chip)

    def pass_on(tile):
        ref = y_ref.at[rows(across, tile)]
        return remote(ref, ref, rsend.at[tile], rrecv.at[tile], to_core)

    def relay(tile):
        ref = y_ref.at[rows(across, tile)]
        remote(ref, ref, asend.at[0], arecv.at[tile], to_chip).wait_recv()
        pass_on(tile).start()

    @pl.loop(0, n_tiles)
    def _(tile):
        skip = jnp.where(early, PRE, 0)

        @pl.when(tile < skip)
        def _():
            xv[tile % 2] = pv[tile % PRE]

        @pl.when(tile >= skip)
        def _():
            load_x(tile).wait()

        @pl.when((tile + 1 >= skip) & (tile + 1 < n_tiles))
        def _():
            load_x(tile + 1).start()

        @pl.loop(0, n_blocks)
        def _(block):
            @pl.when((block >= 2) | (tile >= skip))
            def _():
                block_step(xv.at[tile % 2], block, xv.at[tile % 2])

        y_ref[rows(stage, tile), :] = xv[tile % 2]
        give_core(tile).start()

        @pl.when(tile < mine)
        def _():
            give_chip(tile).start()

        @pl.when((tile >= LAG) & (tile < LAG + theirs))
        def _():
            relay(tile - LAG)

    @pl.loop(n_tiles - LAG, theirs)
    def _(tile):
        relay(tile)

    @pl.loop(0, n_tiles)
    def _(tile):
        ref = y_ref.at[rows(partner, tile)]
        remote(ref, ref, csend.at[0], crecv.at[tile], to_core).wait_recv()
        give_core(tile).wait_send()

    @pl.loop(0, theirs)
    def _(tile):
        ref = y_ref.at[rows(corner, tile)]
        remote(ref, ref, rsend.at[0], rrecv.at[tile], to_core).wait_recv()
        pass_on(tile).wait_send()

    @pl.loop(0, mine)
    def _(tile):
        give_chip(tile).wait_send()

    for copy in sends:
        copy.wait_send()
    for copy in swaps:
        copy.wait()


def forward_all(x_rows, own, chip, twin, near_first, near_second, n_stage, n_both):
    n_rows, dim = x_rows.shape
    width = own[0].shape[1]
    n_own = max(OWN_TILES)
    n_tiles = n_own + n_both
    assert TILE * (sum(OWN_TILES) + 2 * n_both) == n_rows
    dma = pltpu.SemaphoreType.DMA
    flops = 4 * n_tiles * TILE * dim * width * n_stage
    return pl.pallas_call(
        functools.partial(forward_kernel, OWN_TILES[0], OWN_TILES[2], n_both),
        out_shape=(pltpu.VMEM((n_rows, dim), jnp.bfloat16), jax.ShapeDtypeStruct(near_first.shape, jnp.float32), jax.ShapeDtypeStruct(near_second.shape, jnp.float32)),
        in_specs=[pl.BlockSpec(memory_space=pl.ANY)] * 9,
        out_specs=(pl.BlockSpec(memory_space=pltpu.VMEM),) + (pl.BlockSpec(memory_space=pl.ANY),) * 2,
        scratch_shapes=[
            pltpu.VMEM((2, TILE, dim), jnp.bfloat16),
            pltpu.VMEM((PRE, TILE, dim), jnp.bfloat16),
            pltpu.VMEM((n_stage, dim, width), jnp.bfloat16),
            pltpu.VMEM((n_stage, width, dim), jnp.bfloat16),
            dma((2,)), dma((PRE,)), dma((6,)), dma((n_tiles,)), dma((n_own,)), dma((n_own,)),
            dma((n_tiles,)), dma((n_own,)), dma((n_own,)), dma((10,)), dma((4 * n_stage,)), dma((2,)), dma((2,)),
        ],
        compiler_params=pltpu.CompilerParams(collective_id=0, has_side_effects=True, vmem_limit_bytes=FORWARD_VMEM * 2 ** 20),
        cost_estimate=pl.CostEstimate(flops=flops, bytes_accessed=2 * n_rows * dim * 2, transcendentals=0),
        name='forward_all',
    )(x_rows, *own, *chip, *twin, near_first, near_second)


def adamw_rows(coef, rate, param, moment, second, grad_val):
    scaled = coef * grad_val
    mom_new = BETA_ONE * moment + (1.0 - BETA_ONE) * scaled
    sec_new = BETA_TWO * second + (1.0 - BETA_TWO) * scaled * scaled
    mom_hat = mom_new * (1.0 / (1.0 - BETA_ONE ** STEP_COUNT))
    sec_hat = sec_new * (1.0 / (1.0 - BETA_TWO ** STEP_COUNT))
    return param - rate * (mom_hat / (jnp.sqrt(sec_hat) + ADAM_EPS) + WEIGHT_DECAY * param), mom_new, sec_new


def update_kernel(n_ins, half_ref, rate_ref, clip_ref, *refs):
    outs = refs[n_ins:]
    if len(outs) == 8:
        step, steps = pl.program_id(0), pl.num_programs(0)

        def drain(idx):
            size = outs[6].shape[0] // FINAL_STEPS
            span = pl.ds(pl.multiple_of(idx * size, size), size)
            return pltpu.make_async_copy(refs[8].at[span], outs[6].at[span], outs[7].at[idx])

        drain(step).start()

    for side in (0, 1):
        param, moment, second, grad_val = (ref[...] for ref in refs[4 * side:4 * side + 4])
        news = adamw_rows(clip_ref[0:1, 0:1], rate_ref[0], param, moment, second, grad_val)
        for ref, new in zip(outs[3 * side:3 * side + 3], news):
            ref[...] = new
    if len(outs) == 8:
        @pl.when(step == steps - 1)
        def _():
            for idx in range(FINAL_STEPS):
                drain(idx).wait()


def half_update(half_idx, rate, clip, first, second, grads, made=(), rows=None):
    steps = FINAL_STEPS if made else UPDATE_STEPS
    full, out_specs, out_shape = [], [], []
    for arr, grad in zip((first[0], second[0]), grads):
        block = (grad.shape[0] // steps, grad.shape[1])
        picked = pl.BlockSpec(block, lambda step, half: (half[0] * steps + step, 0))
        full += [picked] * 3 + [pl.BlockSpec(block, lambda step, half: (step, 0))]
        out_specs += [picked] * 3
        out_shape += [jax.ShapeDtypeStruct(arr.shape, jnp.float32)] * 3
    in_specs = [pl.BlockSpec(memory_space=pltpu.SMEM), pl.BlockSpec(clip.shape, lambda step, half: (0, 0))] + full
    args = [half_idx, rate, clip, *first, grads[0], *second, grads[1]]
    aliases = {}
    if made:
        in_specs.append(pl.BlockSpec(memory_space=pl.ANY))
        args.append(pltpu.with_memory_space_constraint(rows, pltpu.VMEM))
        out_specs.append(pl.BlockSpec(memory_space=pl.ANY))
        out_shape.append(jax.ShapeDtypeStruct(rows.shape, rows.dtype))
        aliases = {len(args) + idx: idx for idx in range(6)}
        in_specs += [pl.BlockSpec(memory_space=pl.ANY)] * 6
        args += list(made)
    return pl.pallas_call(
        functools.partial(update_kernel, len(in_specs) - 2),
        out_shape=tuple(out_shape),
        grid_spec=pltpu.PrefetchScalarGridSpec(num_scalar_prefetch=1, grid=(steps,), in_specs=in_specs, out_specs=tuple(out_specs),
                                              scratch_shapes=[pltpu.SemaphoreType.DMA((FINAL_STEPS,))] if made else []),
        input_output_aliases=aliases,
        compiler_params=pltpu.CompilerParams(vmem_limit_bytes=(28 if made else 62) * 2 ** 20),
        cost_estimate=pl.CostEstimate(flops=30 * 2 ** 20, bytes_accessed=30 * 2 ** 20, transcendentals=0),
        name='far_update' if made else 'near_update',
    )(*args)


def backward_kernel(limit_ref, rate_ref, act_ref, dout_ref, w1_ref, w2_ref, m1_ref, m2_ref, v1_ref, v2_ref, acc1_ref, acc2_ref,
                    g1_ref, g2_ref, clip_ref, b1_ref, b2_ref,
                    actv, grad, w1v, w2v, hid, slope, dpre, sent, accv, inbox,
                    norms, lsem, hsem, asem, csend, crecv, rsend, rrecv, nsend, nrecv):
    stage = lax.axis_index('stage')
    rep = lax.axis_index('data')
    far = 1 - rep
    n_rows, dim = actv.shape
    width = w1v.shape[1]
    n_chunks = n_rows // ROWS
    last = 3
    half1 = dim // 2
    half2 = width // 2
    n_parts = inbox.shape[0]
    n_cols = width // PART

    def chunk(idx):
        return pl.ds(pl.multiple_of(idx * ROWS, ROWS), ROWS)

    def peer(**where):
        return dict(device_id=where, device_id_type=pl.DeviceIdType.MESH)

    loads = [pltpu.make_async_copy(w1_ref, slope.at[2 * dim:3 * dim, :], lsem.at[0]), pltpu.make_async_copy(act_ref, actv, lsem.at[1])]
    loads += [pltpu.make_async_copy(w2_ref.at[idx * dim:(idx + 1) * dim, :], slope.at[3 * dim:4 * dim, idx * dim:(idx + 1) * dim], lsem.at[2 + idx]) for idx in range(4)]
    for copy in loads:
        copy.start()
    top = pltpu.make_async_copy(dout_ref, grad, lsem.at[6])

    @pl.when(stage == last)
    def _():
        top.start()

    def load_acc(idx, side, step):
        slot = step % accv.shape[0]
        if idx < n_cols:
            src = acc1_ref.at[pl.ds(pl.multiple_of(side * half1, half1), half1), pl.ds(idx * PART, PART)]
        else:
            src = acc2_ref.at[pl.ds(pl.multiple_of(side * half2 + (idx - n_cols) * half1, half1), half1), :]
        return pltpu.make_async_copy(src, accv.at[slot], asem.at[slot])

    steps = [(idx, far) for idx in range(n_parts)] + [(idx, rep) for idx in range(n_parts)]
    ahead = accv.shape[0]
    for step in range(ahead):
        load_acc(*steps[step], step).start()

    barrier = pltpu.get_barrier_semaphore()
    place = rep * 4 + stage
    others = [(place + hop) % 8 for hop in range(1, 8)]
    for other in others:
        pl.semaphore_signal(barrier, inc=1, **peer(data=other // 4, stage=other % 4))
    pl.semaphore_wait(barrier, 7)

    def hop(idx):
        return pltpu.make_async_remote_copy(src_ref=sent.at[chunk(idx)], dst_ref=grad.at[chunk(idx)], send_sem=csend.at[idx], recv_sem=crecv.at[idx],
                                            **peer(stage=(stage + 3) % 4))

    def prepare(idx):
        act = actv[chunk(idx), :]
        for first in range(0, width, COLS):
            cols = slice(first, first + COLS)
            z = jnp.dot(act, w1v[:, cols], preferred_element_type=jnp.float32)
            sq = z * z
            th = jnp.tanh(z * (0.7978845608028654 + 0.035677408136300125 * sq))
            gate = 0.5 + 0.5 * th
            hid[chunk(idx), cols] = (z * gate).astype(jnp.bfloat16)
            slope[chunk(idx), cols] = gate + (0.5 * z) * (1.0 - th * th) * (0.7978845608028654 + 0.10703222440890037 * sq)

    def descend(idx):
        grad_rows = grad[chunk(idx), :]
        total = None
        for first in range(0, width, COLS):
            cols = slice(first, first + COLS)
            d_hid = lax.dot_general(grad_rows, w2v[cols, :], TRANS_DIMS, preferred_element_type=jnp.float32)
            d_pre = (slope[chunk(idx), cols] * d_hid).astype(jnp.bfloat16)
            dpre[chunk(idx), cols] = d_pre
            part = lax.dot_general(d_pre, w1v[:, cols], TRANS_DIMS, preferred_element_type=jnp.float32)
            total = part if first == 0 else total + part
        sent[chunk(idx), :] = (grad_rows.astype(jnp.float32) + total).astype(jnp.bfloat16)

    loads[0].wait()

    @pl.loop(0, dim // 64)
    def _(idx):
        span = pl.ds(pl.multiple_of(idx * 64, 64), 64)
        w1v[span, :] = slope[pl.ds(pl.multiple_of(2 * dim + idx * 64, 64), 64), :].astype(jnp.bfloat16)

    loads[1].wait()
    prepare(0)
    for copy in loads[2:]:
        copy.wait()

    @pl.loop(0, dim // 64)
    def _(idx):
        for group in range(4):
            span = pl.ds(pl.multiple_of(group * dim + idx * 64, 64), 64)
            w2v[span, :] = slope[pl.ds(pl.multiple_of(3 * dim + idx * 64, 64), 64), group * dim:(group + 1) * dim].astype(jnp.bfloat16)

    @pl.when(stage == last)
    def _():
        top.wait()

    @pl.loop(0, n_chunks)
    def _(idx):
        @pl.when(stage < last)
        def _():
            hop(idx).wait_recv()

        descend(idx)

        @pl.when(stage > 0)
        def _():
            hop(idx).start()

        @pl.when(idx + 1 < n_chunks)
        def _():
            prepare(idx + 1)

    near = []
    for idx, ref in enumerate((w1_ref, m1_ref, v1_ref)):
        near.append(pltpu.make_async_copy(ref.at[pl.ds(pl.multiple_of(rep * half1, half1), half1), :], slope.at[dim + idx * half1:dim + (idx + 1) * half1, :], hsem.at[len(near)]))
    for idx, ref in enumerate((w2_ref, m2_ref, v2_ref)):
        for group in range(4):
            near.append(pltpu.make_async_copy(ref.at[pl.ds(pl.multiple_of(rep * half2 + group * half1, half1), half1), :],
                                              slope.at[dim + (3 + idx) * half1:dim + (4 + idx) * half1, group * dim:(group + 1) * dim], hsem.at[len(near)]))
    for copy in near:
        copy.start()

    def weight_grad(idx, side):
        if idx < n_cols:
            left = actv[:, pl.ds(pl.multiple_of(side * half1, half1), half1)]
            right = dpre[:, idx * PART:(idx + 1) * PART]
        else:
            left = hid[:, pl.ds(pl.multiple_of(side * half2 + (idx - n_cols) * half1, half1), half1)]
            right = grad[...]
        return lax.dot_general(left, right, FIRST_DIMS, preferred_element_type=jnp.float32)

    def own_part(idx):
        if idx < n_cols:
            return g1_ref, (slice(None), slice(idx * PART, (idx + 1) * PART))
        return g2_ref, (slice((idx - n_cols) * half1, (idx - n_cols + 1) * half1), slice(None))

    def outbox(idx):
        return slope.at[pl.ds((idx // n_cols) * half1, half1), pl.ds((idx % n_cols) * PART, PART)]

    def post(idx):
        return pltpu.make_async_remote_copy(src_ref=outbox(idx), dst_ref=inbox.at[idx], send_sem=rsend.at[idx], recv_sem=rrecv.at[idx], **peer(data=far))

    for step, (idx, side) in enumerate(steps):
        load_acc(idx, side, step).wait()
        value = accv[step % ahead] + weight_grad(idx, side)
        if step < n_parts:
            outbox(idx)[...] = value
            post(idx).start()
        else:
            ref, where = own_part(idx)
            ref[where] = value
        if step + ahead < len(steps):
            load_acc(*steps[step + ahead], step + ahead).start()

    squares = jnp.zeros((8, PART), jnp.float32)
    for idx in range(n_parts):
        post(idx).wait_recv()
        ref, where = own_part(idx)
        mean = 0.5 * (ref[where] + inbox[idx])
        ref[where] = mean
        squares = squares + jnp.sum((mean * mean).reshape(half1 // 8, 8, PART), axis=0)
    norms[place] = squares

    def tell(idx):
        return pltpu.make_async_remote_copy(src_ref=norms.at[place], dst_ref=norms.at[place], send_sem=nsend.at[idx], recv_sem=nrecv.at[place],
                                            **peer(data=others[idx] // 4, stage=others[idx] % 4))

    def hear(idx):
        ref = norms.at[others[idx]]
        return pltpu.make_async_remote_copy(src_ref=ref, dst_ref=ref, send_sem=nsend.at[idx], recv_sem=nrecv.at[others[idx]],
                                            **peer(data=others[idx] // 4, stage=others[idx] % 4))

    for idx in range(7):
        tell(idx).start()
    for idx in range(7):
        hear(idx).wait_recv()
    total = norms[0]
    for idx in range(1, 8):
        total = total + norms[idx]
    total = jnp.sum(jnp.sum(total, axis=0, keepdims=True), axis=1, keepdims=True)
    clip = jnp.minimum(1.0, limit_ref[0] / (jnp.sqrt(total) + NORM_EPS))
    clip_ref[...] = jnp.broadcast_to(clip, clip_ref.shape)
    for copy in near:
        copy.wait()

    @pl.loop(0, half1 // ADAM_ROWS)
    def _(idx):
        def from_slope(which, cols):
            return slope[pl.ds(pl.multiple_of(dim + which * half1 + idx * ADAM_ROWS, ADAM_ROWS), ADAM_ROWS), cols]

        coef = clip_ref[0:1, 0:1]
        span = pl.ds(pl.multiple_of(idx * ADAM_ROWS, ADAM_ROWS), ADAM_ROWS)
        every = slice(0, width)
        new_w, _, _ = adamw_rows(coef, rate_ref[0], from_slope(0, every), from_slope(1, every), from_slope(2, every), g1_ref[span, :])
        b1_ref[span, :] = (0.5 * new_w).astype(jnp.bfloat16)
        for group in range(4):
            cols = slice(group * dim, (group + 1) * dim)
            span = pl.ds(pl.multiple_of(group * half1 + idx * ADAM_ROWS, ADAM_ROWS), ADAM_ROWS)
            new_w, _, _ = adamw_rows(coef, rate_ref[0], from_slope(3, cols), from_slope(4, cols), from_slope(5, cols), g2_ref[span, :])
            b2_ref[span, :] = new_w.astype(jnp.bfloat16)

    for idx in range(7):
        tell(idx).wait_send()
    for idx in range(n_parts):
        post(idx).wait_send()

    @pl.when(stage > 0)
    def _():
        @pl.loop(0, n_chunks)
        def _(idx):
            hop(idx).wait_send()


def backward_all(limit, rate, act, d_out, first, second, acc_first, acc_second):
    n_rows, dim = act.shape
    width = first[0].shape[1]
    half1 = dim // 2
    n_chunks = n_rows // ROWS
    n_parts = 2 * (width // PART)
    dma = pltpu.SemaphoreType.DMA
    bf16, f32 = jnp.bfloat16, jnp.float32
    vmem = pl.BlockSpec(memory_space=pltpu.VMEM)
    return pl.pallas_call(
        backward_kernel,
        out_shape=(jax.ShapeDtypeStruct((half1, width), f32), jax.ShapeDtypeStruct((width // 2, dim), f32), jax.ShapeDtypeStruct((8, 128), f32),
                   jax.ShapeDtypeStruct((half1, width), bf16), jax.ShapeDtypeStruct((width // 2, dim), bf16)),
        in_specs=[pl.BlockSpec(memory_space=pltpu.SMEM)] * 2 + [pl.BlockSpec(memory_space=pl.ANY)] * 10,
        out_specs=(vmem,) * 5,
        scratch_shapes=[
            pltpu.VMEM((n_rows, dim), bf16), pltpu.VMEM((n_rows, dim), bf16),
            pltpu.VMEM((dim, width), bf16), pltpu.VMEM((width, dim), bf16),
            pltpu.VMEM((n_rows, width), bf16), pltpu.VMEM((n_rows, width), f32), pltpu.VMEM((n_rows, width), bf16),
            pltpu.VMEM((n_rows, dim), bf16), pltpu.VMEM((4, half1, PART), f32), pltpu.VMEM((n_parts, half1, PART), f32), pltpu.VMEM((8, 8, PART), f32),
            dma((7,)), dma((15,)), dma((4,)), dma((n_chunks,)), dma((n_chunks,)), dma((n_parts,)), dma((n_parts,)), dma((7,)), dma((8,)),
        ],
        compiler_params=pltpu.CompilerParams(collective_id=1, has_side_effects=True, vmem_limit_bytes=63 * 2 ** 20),
        cost_estimate=pl.CostEstimate(flops=10 * n_rows * dim * width, bytes_accessed=40 * 2 ** 20, transcendentals=0),
        name='backward_all',
    )(limit, rate, act, d_out, first[0], second[0], first[1], second[1], first[2], second[2], acc_first, acc_second)


def solution(mesh):
    n_stage = mesh.shape['stage']
    w_spec = P('stage', None, None)
    acc_spec = P('data', 'stage', None, None)
    row_spec = P(None, 'data', None)

    def stage_program(w_in, w_out, mom_in, mom_out, var_in, var_out, acc_in, acc_out, stage_acts, d_out, next_x, learn_rate, max_norm):
        rep_idx = lax.axis_index('data')
        first = (w_in[0], mom_in[0], var_in[0])
        second = (w_out[0], mom_out[0], var_out[0])
        near_first, near_second, clip, half_first, half_second = backward_all(
            max_norm, learn_rate, stage_acts[0], d_out, first, second, acc_in[0, 0], acc_out[0, 0])
        own = (half_first, half_second)
        chip = tuple(lax.ppermute(arr, 'stage', [(src, (src + 2) % 4) for src in range(4)]) for arr in own)
        twin = tuple(lax.ppermute(arr, 'data', [(0, 1), (1, 0)]) for arr in own)
        near = half_update(rep_idx.reshape(1), learn_rate, clip, first, second, (near_first, near_second))
        n_micro, n_rows, dim = next_x.shape
        rows, far_first, far_second = forward_all(next_x.reshape(n_micro * n_rows, dim), own, chip, twin, near_first, near_second, n_stage, SHARED)
        *news, next_y = half_update((1 - rep_idx).reshape(1), learn_rate, clip, first, second, (far_first, far_second), near, rows)
        return (news[0][None], news[3][None], news[1][None], news[4][None], news[2][None], news[5][None], next_y.reshape(next_x.shape))

    return jax.shard_map(stage_program, mesh=mesh, in_specs=(w_spec, w_spec, w_spec, w_spec, w_spec, w_spec, acc_spec, acc_spec, P('stage', 'data', None), P('data', None), row_spec, P(None), P(None)), out_specs=(w_spec, w_spec, w_spec, w_spec, w_spec, w_spec, row_spec), check_vma=False)
```

```python
import functools

import jax
import jax.numpy as jnp
from jax import lax
from jax.experimental import pallas as pl
from jax.experimental.pallas import tpu as pltpu
from jax.sharding import PartitionSpec as P

BETA_ONE = 0.9
BETA_TWO = 0.95
ADAM_EPS = 1e-8
WEIGHT_DECAY = 0.1
STEP_COUNT = 10
NORM_EPS = 1e-6
TRANS_DIMS = (((1,), (1,)), ((), ()))
FIRST_DIMS = (((0,), (0,)), ((), ()))
TILE = 512
CHUNK = 512
BEHIND = 3
FORWARD_VMEM = 30
LAG = 5
PRE = 4
SHARED = 4
OWN_TILES = (14, 14, 14, 14)
UPDATE_STEPS = 8
FINAL_STEPS = 8
ADAM_ROWS = 32
ROWS = 256
PART = 512
COLS = 512


def gelu_of_half(half):
    return half + half * jnp.tanh(half * (1.5957691216057308 + 0.28541926509040104 * (half * half)))


def forward_kernel(n_low, n_high, n_both, x_ref, w1_ref, w2_ref, xw1_ref, xw2_ref, rw1_ref, rw2_ref, g1_ref, g2_ref, y_ref, far1_ref, far2_ref,
                   xv, pv, w1v, w2v, xsem, psem, lsem, csend, asend, rsend, crecv, arecv, rrecv, wsend, wrecv, fsend, frecv):
    stage = lax.axis_index('stage')
    rep = lax.axis_index('data')
    far = 1 - rep
    core = stage % 2
    partner = stage + 1 - 2 * core
    across = (stage + 2) % 4
    corner = (partner + 2) % 4
    early = stage < 2
    mine, theirs = jnp.where(early, n_low, n_high), jnp.where(early, n_high, n_low)
    n_tiles = mine + n_both
    n_blocks, dim, width = w1v.shape
    half1, half2 = dim // 2, width // 2
    to_core, to_chip, to_rep = {'stage': partner}, {'stage': across}, {'data': far}

    def rows(owner, tile):
        count = jnp.where(owner < 2, n_low, n_high)
        base = jnp.where(owner < 2, owner * n_low, 2 * n_low + (owner - 2) * n_high)
        place = jnp.where(tile < count, base + tile, 2 * (n_low + n_high) + (owner % 2) * n_both + tile - count)
        return pl.ds(pl.multiple_of(place * TILE, TILE), TILE)

    def remote(src, dst, send, recv, target):
        return pltpu.make_async_remote_copy(src_ref=src, dst_ref=dst, send_sem=send, recv_sem=recv, device_id=target, device_id_type=pl.DeviceIdType.MESH)

    def load_x(tile):
        return pltpu.make_async_copy(x_ref.at[rows(stage, tile)], xv.at[tile % 2], xsem.at[tile % 2])

    def load_p(tile):
        return pltpu.make_async_copy(x_ref.at[rows(stage, tile)], pv.at[tile], psem.at[tile])

    def part(owner, block, kind):
        if kind == 0:
            return w1v.at[block, pl.ds(pl.multiple_of(owner * half1, half1), half1), :]
        return w2v.at[block, pl.ds(pl.multiple_of(owner * half2, half2), half2), :]

    def move(owner, block, kind, target, lane):
        ref = part(owner, block, kind)
        return remote(ref, ref, wsend.at[lane], wrecv.at[(owner * n_blocks + block) * 2 + kind], target)

    def arrive(owner, block, kind):
        move(owner, block, kind, to_core, 0).wait_recv()

    fetched = {}
    for lane, (where, kind, ref) in enumerate((('chip', 0, xw1_ref), ('rep', 1, rw2_ref), ('rep', 0, rw1_ref), ('chip', 1, xw2_ref), ('own', 0, w1_ref), ('own', 1, w2_ref))):
        owner, block = {'own': (rep, stage), 'chip': (rep, across), 'rep': (far, stage)}[where]
        fetched[where, kind] = pltpu.make_async_copy(ref, part(owner, block, kind), lsem.at[lane])
        fetched[where, kind].start()

    @pl.when(early)
    def _():
        for tile in range(PRE):
            load_p(tile).start()

    @pl.when(stage >= 2)
    def _():
        load_x(0).start()

    barrier = pltpu.get_barrier_semaphore()
    for target in (to_core, to_chip, to_rep):
        pl.semaphore_signal(barrier, inc=1, device_id=target, device_id_type=pl.DeviceIdType.MESH)
    pl.semaphore_wait(barrier, 3)

    sends = []

    def send(owner, block, kind, target):
        copy = move(owner, block, kind, target, len(sends))
        sends.append(copy)
        copy.start()

    fetched['chip', 0].wait()
    send(rep, across, 0, to_rep)
    fetched['rep', 1].wait()
    send(far, stage, 1, to_chip)
    for kind in (0, 1):
        fetched['own', kind].wait()
        send(rep, stage, kind, to_core)
    fetched['rep', 0].wait()
    for kind in (0, 1):
        send(far, stage, kind, to_core)
    fetched['chip', 1].wait()
    for kind in (0, 1):
        send(rep, across, kind, to_core)
    for owner in (rep, far):
        for kind in (0, 1):
            arrive(owner, partner, kind)

    def two_blocks(ref, pair):
        half = TILE // 2
        pieces = [(side, first) for first in range(0, width, CHUNK) for side in (0, 1)]
        x_rows = [ref[side * half:(side + 1) * half, :] for side in (0, 1)]
        for block in (2 * pair, 2 * pair + 1):
            total = [None, None]
            act_h = {}
            for turn in range(len(pieces) + BEHIND):
                if turn < len(pieces):
                    side, first = pieces[turn]
                    halved = jnp.dot(x_rows[side], w1v[block, :, first:first + CHUNK], preferred_element_type=jnp.float32)
                    act_h[turn] = gelu_of_half(halved).astype(jnp.bfloat16)
                if turn >= BEHIND:
                    side, first = pieces[turn - BEHIND]
                    piece = jnp.dot(act_h.pop(turn - BEHIND), w2v[block, first:first + CHUNK, :], preferred_element_type=jnp.float32)
                    total[side] = piece if first == 0 else total[side] + piece
            x_rows = [(x_rows[side].astype(jnp.float32) + total[side]).astype(jnp.bfloat16) for side in (0, 1)]
        for side in (0, 1):
            ref[side * half:(side + 1) * half, :] = x_rows[side]

    @pl.when(early)
    def _():
        @pl.loop(0, PRE)
        def _(tile):
            load_p(tile).wait()

            two_blocks(pv.at[tile], 0)

    for kind in (0, 1):
        arrive(far, across, kind)
        send(far, across, kind, to_core)
    swaps = [remote(src, dst, fsend.at[idx], frecv.at[idx], to_rep) for idx, (src, dst) in enumerate(((g1_ref, far1_ref), (g2_ref, far2_ref)))]
    for copy in swaps:
        copy.start()
    for owner in (rep, far):
        for kind in (0, 1):
            arrive(owner, corner, kind)

    def give(tile, send, recv, target):
        ref = y_ref.at[rows(stage, tile)]
        return remote(ref, ref, send.at[tile], recv.at[tile], target)

    def give_core(tile):
        return give(tile, csend, crecv, to_core)

    def give_chip(tile):
        return give(tile, asend, arecv, to_chip)

    def pass_on(tile):
        ref = y_ref.at[rows(across, tile)]
        return remote(ref, ref, rsend.at[tile], rrecv.at[tile], to_core)

    def relay(tile):
        ref = y_ref.at[rows(across, tile)]
        remote(ref, ref, asend.at[0], arecv.at[tile], to_chip).wait_recv()
        pass_on(tile).start()

    @pl.loop(0, n_tiles)
    def _(tile):
        skip = jnp.where(early, PRE, 0)

        @pl.when(tile < skip)
        def _():
            xv[tile % 2] = pv[tile % PRE]

        @pl.when(tile >= skip)
        def _():
            load_x(tile).wait()

        @pl.when((tile + 1 >= skip) & (tile + 1 < n_tiles))
        def _():
            load_x(tile + 1).start()

        @pl.loop(0, n_blocks // 2)
        def _(pair):
            @pl.when((pair > 0) | (tile >= skip))
            def _():
                two_blocks(xv.at[tile % 2], pair)

        y_ref[rows(stage, tile), :] = xv[tile % 2]
        give_core(tile).start()

        @pl.when(tile < mine)
        def _():
            give_chip(tile).start()

        @pl.when((tile >= LAG) & (tile < LAG + theirs))
        def _():
            relay(tile - LAG)

    @pl.loop(n_tiles - LAG, theirs)
    def _(tile):
        relay(tile)

    @pl.loop(0, n_tiles)
    def _(tile):
        ref = y_ref.at[rows(partner, tile)]
        remote(ref, ref, csend.at[0], crecv.at[tile], to_core).wait_recv()
        give_core(tile).wait_send()

    @pl.loop(0, theirs)
    def _(tile):
        ref = y_ref.at[rows(corner, tile)]
        remote(ref, ref, rsend.at[0], rrecv.at[tile], to_core).wait_recv()
        pass_on(tile).wait_send()

    @pl.loop(0, mine)
    def _(tile):
        give_chip(tile).wait_send()

    for copy in sends:
        copy.wait_send()
    for copy in swaps:
        copy.wait()


def forward_all(x_rows, own, chip, twin, near_first, near_second, n_stage, n_both):
    n_rows, dim = x_rows.shape
    width = own[0].shape[1]
    n_own = max(OWN_TILES)
    n_tiles = n_own + n_both
    assert TILE * (sum(OWN_TILES) + 2 * n_both) == n_rows
    dma = pltpu.SemaphoreType.DMA
    flops = 4 * n_tiles * TILE * dim * width * n_stage
    return pl.pallas_call(
        functools.partial(forward_kernel, OWN_TILES[0], OWN_TILES[2], n_both),
        out_shape=(pltpu.VMEM((n_rows, dim), jnp.bfloat16), jax.ShapeDtypeStruct(near_first.shape, jnp.float32), jax.ShapeDtypeStruct(near_second.shape, jnp.float32)),
        in_specs=[pl.BlockSpec(memory_space=pl.ANY)] * 9,
        out_specs=(pl.BlockSpec(memory_space=pltpu.VMEM),) + (pl.BlockSpec(memory_space=pl.ANY),) * 2,
        scratch_shapes=[
            pltpu.VMEM((2, TILE, dim), jnp.bfloat16),
            pltpu.VMEM((PRE, TILE, dim), jnp.bfloat16),
            pltpu.VMEM((n_stage, dim, width), jnp.bfloat16),
            pltpu.VMEM((n_stage, width, dim), jnp.bfloat16),
            dma((2,)), dma((PRE,)), dma((6,)), dma((n_tiles,)), dma((n_own,)), dma((n_own,)),
            dma((n_tiles,)), dma((n_own,)), dma((n_own,)), dma((10,)), dma((4 * n_stage,)), dma((2,)), dma((2,)),
        ],
        compiler_params=pltpu.CompilerParams(collective_id=0, has_side_effects=True, vmem_limit_bytes=FORWARD_VMEM * 2 ** 20),
        cost_estimate=pl.CostEstimate(flops=flops, bytes_accessed=2 * n_rows * dim * 2, transcendentals=0),
        name='forward_all',
    )(x_rows, *own, *chip, *twin, near_first, near_second)


def adamw_rows(coef, rate, param, moment, second, grad_val):
    scaled = coef * grad_val
    mom_new = BETA_ONE * moment + (1.0 - BETA_ONE) * scaled
    sec_new = BETA_TWO * second + (1.0 - BETA_TWO) * scaled * scaled
    mom_hat = mom_new * (1.0 / (1.0 - BETA_ONE ** STEP_COUNT))
    sec_hat = sec_new * (1.0 / (1.0 - BETA_TWO ** STEP_COUNT))
    return param - rate * (mom_hat / (jnp.sqrt(sec_hat) + ADAM_EPS) + WEIGHT_DECAY * param), mom_new, sec_new


def update_kernel(n_ins, half_ref, rate_ref, clip_ref, *refs):
    outs = refs[n_ins:]
    if len(outs) == 8:
        step, steps = pl.program_id(0), pl.num_programs(0)

        def drain(idx):
            size = outs[6].shape[0] // FINAL_STEPS
            span = pl.ds(pl.multiple_of(idx * size, size), size)
            return pltpu.make_async_copy(refs[8].at[span], outs[6].at[span], outs[7].at[idx])

        drain(step).start()

    for side in (0, 1):
        param, moment, second, grad_val = (ref[...] for ref in refs[4 * side:4 * side + 4])
        news = adamw_rows(clip_ref[0:1, 0:1], rate_ref[0], param, moment, second, grad_val)
        for ref, new in zip(outs[3 * side:3 * side + 3], news):
            ref[...] = new
    if len(outs) == 8:
        @pl.when(step == steps - 1)
        def _():
            for idx in range(FINAL_STEPS):
                drain(idx).wait()


def half_update(half_idx, rate, clip, first, second, grads, made=(), rows=None):
    steps = FINAL_STEPS if made else UPDATE_STEPS
    full, out_specs, out_shape = [], [], []
    for arr, grad in zip((first[0], second[0]), grads):
        block = (grad.shape[0] // steps, grad.shape[1])
        picked = pl.BlockSpec(block, lambda step, half: (half[0] * steps + step, 0))
        full += [picked] * 3 + [pl.BlockSpec(block, lambda step, half: (step, 0))]
        out_specs += [picked] * 3
        out_shape += [jax.ShapeDtypeStruct(arr.shape, jnp.float32)] * 3
    in_specs = [pl.BlockSpec(memory_space=pltpu.SMEM), pl.BlockSpec(clip.shape, lambda step, half: (0, 0))] + full
    args = [half_idx, rate, clip, *first, grads[0], *second, grads[1]]
    aliases = {}
    if made:
        in_specs.append(pl.BlockSpec(memory_space=pl.ANY))
        args.append(pltpu.with_memory_space_constraint(rows, pltpu.VMEM))
        out_specs.append(pl.BlockSpec(memory_space=pl.ANY))
        out_shape.append(jax.ShapeDtypeStruct(rows.shape, rows.dtype))
        aliases = {len(args) + idx: idx for idx in range(6)}
        in_specs += [pl.BlockSpec(memory_space=pl.ANY)] * 6
        args += list(made)
    return pl.pallas_call(
        functools.partial(update_kernel, len(in_specs) - 2),
        out_shape=tuple(out_shape),
        grid_spec=pltpu.PrefetchScalarGridSpec(num_scalar_prefetch=1, grid=(steps,), in_specs=in_specs, out_specs=tuple(out_specs),
                                              scratch_shapes=[pltpu.SemaphoreType.DMA((FINAL_STEPS,))] if made else []),
        input_output_aliases=aliases,
        compiler_params=pltpu.CompilerParams(vmem_limit_bytes=(24 if made else 62) * 2 ** 20),
        cost_estimate=pl.CostEstimate(flops=30 * 2 ** 20, bytes_accessed=30 * 2 ** 20, transcendentals=0),
        name='far_update' if made else 'near_update',
    )(*args)


def backward_kernel(limit_ref, rate_ref, act_ref, dout_ref, w1_ref, w2_ref, m1_ref, m2_ref, v1_ref, v2_ref, acc1_ref, acc2_ref,
                    g1_ref, g2_ref, clip_ref, b1_ref, b2_ref,
                    actv, grad, w1v, w2v, hid, slope, dpre, sent, accv, inbox,
                    norms, lsem, hsem, asem, csend, crecv, rsend, rrecv, nsend, nrecv):
    stage = lax.axis_index('stage')
    rep = lax.axis_index('data')
    far = 1 - rep
    n_rows, dim = actv.shape
    width = w1v.shape[1]
    n_chunks = n_rows // ROWS
    last = 3
    half1 = dim // 2
    half2 = width // 2
    n_parts = inbox.shape[0]
    n_cols = width // PART

    def chunk(idx):
        return pl.ds(pl.multiple_of(idx * ROWS, ROWS), ROWS)

    def peer(**where):
        return dict(device_id=where, device_id_type=pl.DeviceIdType.MESH)

    loads = [pltpu.make_async_copy(w1_ref, slope.at[2 * dim:3 * dim, :], lsem.at[0]), pltpu.make_async_copy(act_ref, actv, lsem.at[1])]
    loads += [pltpu.make_async_copy(w2_ref.at[idx * dim:(idx + 1) * dim, :], slope.at[3 * dim:4 * dim, idx * dim:(idx + 1) * dim], lsem.at[2 + idx]) for idx in range(4)]
    for copy in loads:
        copy.start()
    top = pltpu.make_async_copy(dout_ref, grad, lsem.at[6])

    @pl.when(stage == last)
    def _():
        top.start()

    def load_acc(idx, side, step):
        slot = step % accv.shape[0]
        if idx < n_cols:
            src = acc1_ref.at[pl.ds(pl.multiple_of(side * half1, half1), half1), pl.ds(idx * PART, PART)]
        else:
            src = acc2_ref.at[pl.ds(pl.multiple_of(side * half2 + (idx - n_cols) * half1, half1), half1), :]
        return pltpu.make_async_copy(src, accv.at[slot], asem.at[slot])

    steps = [(idx, far) for idx in range(n_parts)] + [(idx, rep) for idx in range(n_parts)]
    ahead = accv.shape[0]
    for step in range(ahead):
        load_acc(*steps[step], step).start()

    barrier = pltpu.get_barrier_semaphore()
    place = rep * 4 + stage
    others = [(place + hop) % 8 for hop in range(1, 8)]
    for other in others:
        pl.semaphore_signal(barrier, inc=1, **peer(data=other // 4, stage=other % 4))
    pl.semaphore_wait(barrier, 7)

    def hop(idx):
        return pltpu.make_async_remote_copy(src_ref=sent.at[chunk(idx)], dst_ref=grad.at[chunk(idx)], send_sem=csend.at[idx], recv_sem=crecv.at[idx],
                                            **peer(stage=(stage + 3) % 4))

    def prepare(idx):
        act = actv[chunk(idx), :]
        for first in range(0, width, COLS):
            cols = slice(first, first + COLS)
            z = jnp.dot(act, w1v[:, cols], preferred_element_type=jnp.float32)
            sq = z * z
            th = jnp.tanh(z * (0.7978845608028654 + 0.035677408136300125 * sq))
            gate = 0.5 + 0.5 * th
            hid[chunk(idx), cols] = (z * gate).astype(jnp.bfloat16)
            slope[chunk(idx), cols] = gate + (0.5 * z) * (1.0 - th * th) * (0.7978845608028654 + 0.10703222440890037 * sq)

    def descend(idx):
        grad_rows = grad[chunk(idx), :]
        total = None
        for first in range(0, width, COLS):
            cols = slice(first, first + COLS)
            d_hid = lax.dot_general(grad_rows, w2v[cols, :], TRANS_DIMS, preferred_element_type=jnp.float32)
            d_pre = (slope[chunk(idx), cols] * d_hid).astype(jnp.bfloat16)
            dpre[chunk(idx), cols] = d_pre
            part = lax.dot_general(d_pre, w1v[:, cols], TRANS_DIMS, preferred_element_type=jnp.float32)
            total = part if first == 0 else total + part
        sent[chunk(idx), :] = (grad_rows.astype(jnp.float32) + total).astype(jnp.bfloat16)

    loads[0].wait()

    @pl.loop(0, dim // 64)
    def _(idx):
        span = pl.ds(pl.multiple_of(idx * 64, 64), 64)
        w1v[span, :] = slope[pl.ds(pl.multiple_of(2 * dim + idx * 64, 64), 64), :].astype(jnp.bfloat16)

    loads[1].wait()
    prepare(0)
    for copy in loads[2:]:
        copy.wait()

    @pl.loop(0, dim // 64)
    def _(idx):
        for group in range(4):
            span = pl.ds(pl.multiple_of(group * dim + idx * 64, 64), 64)
            w2v[span, :] = slope[pl.ds(pl.multiple_of(3 * dim + idx * 64, 64), 64), group * dim:(group + 1) * dim].astype(jnp.bfloat16)

    @pl.when(stage == last)
    def _():
        top.wait()

    @pl.loop(0, n_chunks)
    def _(idx):
        @pl.when(stage < last)
        def _():
            hop(idx).wait_recv()

        descend(idx)

        @pl.when(stage > 0)
        def _():
            hop(idx).start()

        @pl.when(idx + 1 < n_chunks)
        def _():
            prepare(idx + 1)

    near = []
    for idx, ref in enumerate((w1_ref, m1_ref, v1_ref)):
        near.append(pltpu.make_async_copy(ref.at[pl.ds(pl.multiple_of(rep * half1, half1), half1), :], slope.at[dim + idx * half1:dim + (idx + 1) * half1, :], hsem.at[len(near)]))
    for idx, ref in enumerate((w2_ref, m2_ref, v2_ref)):
        for group in range(4):
            near.append(pltpu.make_async_copy(ref.at[pl.ds(pl.multiple_of(rep * half2 + group * half1, half1), half1), :],
                                              slope.at[dim + (3 + idx) * half1:dim + (4 + idx) * half1, group * dim:(group + 1) * dim], hsem.at[len(near)]))
    for copy in near:
        copy.start()

    def weight_grad(idx, side):
        if idx < n_cols:
            left = actv[:, pl.ds(pl.multiple_of(side * half1, half1), half1)]
            right = dpre[:, idx * PART:(idx + 1) * PART]
        else:
            left = hid[:, pl.ds(pl.multiple_of(side * half2 + (idx - n_cols) * half1, half1), half1)]
            right = grad[...]
        return lax.dot_general(left, right, FIRST_DIMS, preferred_element_type=jnp.float32)

    def own_part(idx):
        if idx < n_cols:
            return g1_ref, (slice(None), slice(idx * PART, (idx + 1) * PART))
        return g2_ref, (slice((idx - n_cols) * half1, (idx - n_cols + 1) * half1), slice(None))

    def outbox(idx):
        return slope.at[pl.ds((idx // n_cols) * half1, half1), pl.ds((idx % n_cols) * PART, PART)]

    def post(idx):
        return pltpu.make_async_remote_copy(src_ref=outbox(idx), dst_ref=inbox.at[idx], send_sem=rsend.at[idx], recv_sem=rrecv.at[idx], **peer(data=far))

    for step, (idx, side) in enumerate(steps):
        load_acc(idx, side, step).wait()
        value = accv[step % ahead] + weight_grad(idx, side)
        if step < n_parts:
            outbox(idx)[...] = value
            post(idx).start()
        else:
            ref, where = own_part(idx)
            ref[where] = value
        if step + ahead < len(steps):
            load_acc(*steps[step + ahead], step + ahead).start()

    squares = jnp.zeros((8, PART), jnp.float32)
    for idx in range(n_parts):
        post(idx).wait_recv()
        ref, where = own_part(idx)
        mean = 0.5 * (ref[where] + inbox[idx])
        ref[where] = mean
        squares = squares + jnp.sum((mean * mean).reshape(half1 // 8, 8, PART), axis=0)
    norms[place] = squares

    def tell(idx):
        return pltpu.make_async_remote_copy(src_ref=norms.at[place], dst_ref=norms.at[place], send_sem=nsend.at[idx], recv_sem=nrecv.at[place],
                                            **peer(data=others[idx] // 4, stage=others[idx] % 4))

    def hear(idx):
        ref = norms.at[others[idx]]
        return pltpu.make_async_remote_copy(src_ref=ref, dst_ref=ref, send_sem=nsend.at[idx], recv_sem=nrecv.at[others[idx]],
                                            **peer(data=others[idx] // 4, stage=others[idx] % 4))

    for idx in range(7):
        tell(idx).start()
    for idx in range(7):
        hear(idx).wait_recv()
    total = norms[0]
    for idx in range(1, 8):
        total = total + norms[idx]
    total = jnp.sum(jnp.sum(total, axis=0, keepdims=True), axis=1, keepdims=True)
    clip = jnp.minimum(1.0, limit_ref[0] / (jnp.sqrt(total) + NORM_EPS))
    clip_ref[...] = jnp.broadcast_to(clip, clip_ref.shape)
    for copy in near:
        copy.wait()

    @pl.loop(0, half1 // ADAM_ROWS)
    def _(idx):
        def from_slope(which, cols):
            return slope[pl.ds(pl.multiple_of(dim + which * half1 + idx * ADAM_ROWS, ADAM_ROWS), ADAM_ROWS), cols]

        coef = clip_ref[0:1, 0:1]
        span = pl.ds(pl.multiple_of(idx * ADAM_ROWS, ADAM_ROWS), ADAM_ROWS)
        every = slice(0, width)
        new_w, _, _ = adamw_rows(coef, rate_ref[0], from_slope(0, every), from_slope(1, every), from_slope(2, every), g1_ref[span, :])
        b1_ref[span, :] = (0.5 * new_w).astype(jnp.bfloat16)
        for group in range(4):
            cols = slice(group * dim, (group + 1) * dim)
            span = pl.ds(pl.multiple_of(group * half1 + idx * ADAM_ROWS, ADAM_ROWS), ADAM_ROWS)
            new_w, _, _ = adamw_rows(coef, rate_ref[0], from_slope(3, cols), from_slope(4, cols), from_slope(5, cols), g2_ref[span, :])
            b2_ref[span, :] = new_w.astype(jnp.bfloat16)

    for idx in range(7):
        tell(idx).wait_send()
    for idx in range(n_parts):
        post(idx).wait_send()

    @pl.when(stage > 0)
    def _():
        @pl.loop(0, n_chunks)
        def _(idx):
            hop(idx).wait_send()


def backward_all(limit, rate, act, d_out, first, second, acc_first, acc_second):
    n_rows, dim = act.shape
    width = first[0].shape[1]
    half1 = dim // 2
    n_chunks = n_rows // ROWS
    n_parts = 2 * (width // PART)
    dma = pltpu.SemaphoreType.DMA
    bf16, f32 = jnp.bfloat16, jnp.float32
    vmem = pl.BlockSpec(memory_space=pltpu.VMEM)
    return pl.pallas_call(
        backward_kernel,
        out_shape=(jax.ShapeDtypeStruct((half1, width), f32), jax.ShapeDtypeStruct((width // 2, dim), f32), jax.ShapeDtypeStruct((8, 128), f32),
                   jax.ShapeDtypeStruct((half1, width), bf16), jax.ShapeDtypeStruct((width // 2, dim), bf16)),
        in_specs=[pl.BlockSpec(memory_space=pltpu.SMEM)] * 2 + [pl.BlockSpec(memory_space=pl.ANY)] * 10,
        out_specs=(vmem,) * 5,
        scratch_shapes=[
            pltpu.VMEM((n_rows, dim), bf16), pltpu.VMEM((n_rows, dim), bf16),
            pltpu.VMEM((dim, width), bf16), pltpu.VMEM((width, dim), bf16),
            pltpu.VMEM((n_rows, width), bf16), pltpu.VMEM((n_rows, width), f32), pltpu.VMEM((n_rows, width), bf16),
            pltpu.VMEM((n_rows, dim), bf16), pltpu.VMEM((4, half1, PART), f32), pltpu.VMEM((n_parts, half1, PART), f32), pltpu.VMEM((8, 8, PART), f32),
            dma((7,)), dma((15,)), dma((4,)), dma((n_chunks,)), dma((n_chunks,)), dma((n_parts,)), dma((n_parts,)), dma((7,)), dma((8,)),
        ],
        compiler_params=pltpu.CompilerParams(collective_id=1, has_side_effects=True, vmem_limit_bytes=63 * 2 ** 20),
        cost_estimate=pl.CostEstimate(flops=10 * n_rows * dim * width, bytes_accessed=40 * 2 ** 20, transcendentals=0),
        name='backward_all',
    )(limit, rate, act, d_out, first[0], second[0], first[1], second[1], first[2], second[2], acc_first, acc_second)


def solution(mesh):
    n_stage = mesh.shape['stage']
    w_spec = P('stage', None, None)
    acc_spec = P('data', 'stage', None, None)
    row_spec = P(None, 'data', None)

    def stage_program(w_in, w_out, mom_in, mom_out, var_in, var_out, acc_in, acc_out, stage_acts, d_out, next_x, learn_rate, max_norm):
        rep_idx = lax.axis_index('data')
        first = (w_in[0], mom_in[0], var_in[0])
        second = (w_out[0], mom_out[0], var_out[0])
        near_first, near_second, clip, half_first, half_second = backward_all(
            max_norm, learn_rate, stage_acts[0], d_out, first, second, acc_in[0, 0], acc_out[0, 0])
        own = (half_first, half_second)
        chip = tuple(lax.ppermute(arr, 'stage', [(src, (src + 2) % 4) for src in range(4)]) for arr in own)
        twin = tuple(lax.ppermute(arr, 'data', [(0, 1), (1, 0)]) for arr in own)
        near = half_update(rep_idx.reshape(1), learn_rate, clip, first, second, (near_first, near_second))
        n_micro, n_rows, dim = next_x.shape
        rows, far_first, far_second = forward_all(next_x.reshape(n_micro * n_rows, dim), own, chip, twin, near_first, near_second, n_stage, SHARED)
        *news, next_y = half_update((1 - rep_idx).reshape(1), learn_rate, clip, first, second, (far_first, far_second), near, rows)
        return (news[0][None], news[3][None], news[1][None], news[4][None], news[2][None], news[5][None], next_y.reshape(next_x.shape))

    return jax.shard_map(stage_program, mesh=mesh, in_specs=(w_spec, w_spec, w_spec, w_spec, w_spec, w_spec, acc_spec, acc_spec, P('stage', 'data', None), P('data', None), row_spec, P(None), P(None)), out_specs=(w_spec, w_spec, w_spec, w_spec, w_spec, w_spec, row_spec), check_vma=False)
```

```python
import functools

import jax
import jax.numpy as jnp
from jax import lax
from jax.experimental import pallas as pl
from jax.experimental.pallas import tpu as pltpu
from jax.sharding import PartitionSpec as P

BETA_ONE = 0.9
BETA_TWO = 0.95
ADAM_EPS = 1e-8
WEIGHT_DECAY = 0.1
STEP_COUNT = 10
NORM_EPS = 1e-6
TRANS_DIMS = (((1,), (1,)), ((), ()))
FIRST_DIMS = (((0,), (0,)), ((), ()))
TILE = 512
CHUNK = 512
BEHIND = 3
FORWARD_VMEM = 30
LAG = 5
PRE = 4
SHARED = 4
OWN_TILES = (14, 14, 14, 14)
UPDATE_STEPS = 8
FINAL_STEPS = 8
ADAM_ROWS = 32
ROWS = 256
PART = 512
COLS = 512


def gelu_of_half(half):
    return half + half * jnp.tanh(half * (1.5957691216057308 + 0.28541926509040104 * (half * half)))


def forward_kernel(n_low, n_high, n_both, x_ref, w1_ref, w2_ref, xw1_ref, xw2_ref, rw1_ref, rw2_ref, g1_ref, g2_ref, y_ref, far1_ref, far2_ref,
                   xv, pv, w1v, w2v, xsem, psem, lsem, csend, asend, rsend, crecv, arecv, rrecv, wsend, wrecv, fsend, frecv):
    stage = lax.axis_index('stage')
    rep = lax.axis_index('data')
    far = 1 - rep
    core = stage % 2
    partner = stage + 1 - 2 * core
    across = (stage + 2) % 4
    corner = (partner + 2) % 4
    early = stage < 2
    mine, theirs = jnp.where(early, n_low, n_high), jnp.where(early, n_high, n_low)
    n_tiles = mine + n_both
    n_blocks, dim, width = w1v.shape
    half1, half2 = dim // 2, width // 2
    to_core, to_chip, to_rep = {'stage': partner}, {'stage': across}, {'data': far}

    def rows(owner, tile):
        count = jnp.where(owner < 2, n_low, n_high)
        base = jnp.where(owner < 2, owner * n_low, 2 * n_low + (owner - 2) * n_high)
        place = jnp.where(tile < count, base + tile, 2 * (n_low + n_high) + (owner % 2) * n_both + tile - count)
        return pl.ds(pl.multiple_of(place * TILE, TILE), TILE)

    def remote(src, dst, send, recv, target):
        return pltpu.make_async_remote_copy(src_ref=src, dst_ref=dst, send_sem=send, recv_sem=recv, device_id=target, device_id_type=pl.DeviceIdType.MESH)

    def load_x(tile):
        return pltpu.make_async_copy(x_ref.at[rows(stage, tile)], xv.at[tile % 2], xsem.at[tile % 2])

    def load_p(tile):
        return pltpu.make_async_copy(x_ref.at[rows(stage, tile)], pv.at[tile], psem.at[tile])

    def part(owner, block, kind):
        if kind == 0:
            return w1v.at[block, pl.ds(pl.multiple_of(owner * half1, half1), half1), :]
        return w2v.at[block, pl.ds(pl.multiple_of(owner * half2, half2), half2), :]

    def move(owner, block, kind, target, lane):
        ref = part(owner, block, kind)
        return remote(ref, ref, wsend.at[lane], wrecv.at[(owner * n_blocks + block) * 2 + kind], target)

    def arrive(owner, block, kind):
        move(owner, block, kind, to_core, 0).wait_recv()

    fetched = {}
    for lane, (where, kind, ref) in enumerate((('chip', 0, xw1_ref), ('rep', 1, rw2_ref), ('rep', 0, rw1_ref), ('chip', 1, xw2_ref), ('own', 0, w1_ref), ('own', 1, w2_ref))):
        owner, block = {'own': (rep, stage), 'chip': (rep, across), 'rep': (far, stage)}[where]
        fetched[where, kind] = pltpu.make_async_copy(ref, part(owner, block, kind), lsem.at[lane])
        fetched[where, kind].start()

    @pl.when(early)
    def _():
        for tile in range(PRE):
            load_p(tile).start()

    @pl.when(stage >= 2)
    def _():
        load_x(0).start()

    barrier = pltpu.get_barrier_semaphore()
    for target in (to_core, to_chip, to_rep):
        pl.semaphore_signal(barrier, inc=1, device_id=target, device_id_type=pl.DeviceIdType.MESH)
    pl.semaphore_wait(barrier, 3)

    sends = []

    def send(owner, block, kind, target):
        copy = move(owner, block, kind, target, len(sends))
        sends.append(copy)
        copy.start()

    fetched['chip', 0].wait()
    send(rep, across, 0, to_rep)
    fetched['rep', 1].wait()
    send(far, stage, 1, to_chip)
    for kind in (0, 1):
        fetched['own', kind].wait()
        send(rep, stage, kind, to_core)
    fetched['rep', 0].wait()
    for kind in (0, 1):
        send(far, stage, kind, to_core)
    fetched['chip', 1].wait()
    for kind in (0, 1):
        send(rep, across, kind, to_core)
    for owner in (rep, far):
        for kind in (0, 1):
            arrive(owner, partner, kind)

    def two_blocks(ref, pair):
        half = TILE // 2
        pieces = [(side, first) for first in range(0, width, CHUNK) for side in (0, 1)]
        x_rows = [ref[side * half:(side + 1) * half, :] for side in (0, 1)]
        for block in (2 * pair, 2 * pair + 1):
            total = [None, None]
            act_h = {}
            for turn in range(len(pieces) + BEHIND):
                if turn < len(pieces):
                    side, first = pieces[turn]
                    halved = jnp.dot(x_rows[side], w1v[block, :, first:first + CHUNK], preferred_element_type=jnp.float32)
                    act_h[turn] = gelu_of_half(halved).astype(jnp.bfloat16)
                if turn >= BEHIND:
                    side, first = pieces[turn - BEHIND]
                    piece = jnp.dot(act_h.pop(turn - BEHIND), w2v[block, first:first + CHUNK, :], preferred_element_type=jnp.float32)
                    total[side] = piece if first == 0 else total[side] + piece
            x_rows = [(x_rows[side].astype(jnp.float32) + total[side]).astype(jnp.bfloat16) for side in (0, 1)]
        for side in (0, 1):
            ref[side * half:(side + 1) * half, :] = x_rows[side]

    @pl.when(early)
    def _():
        @pl.loop(0, PRE)
        def _(tile):
            load_p(tile).wait()

            two_blocks(pv.at[tile], 0)

    for kind in (0, 1):
        arrive(far, across, kind)
        send(far, across, kind, to_core)
    swaps = [remote(src, dst, fsend.at[idx], frecv.at[idx], to_rep) for idx, (src, dst) in enumerate(((g1_ref, far1_ref), (g2_ref, far2_ref)))]
    for copy in swaps:
        copy.start()
    for owner in (rep, far):
        for kind in (0, 1):
            arrive(owner, corner, kind)

    def give(tile, send, recv, target):
        ref = y_ref.at[rows(stage, tile)]
        return remote(ref, ref, send.at[tile], recv.at[tile], target)

    def give_core(tile):
        return give(tile, csend, crecv, to_core)

    def give_chip(tile):
        return give(tile, asend, arecv, to_chip)

    def pass_on(tile):
        ref = y_ref.at[rows(across, tile)]
        return remote(ref, ref, rsend.at[tile], rrecv.at[tile], to_core)

    def relay(tile):
        ref = y_ref.at[rows(across, tile)]
        remote(ref, ref, asend.at[0], arecv.at[tile], to_chip).wait_recv()
        pass_on(tile).start()

    @pl.loop(0, n_tiles)
    def _(tile):
        skip = jnp.where(early, PRE, 0)

        @pl.when(tile < skip)
        def _():
            xv[tile % 2] = pv[tile % PRE]

        @pl.when(tile >= skip)
        def _():
            load_x(tile).wait()

        @pl.when((tile + 1 >= skip) & (tile + 1 < n_tiles))
        def _():
            load_x(tile + 1).start()

        @pl.loop(0, n_blocks // 2)
        def _(pair):
            @pl.when((pair > 0) | (tile >= skip))
            def _():
                two_blocks(xv.at[tile % 2], pair)

        y_ref[rows(stage, tile), :] = xv[tile % 2]
        give_core(tile).start()

        @pl.when(tile < mine)
        def _():
            give_chip(tile).start()

        @pl.when((tile >= LAG) & (tile < LAG + theirs))
        def _():
            relay(tile - LAG)

    @pl.loop(n_tiles - LAG, theirs)
    def _(tile):
        relay(tile)

    @pl.loop(0, n_tiles)
    def _(tile):
        ref = y_ref.at[rows(partner, tile)]
        remote(ref, ref, csend.at[0], crecv.at[tile], to_core).wait_recv()
        give_core(tile).wait_send()

    @pl.loop(0, theirs)
    def _(tile):
        ref = y_ref.at[rows(corner, tile)]
        remote(ref, ref, rsend.at[0], rrecv.at[tile], to_core).wait_recv()
        pass_on(tile).wait_send()

    @pl.loop(0, mine)
    def _(tile):
        give_chip(tile).wait_send()

    for copy in sends:
        copy.wait_send()
    for copy in swaps:
        copy.wait()


def forward_all(x_rows, own, chip, twin, near_first, near_second, n_stage, n_both):
    n_rows, dim = x_rows.shape
    width = own[0].shape[1]
    n_own = max(OWN_TILES)
    n_tiles = n_own + n_both
    assert TILE * (sum(OWN_TILES) + 2 * n_both) == n_rows
    dma = pltpu.SemaphoreType.DMA
    flops = 4 * n_tiles * TILE * dim * width * n_stage
    return pl.pallas_call(
        functools.partial(forward_kernel, OWN_TILES[0], OWN_TILES[2], n_both),
        out_shape=(pltpu.VMEM((n_rows, dim), jnp.bfloat16), jax.ShapeDtypeStruct(near_first.shape, jnp.float32), jax.ShapeDtypeStruct(near_second.shape, jnp.float32)),
        in_specs=[pl.BlockSpec(memory_space=pl.ANY)] * 9,
        out_specs=(pl.BlockSpec(memory_space=pltpu.VMEM),) + (pl.BlockSpec(memory_space=pl.ANY),) * 2,
        scratch_shapes=[
            pltpu.VMEM((2, TILE, dim), jnp.bfloat16),
            pltpu.VMEM((PRE, TILE, dim), jnp.bfloat16),
            pltpu.VMEM((n_stage, dim, width), jnp.bfloat16),
            pltpu.VMEM((n_stage, width, dim), jnp.bfloat16),
            dma((2,)), dma((PRE,)), dma((6,)), dma((n_tiles,)), dma((n_own,)), dma((n_own,)),
            dma((n_tiles,)), dma((n_own,)), dma((n_own,)), dma((10,)), dma((4 * n_stage,)), dma((2,)), dma((2,)),
        ],
        compiler_params=pltpu.CompilerParams(collective_id=0, has_side_effects=True, vmem_limit_bytes=FORWARD_VMEM * 2 ** 20),
        cost_estimate=pl.CostEstimate(flops=flops, bytes_accessed=2 * n_rows * dim * 2, transcendentals=0),
        name='forward_all',
    )(x_rows, *own, *chip, *twin, near_first, near_second)


def adamw_rows(coef, rate, param, moment, second, grad_val):
    scaled = coef * grad_val
    mom_new = BETA_ONE * moment + (1.0 - BETA_ONE) * scaled
    sec_new = BETA_TWO * second + (1.0 - BETA_TWO) * scaled * scaled
    mom_hat = mom_new * (1.0 / (1.0 - BETA_ONE ** STEP_COUNT))
    sec_hat = sec_new * (1.0 / (1.0 - BETA_TWO ** STEP_COUNT))
    return param - rate * (mom_hat / (jnp.sqrt(sec_hat) + ADAM_EPS) + WEIGHT_DECAY * param), mom_new, sec_new


def update_kernel(n_ins, half_ref, rate_ref, clip_ref, *refs):
    outs = refs[n_ins:]
    if len(outs) == 8:
        step, steps = pl.program_id(0), pl.num_programs(0)

        def drain(idx):
            size = outs[6].shape[0] // FINAL_STEPS
            span = pl.ds(pl.multiple_of(idx * size, size), size)
            return pltpu.make_async_copy(refs[8].at[span], outs[6].at[span], outs[7].at[idx])

        drain(step).start()

    for side in (0, 1):
        param, moment, second, grad_val = (ref[...] for ref in refs[4 * side:4 * side + 4])
        news = adamw_rows(clip_ref[0:1, 0:1], rate_ref[0], param, moment, second, grad_val)
        for ref, new in zip(outs[3 * side:3 * side + 3], news):
            ref[...] = new
    if len(outs) == 8:
        @pl.when(step == steps - 1)
        def _():
            for idx in range(FINAL_STEPS):
                drain(idx).wait()


def half_update(half_idx, rate, clip, first, second, grads, made=(), rows=None):
    steps = FINAL_STEPS if made else UPDATE_STEPS
    full, out_specs, out_shape = [], [], []
    for arr, grad in zip((first[0], second[0]), grads):
        block = (grad.shape[0] // steps, grad.shape[1])
        picked = pl.BlockSpec(block, lambda step, half: (half[0] * steps + step, 0))
        full += [picked] * 3 + [pl.BlockSpec(block, lambda step, half: (step, 0))]
        out_specs += [picked] * 3
        out_shape += [jax.ShapeDtypeStruct(arr.shape, jnp.float32)] * 3
    in_specs = [pl.BlockSpec(memory_space=pltpu.SMEM), pl.BlockSpec(clip.shape, lambda step, half: (0, 0))] + full
    args = [half_idx, rate, clip, *first, grads[0], *second, grads[1]]
    aliases = {}
    if made:
        in_specs.append(pl.BlockSpec(memory_space=pl.ANY))
        args.append(pltpu.with_memory_space_constraint(rows, pltpu.VMEM))
        out_specs.append(pl.BlockSpec(memory_space=pl.ANY))
        out_shape.append(jax.ShapeDtypeStruct(rows.shape, rows.dtype))
        aliases = {len(args) + idx: idx for idx in range(6)}
        in_specs += [pl.BlockSpec(memory_space=pl.ANY)] * 6
        args += list(made)
    return pl.pallas_call(
        functools.partial(update_kernel, len(in_specs) - 2),
        out_shape=tuple(out_shape),
        grid_spec=pltpu.PrefetchScalarGridSpec(num_scalar_prefetch=1, grid=(steps,), in_specs=in_specs, out_specs=tuple(out_specs),
                                              scratch_shapes=[pltpu.SemaphoreType.DMA((FINAL_STEPS,))] if made else []),
        input_output_aliases=aliases,
        compiler_params=pltpu.CompilerParams(vmem_limit_bytes=(24 if made else 62) * 2 ** 20),
        cost_estimate=pl.CostEstimate(flops=30 * 2 ** 20, bytes_accessed=30 * 2 ** 20, transcendentals=0),
        name='far_update' if made else 'near_update',
    )(*args)


def backward_kernel(limit_ref, rate_ref, act_ref, dout_ref, w1_ref, w2_ref, m1_ref, m2_ref, v1_ref, v2_ref, acc1_ref, acc2_ref,
                    g1_out, g2_out, clip_ref, b1_out, b2_out, g1_ref, g2_ref, b1_ref, b2_ref,
                    actv, grad, w1v, w2v, hid, slope, dpre, sent, accv, inbox,
                    norms, lsem, hsem, gsem, bsem, asem, csend, crecv, rsend, rrecv, nsend, nrecv):
    stage = lax.axis_index('stage')
    rep = lax.axis_index('data')
    far = 1 - rep
    n_rows, dim = actv.shape
    width = w1v.shape[1]
    n_chunks = n_rows // ROWS
    last = 3
    half1 = dim // 2
    half2 = width // 2
    n_parts = inbox.shape[0]
    n_cols = width // PART

    def chunk(idx):
        return pl.ds(pl.multiple_of(idx * ROWS, ROWS), ROWS)

    def peer(**where):
        return dict(device_id=where, device_id_type=pl.DeviceIdType.MESH)

    loads = [pltpu.make_async_copy(w1_ref, slope.at[2 * dim:3 * dim, :], lsem.at[0]), pltpu.make_async_copy(act_ref, actv, lsem.at[1])]
    loads += [pltpu.make_async_copy(w2_ref.at[idx * dim:(idx + 1) * dim, :], slope.at[3 * dim:4 * dim, idx * dim:(idx + 1) * dim], lsem.at[2 + idx]) for idx in range(4)]
    for copy in loads:
        copy.start()
    top = pltpu.make_async_copy(dout_ref, grad, lsem.at[6])

    @pl.when(stage == last)
    def _():
        top.start()

    def load_acc(idx, side, step):
        slot = step % accv.shape[0]
        if idx < n_cols:
            src = acc1_ref.at[pl.ds(pl.multiple_of(side * half1, half1), half1), pl.ds(idx * PART, PART)]
        else:
            src = acc2_ref.at[pl.ds(pl.multiple_of(side * half2 + (idx - n_cols) * half1, half1), half1), :]
        return pltpu.make_async_copy(src, accv.at[slot], asem.at[slot])

    steps = [(idx, far) for idx in range(n_parts)] + [(idx, rep) for idx in range(n_parts)]
    ahead = accv.shape[0]
    for step in range(ahead):
        load_acc(*steps[step], step).start()

    barrier = pltpu.get_barrier_semaphore()
    place = rep * 4 + stage
    others = [(place + hop) % 8 for hop in range(1, 8)]
    for other in others:
        pl.semaphore_signal(barrier, inc=1, **peer(data=other // 4, stage=other % 4))
    pl.semaphore_wait(barrier, 7)

    def hop(idx):
        return pltpu.make_async_remote_copy(src_ref=sent.at[chunk(idx)], dst_ref=grad.at[chunk(idx)], send_sem=csend.at[idx], recv_sem=crecv.at[idx],
                                            **peer(stage=(stage + 3) % 4))

    def prepare(idx):
        act = actv[chunk(idx), :]
        for first in range(0, width, COLS):
            cols = slice(first, first + COLS)
            z = jnp.dot(act, w1v[:, cols], preferred_element_type=jnp.float32)
            sq = z * z
            th = jnp.tanh(z * (0.7978845608028654 + 0.035677408136300125 * sq))
            gate = 0.5 + 0.5 * th
            hid[chunk(idx), cols] = (z * gate).astype(jnp.bfloat16)
            slope[chunk(idx), cols] = gate + (0.5 * z) * (1.0 - th * th) * (0.7978845608028654 + 0.10703222440890037 * sq)

    def descend(idx):
        grad_rows = grad[chunk(idx), :]
        total = None
        for first in range(0, width, COLS):
            cols = slice(first, first + COLS)
            d_hid = lax.dot_general(grad_rows, w2v[cols, :], TRANS_DIMS, preferred_element_type=jnp.float32)
            d_pre = (slope[chunk(idx), cols] * d_hid).astype(jnp.bfloat16)
            dpre[chunk(idx), cols] = d_pre
            part = lax.dot_general(d_pre, w1v[:, cols], TRANS_DIMS, preferred_element_type=jnp.float32)
            total = part if first == 0 else total + part
        sent[chunk(idx), :] = (grad_rows.astype(jnp.float32) + total).astype(jnp.bfloat16)

    loads[0].wait()

    @pl.loop(0, dim // 64)
    def _(idx):
        span = pl.ds(pl.multiple_of(idx * 64, 64), 64)
        w1v[span, :] = slope[pl.ds(pl.multiple_of(2 * dim + idx * 64, 64), 64), :].astype(jnp.bfloat16)

    loads[1].wait()
    prepare(0)
    for copy in loads[2:]:
        copy.wait()

    @pl.loop(0, dim // 64)
    def _(idx):
        for group in range(4):
            span = pl.ds(pl.multiple_of(group * dim + idx * 64, 64), 64)
            w2v[span, :] = slope[pl.ds(pl.multiple_of(3 * dim + idx * 64, 64), 64), group * dim:(group + 1) * dim].astype(jnp.bfloat16)

    @pl.when(stage == last)
    def _():
        top.wait()

    @pl.loop(0, n_chunks)
    def _(idx):
        @pl.when(stage < last)
        def _():
            hop(idx).wait_recv()

        descend(idx)

        @pl.when(stage > 0)
        def _():
            hop(idx).start()

        @pl.when(idx + 1 < n_chunks)
        def _():
            prepare(idx + 1)

    near = []
    for idx, ref in enumerate((w1_ref, m1_ref, v1_ref)):
        near.append(pltpu.make_async_copy(ref.at[pl.ds(pl.multiple_of(rep * half1, half1), half1), :], slope.at[dim + idx * half1:dim + (idx + 1) * half1, :], hsem.at[len(near)]))
    for idx, ref in enumerate((w2_ref, m2_ref, v2_ref)):
        for group in range(4):
            near.append(pltpu.make_async_copy(ref.at[pl.ds(pl.multiple_of(rep * half2 + group * half1, half1), half1), :],
                                              slope.at[dim + (3 + idx) * half1:dim + (4 + idx) * half1, group * dim:(group + 1) * dim], hsem.at[len(near)]))
    for copy in near:
        copy.start()

    def weight_grad(idx, side):
        if idx < n_cols:
            left = actv[:, pl.ds(pl.multiple_of(side * half1, half1), half1)]
            right = dpre[:, idx * PART:(idx + 1) * PART]
        else:
            left = hid[:, pl.ds(pl.multiple_of(side * half2 + (idx - n_cols) * half1, half1), half1)]
            right = grad[...]
        return lax.dot_general(left, right, FIRST_DIMS, preferred_element_type=jnp.float32)

    def own_part(idx):
        if idx < n_cols:
            return g1_ref, (slice(None), slice(idx * PART, (idx + 1) * PART))
        return g2_ref, (slice((idx - n_cols) * half1, (idx - n_cols + 1) * half1), slice(None))

    def outbox(idx):
        return slope.at[pl.ds((idx // n_cols) * half1, half1), pl.ds((idx % n_cols) * PART, PART)]

    def post(idx):
        return pltpu.make_async_remote_copy(src_ref=outbox(idx), dst_ref=inbox.at[idx], send_sem=rsend.at[idx], recv_sem=rrecv.at[idx], **peer(data=far))

    for step, (idx, side) in enumerate(steps):
        load_acc(idx, side, step).wait()
        value = accv[step % ahead] + weight_grad(idx, side)
        if step < n_parts:
            outbox(idx)[...] = value
            post(idx).start()
        else:
            ref, where = own_part(idx)
            ref[where] = value
        if step + ahead < len(steps):
            load_acc(*steps[step + ahead], step + ahead).start()

    for copy in near:
        copy.wait()
    mom_fix, sec_fix = 1.0 / (1.0 - BETA_ONE ** STEP_COUNT), 1.0 / (1.0 - BETA_TWO ** STEP_COUNT)
    kept = (1.0 - WEIGHT_DECAY * rate_ref[0], BETA_ONE * mom_fix, BETA_TWO * sec_fix)

    @pl.loop(0, half1 // ADAM_ROWS)
    def _(idx):
        for which in range(6):
            span = pl.ds(pl.multiple_of(dim + which * half1 + idx * ADAM_ROWS, ADAM_ROWS), ADAM_ROWS)
            slope[span, :] = kept[which % 3] * slope[span, :]

    def new_weight(which, coef, slope_rows, cols, grad_val):
        base, mom, sec = (slope[pl.ds(pl.multiple_of(dim + (which + idx) * half1 + slope_rows, ADAM_ROWS), ADAM_ROWS), cols] for idx in range(3))
        scaled = coef * grad_val
        top = mom + ((1.0 - BETA_ONE) * mom_fix) * scaled
        low = jnp.sqrt(sec + ((1.0 - BETA_TWO) * sec_fix) * (scaled * scaled)) + ADAM_EPS
        return base - rate_ref[0] * (top / low)

    def put_grad(idx):
        if idx < n_cols:
            where = (slice(None), slice(idx * PART, (idx + 1) * PART))
            return pltpu.make_async_copy(g1_ref.at[where], g1_out.at[where], gsem.at[idx])
        where = slice((idx - n_cols) * half1, (idx - n_cols + 1) * half1)
        return pltpu.make_async_copy(g2_ref.at[where], g2_out.at[where], gsem.at[idx])

    squares = jnp.zeros((8, PART), jnp.float32)
    for idx in range(n_parts):
        post(idx).wait_recv()
        ref, where = own_part(idx)
        mean = 0.5 * (ref[where] + inbox[idx])
        ref[where] = mean
        put_grad(idx).start()
        squares = squares + jnp.sum((mean * mean).reshape(half1 // 8, 8, PART), axis=0)
    norms[place] = squares

    def tell(idx):
        return pltpu.make_async_remote_copy(src_ref=norms.at[place], dst_ref=norms.at[place], send_sem=nsend.at[idx], recv_sem=nrecv.at[place],
                                            **peer(data=others[idx] // 4, stage=others[idx] % 4))

    def hear(idx):
        ref = norms.at[others[idx]]
        return pltpu.make_async_remote_copy(src_ref=ref, dst_ref=ref, send_sem=nsend.at[idx], recv_sem=nrecv.at[others[idx]],
                                            **peer(data=others[idx] // 4, stage=others[idx] % 4))

    for idx in range(7):
        tell(idx).start()
    for idx in range(7):
        hear(idx).wait_recv()
    total = norms[0]
    for idx in range(1, 8):
        total = total + norms[idx]
    total = jnp.sum(jnp.sum(total, axis=0, keepdims=True), axis=1, keepdims=True)
    clip = jnp.minimum(1.0, limit_ref[0] / (jnp.sqrt(total) + NORM_EPS))
    clip_ref[...] = jnp.broadcast_to(clip, clip_ref.shape)
    puts = [pltpu.make_async_copy(b1_ref, b1_out, bsem.at[0]), pltpu.make_async_copy(b2_ref, b2_out, bsem.at[1])]

    @pl.loop(0, half1 // ADAM_ROWS)
    def _(idx):
        span = pl.ds(pl.multiple_of(idx * ADAM_ROWS, ADAM_ROWS), ADAM_ROWS)
        new_w = new_weight(0, clip_ref[0:1, 0:1], idx * ADAM_ROWS, slice(0, width), g1_ref[span, :])
        b1_ref[span, :] = (0.5 * new_w).astype(jnp.bfloat16)

    puts[0].start()

    @pl.loop(0, half1 // ADAM_ROWS)
    def _(idx):
        for group in range(4):
            span = pl.ds(pl.multiple_of(group * half1 + idx * ADAM_ROWS, ADAM_ROWS), ADAM_ROWS)
            new_w = new_weight(3, clip_ref[0:1, 0:1], idx * ADAM_ROWS, slice(group * dim, (group + 1) * dim), g2_ref[span, :])
            b2_ref[span, :] = new_w.astype(jnp.bfloat16)

    puts[1].start()
    for idx in range(n_parts):
        put_grad(idx).wait()
    for copy in puts:
        copy.wait()
    for idx in range(7):
        tell(idx).wait_send()
    for idx in range(n_parts):
        post(idx).wait_send()

    @pl.when(stage > 0)
    def _():
        @pl.loop(0, n_chunks)
        def _(idx):
            hop(idx).wait_send()


def backward_all(limit, rate, act, d_out, first, second, acc_first, acc_second):
    n_rows, dim = act.shape
    width = first[0].shape[1]
    half1 = dim // 2
    n_chunks = n_rows // ROWS
    n_parts = 2 * (width // PART)
    dma = pltpu.SemaphoreType.DMA
    bf16, f32 = jnp.bfloat16, jnp.float32
    vmem = pl.BlockSpec(memory_space=pltpu.VMEM)
    return pl.pallas_call(
        backward_kernel,
        out_shape=(jax.ShapeDtypeStruct((half1, width), f32), jax.ShapeDtypeStruct((width // 2, dim), f32), jax.ShapeDtypeStruct((8, 128), f32),
                   jax.ShapeDtypeStruct((half1, width), bf16), jax.ShapeDtypeStruct((width // 2, dim), bf16)),
        in_specs=[pl.BlockSpec(memory_space=pltpu.SMEM)] * 2 + [pl.BlockSpec(memory_space=pl.ANY)] * 10,
        out_specs=(pl.BlockSpec(memory_space=pl.ANY),) * 2 + (vmem,) + (pl.BlockSpec(memory_space=pl.ANY),) * 2,
        scratch_shapes=[
            pltpu.VMEM((half1, width), f32), pltpu.VMEM((width // 2, dim), f32), pltpu.VMEM((half1, width), bf16), pltpu.VMEM((width // 2, dim), bf16),
            pltpu.VMEM((n_rows, dim), bf16), pltpu.VMEM((n_rows, dim), bf16),
            pltpu.VMEM((dim, width), bf16), pltpu.VMEM((width, dim), bf16),
            pltpu.VMEM((n_rows, width), bf16), pltpu.VMEM((n_rows, width), f32), pltpu.VMEM((n_rows, width), bf16),
            pltpu.VMEM((n_rows, dim), bf16), pltpu.VMEM((4, half1, PART), f32), pltpu.VMEM((n_parts, half1, PART), f32), pltpu.VMEM((8, 8, PART), f32),
            dma((7,)), dma((15,)), dma((n_parts,)), dma((2,)), dma((4,)), dma((n_chunks,)), dma((n_chunks,)), dma((n_parts,)), dma((n_parts,)), dma((7,)), dma((8,)),
        ],
        compiler_params=pltpu.CompilerParams(collective_id=1, has_side_effects=True, vmem_limit_bytes=63 * 2 ** 20),
        cost_estimate=pl.CostEstimate(flops=10 * n_rows * dim * width, bytes_accessed=40 * 2 ** 20, transcendentals=0),
        name='backward_all',
    )(limit, rate, act, d_out, first[0], second[0], first[1], second[1], first[2], second[2], acc_first, acc_second)


def solution(mesh):
    n_stage = mesh.shape['stage']
    w_spec = P('stage', None, None)
    acc_spec = P('data', 'stage', None, None)
    row_spec = P(None, 'data', None)

    def stage_program(w_in, w_out, mom_in, mom_out, var_in, var_out, acc_in, acc_out, stage_acts, d_out, next_x, learn_rate, max_norm):
        rep_idx = lax.axis_index('data')
        first = (w_in[0], mom_in[0], var_in[0])
        second = (w_out[0], mom_out[0], var_out[0])
        near_first, near_second, clip, half_first, half_second = backward_all(
            max_norm, learn_rate, stage_acts[0], d_out, first, second, acc_in[0, 0], acc_out[0, 0])
        own = (half_first, half_second)
        chip = tuple(lax.ppermute(arr, 'stage', [(src, (src + 2) % 4) for src in range(4)]) for arr in own)
        twin = tuple(lax.ppermute(arr, 'data', [(0, 1), (1, 0)]) for arr in own)
        near = half_update(rep_idx.reshape(1), learn_rate, clip, first, second, (near_first, near_second))
        n_micro, n_rows, dim = next_x.shape
        rows, far_first, far_second = forward_all(next_x.reshape(n_micro * n_rows, dim), own, chip, twin, near_first, near_second, n_stage, SHARED)
        *news, next_y = half_update((1 - rep_idx).reshape(1), learn_rate, clip, first, second, (far_first, far_second), near, rows)
        return (news[0][None], news[3][None], news[1][None], news[4][None], news[2][None], news[5][None], next_y.reshape(next_x.shape))

    return jax.shard_map(stage_program, mesh=mesh, in_specs=(w_spec, w_spec, w_spec, w_spec, w_spec, w_spec, acc_spec, acc_spec, P('stage', 'data', None), P('data', None), row_spec, P(None), P(None)), out_specs=(w_spec, w_spec, w_spec, w_spec, w_spec, w_spec, row_spec), check_vma=False)
```

```python
import functools

import jax
import jax.numpy as jnp
from jax import lax
from jax.experimental import pallas as pl
from jax.experimental.pallas import tpu as pltpu
from jax.sharding import PartitionSpec as P

BETA_ONE = 0.9
BETA_TWO = 0.95
ADAM_EPS = 1e-8
WEIGHT_DECAY = 0.1
STEP_COUNT = 10
NORM_EPS = 1e-6
TRANS_DIMS = (((1,), (1,)), ((), ()))
FIRST_DIMS = (((0,), (0,)), ((), ()))
TILE = 512
CHUNK = 512
BEHIND = 3
FORWARD_VMEM = 30
LAG = 5
PRE = 4
SHARED = 4
OWN_TILES = (14, 14, 14, 14)
UPDATE_STEPS = 8
FINAL_STEPS = 4
ADAM_ROWS = 32
ROWS = 256
PART = 512
COLS = 512


def gelu_of_half(half):
    return half + half * jnp.tanh(half * (1.5957691216057308 + 0.28541926509040104 * (half * half)))


def forward_kernel(n_low, n_high, n_both, x_ref, w1_ref, w2_ref, xw1_ref, xw2_ref, rw1_ref, rw2_ref, g1_ref, g2_ref, y_ref, far1_ref, far2_ref,
                   xv, pv, w1v, w2v, xsem, psem, lsem, csend, asend, rsend, crecv, arecv, rrecv, wsend, wrecv, fsend, frecv):
    stage = lax.axis_index('stage')
    rep = lax.axis_index('data')
    far = 1 - rep
    core = stage % 2
    partner = stage + 1 - 2 * core
    across = (stage + 2) % 4
    corner = (partner + 2) % 4
    early = stage < 2
    mine, theirs = jnp.where(early, n_low, n_high), jnp.where(early, n_high, n_low)
    n_tiles = mine + n_both
    n_blocks, dim, width = w1v.shape
    half1, half2 = dim // 2, width // 2
    to_core, to_chip, to_rep = {'stage': partner}, {'stage': across}, {'data': far}

    def rows(owner, tile):
        count = jnp.where(owner < 2, n_low, n_high)
        base = jnp.where(owner < 2, owner * n_low, 2 * n_low + (owner - 2) * n_high)
        place = jnp.where(tile < count, base + tile, 2 * (n_low + n_high) + (owner % 2) * n_both + tile - count)
        return pl.ds(pl.multiple_of(place * TILE, TILE), TILE)

    def remote(src, dst, send, recv, target):
        return pltpu.make_async_remote_copy(src_ref=src, dst_ref=dst, send_sem=send, recv_sem=recv, device_id=target, device_id_type=pl.DeviceIdType.MESH)

    def load_x(tile):
        return pltpu.make_async_copy(x_ref.at[rows(stage, tile)], xv.at[tile % 2], xsem.at[tile % 2])

    def load_p(tile):
        return pltpu.make_async_copy(x_ref.at[rows(stage, tile)], pv.at[tile], psem.at[tile])

    def part(owner, block, kind):
        if kind == 0:
            return w1v.at[block, pl.ds(pl.multiple_of(owner * half1, half1), half1), :]
        return w2v.at[block, pl.ds(pl.multiple_of(owner * half2, half2), half2), :]

    def move(owner, block, kind, target, lane):
        ref = part(owner, block, kind)
        return remote(ref, ref, wsend.at[lane], wrecv.at[(owner * n_blocks + block) * 2 + kind], target)

    def arrive(owner, block, kind):
        move(owner, block, kind, to_core, 0).wait_recv()

    fetched = {}
    for lane, (where, kind, ref) in enumerate((('chip', 0, xw1_ref), ('rep', 1, rw2_ref), ('rep', 0, rw1_ref), ('chip', 1, xw2_ref), ('own', 0, w1_ref), ('own', 1, w2_ref))):
        owner, block = {'own': (rep, stage), 'chip': (rep, across), 'rep': (far, stage)}[where]
        fetched[where, kind] = pltpu.make_async_copy(ref, part(owner, block, kind), lsem.at[lane])
        fetched[where, kind].start()

    @pl.when(early)
    def _():
        for tile in range(PRE):
            load_p(tile).start()

    @pl.when(stage >= 2)
    def _():
        load_x(0).start()

    barrier = pltpu.get_barrier_semaphore()
    for target in (to_core, to_chip, to_rep):
        pl.semaphore_signal(barrier, inc=1, device_id=target, device_id_type=pl.DeviceIdType.MESH)
    pl.semaphore_wait(barrier, 3)

    sends = []

    def send(owner, block, kind, target):
        copy = move(owner, block, kind, target, len(sends))
        sends.append(copy)
        copy.start()

    fetched['chip', 0].wait()
    send(rep, across, 0, to_rep)
    fetched['rep', 1].wait()
    send(far, stage, 1, to_chip)
    for kind in (0, 1):
        fetched['own', kind].wait()
        send(rep, stage, kind, to_core)
    fetched['rep', 0].wait()
    for kind in (0, 1):
        send(far, stage, kind, to_core)
    fetched['chip', 1].wait()
    for kind in (0, 1):
        send(rep, across, kind, to_core)
    for owner in (rep, far):
        for kind in (0, 1):
            arrive(owner, partner, kind)

    def two_blocks(src, pair, dst):
        half = TILE // 2
        pieces = [(side, first) for first in range(0, width, CHUNK) for side in (0, 1)]
        x_rows = [src[side * half:(side + 1) * half, :] for side in (0, 1)]
        for block in (2 * pair, 2 * pair + 1):
            total = [None, None]
            act_h = {}
            for turn in range(len(pieces) + BEHIND):
                if turn < len(pieces):
                    side, first = pieces[turn]
                    halved = jnp.dot(x_rows[side], w1v[block, :, first:first + CHUNK], preferred_element_type=jnp.float32)
                    act_h[turn] = gelu_of_half(halved).astype(jnp.bfloat16)
                if turn >= BEHIND:
                    side, first = pieces[turn - BEHIND]
                    piece = jnp.dot(act_h.pop(turn - BEHIND), w2v[block, first:first + CHUNK, :], preferred_element_type=jnp.float32)
                    total[side] = piece if first == 0 else total[side] + piece
            x_rows = [(x_rows[side].astype(jnp.float32) + total[side]).astype(jnp.bfloat16) for side in (0, 1)]
        for side in (0, 1):
            dst[side * half:(side + 1) * half, :] = x_rows[side]

    @pl.when(early)
    def _():
        @pl.loop(0, PRE)
        def _(tile):
            load_p(tile).wait()

            two_blocks(pv.at[tile], 0, pv.at[tile])

    for kind in (0, 1):
        arrive(far, across, kind)
        send(far, across, kind, to_core)
    swaps = [remote(src, dst, fsend.at[idx], frecv.at[idx], to_rep) for idx, (src, dst) in enumerate(((g1_ref, far1_ref), (g2_ref, far2_ref)))]
    for copy in swaps:
        copy.start()
    for owner in (rep, far):
        for kind in (0, 1):
            arrive(owner, corner, kind)

    def give(tile, send, recv, target):
        ref = y_ref.at[rows(stage, tile)]
        return remote(ref, ref, send.at[tile], recv.at[tile], target)

    def give_core(tile):
        return give(tile, csend, crecv, to_core)

    def give_chip(tile):
        return give(tile, asend, arecv, to_chip)

    def pass_on(tile):
        ref = y_ref.at[rows(across, tile)]
        return remote(ref, ref, rsend.at[tile], rrecv.at[tile], to_core)

    def relay(tile):
        ref = y_ref.at[rows(across, tile)]
        remote(ref, ref, asend.at[0], arecv.at[tile], to_chip).wait_recv()
        pass_on(tile).start()

    @pl.loop(0, n_tiles)
    def _(tile):
        skip = jnp.where(early, PRE, 0)

        @pl.when(tile < skip)
        def _():
            xv[tile % 2] = pv[tile % PRE]

        @pl.when(tile >= skip)
        def _():
            load_x(tile).wait()

        @pl.when((tile + 1 >= skip) & (tile + 1 < n_tiles))
        def _():
            load_x(tile + 1).start()

        @pl.when(tile >= skip)
        def _():
            two_blocks(xv.at[tile % 2], 0, xv.at[tile % 2])

        two_blocks(xv.at[tile % 2], 1, y_ref.at[rows(stage, tile)])
        give_core(tile).start()

        @pl.when(tile < mine)
        def _():
            give_chip(tile).start()

        @pl.when((tile >= LAG) & (tile < LAG + theirs))
        def _():
            relay(tile - LAG)

    @pl.loop(n_tiles - LAG, theirs)
    def _(tile):
        relay(tile)

    @pl.loop(0, n_tiles)
    def _(tile):
        ref = y_ref.at[rows(partner, tile)]
        remote(ref, ref, csend.at[0], crecv.at[tile], to_core).wait_recv()
        give_core(tile).wait_send()

    @pl.loop(0, theirs)
    def _(tile):
        ref = y_ref.at[rows(corner, tile)]
        remote(ref, ref, rsend.at[0], rrecv.at[tile], to_core).wait_recv()
        pass_on(tile).wait_send()

    @pl.loop(0, mine)
    def _(tile):
        give_chip(tile).wait_send()

    for copy in sends:
        copy.wait_send()
    for copy in swaps:
        copy.wait()


def forward_all(x_rows, own, chip, twin, near_first, near_second, n_stage, n_both):
    n_rows, dim = x_rows.shape
    width = own[0].shape[1]
    n_own = max(OWN_TILES)
    n_tiles = n_own + n_both
    assert TILE * (sum(OWN_TILES) + 2 * n_both) == n_rows
    dma = pltpu.SemaphoreType.DMA
    flops = 4 * n_tiles * TILE * dim * width * n_stage
    return pl.pallas_call(
        functools.partial(forward_kernel, OWN_TILES[0], OWN_TILES[2], n_both),
        out_shape=(pltpu.VMEM((n_rows, dim), jnp.bfloat16), jax.ShapeDtypeStruct(near_first.shape, jnp.float32), jax.ShapeDtypeStruct(near_second.shape, jnp.float32)),
        in_specs=[pl.BlockSpec(memory_space=pl.ANY)] * 9,
        out_specs=(pl.BlockSpec(memory_space=pltpu.VMEM),) + (pl.BlockSpec(memory_space=pl.ANY),) * 2,
        scratch_shapes=[
            pltpu.VMEM((2, TILE, dim), jnp.bfloat16),
            pltpu.VMEM((PRE, TILE, dim), jnp.bfloat16),
            pltpu.VMEM((n_stage, dim, width), jnp.bfloat16),
            pltpu.VMEM((n_stage, width, dim), jnp.bfloat16),
            dma((2,)), dma((PRE,)), dma((6,)), dma((n_tiles,)), dma((n_own,)), dma((n_own,)),
            dma((n_tiles,)), dma((n_own,)), dma((n_own,)), dma((10,)), dma((4 * n_stage,)), dma((2,)), dma((2,)),
        ],
        compiler_params=pltpu.CompilerParams(collective_id=0, has_side_effects=True, vmem_limit_bytes=FORWARD_VMEM * 2 ** 20),
        cost_estimate=pl.CostEstimate(flops=flops, bytes_accessed=2 * n_rows * dim * 2, transcendentals=0),
        name='forward_all',
    )(x_rows, *own, *chip, *twin, near_first, near_second)


def adamw_rows(coef, rate, param, moment, second, grad_val):
    scaled = coef * grad_val
    mom_new = BETA_ONE * moment + (1.0 - BETA_ONE) * scaled
    sec_new = BETA_TWO * second + (1.0 - BETA_TWO) * scaled * scaled
    mom_hat = mom_new * (1.0 / (1.0 - BETA_ONE ** STEP_COUNT))
    sec_hat = sec_new * (1.0 / (1.0 - BETA_TWO ** STEP_COUNT))
    return param - rate * (mom_hat / (jnp.sqrt(sec_hat) + ADAM_EPS) + WEIGHT_DECAY * param), mom_new, sec_new


def update_kernel(n_ins, half_ref, rate_ref, clip_ref, *refs):
    outs = refs[n_ins:]
    if len(outs) == 8:
        step, steps = pl.program_id(0), pl.num_programs(0)

        def drain(idx):
            size = outs[6].shape[0] // FINAL_STEPS
            span = pl.ds(pl.multiple_of(idx * size, size), size)
            return pltpu.make_async_copy(refs[8].at[span], outs[6].at[span], outs[7].at[idx])

        drain(step).start()

    for side in (0, 1):
        param, moment, second, grad_val = (ref[...] for ref in refs[4 * side:4 * side + 4])
        news = adamw_rows(clip_ref[0:1, 0:1], rate_ref[0], param, moment, second, grad_val)
        for ref, new in zip(outs[3 * side:3 * side + 3], news):
            ref[...] = new
    if len(outs) == 8:
        @pl.when(step == steps - 1)
        def _():
            for idx in range(FINAL_STEPS):
                drain(idx).wait()


def half_update(half_idx, rate, clip, first, second, grads, made=(), rows=None):
    steps = FINAL_STEPS if made else UPDATE_STEPS
    full, out_specs, out_shape = [], [], []
    for arr, grad in zip((first[0], second[0]), grads):
        block = (grad.shape[0] // steps, grad.shape[1])
        picked = pl.BlockSpec(block, lambda step, half: (half[0] * steps + step, 0))
        full += [picked] * 3 + [pl.BlockSpec(block, lambda step, half: (step, 0))]
        out_specs += [picked] * 3
        out_shape += [jax.ShapeDtypeStruct(arr.shape, jnp.float32)] * 3
    in_specs = [pl.BlockSpec(memory_space=pltpu.SMEM), pl.BlockSpec(clip.shape, lambda step, half: (0, 0))] + full
    args = [half_idx, rate, clip, *first, grads[0], *second, grads[1]]
    aliases = {}
    if made:
        in_specs.append(pl.BlockSpec(memory_space=pl.ANY))
        args.append(pltpu.with_memory_space_constraint(rows, pltpu.VMEM))
        out_specs.append(pl.BlockSpec(memory_space=pl.ANY))
        out_shape.append(jax.ShapeDtypeStruct(rows.shape, rows.dtype))
        aliases = {len(args) + idx: idx for idx in range(6)}
        in_specs += [pl.BlockSpec(memory_space=pl.ANY)] * 6
        args += list(made)
    return pl.pallas_call(
        functools.partial(update_kernel, len(in_specs) - 2),
        out_shape=tuple(out_shape),
        grid_spec=pltpu.PrefetchScalarGridSpec(num_scalar_prefetch=1, grid=(steps,), in_specs=in_specs, out_specs=tuple(out_specs),
                                              scratch_shapes=[pltpu.SemaphoreType.DMA((FINAL_STEPS,))] if made else []),
        input_output_aliases=aliases,
        compiler_params=pltpu.CompilerParams(vmem_limit_bytes=(24 if made else 62) * 2 ** 20),
        cost_estimate=pl.CostEstimate(flops=30 * 2 ** 20, bytes_accessed=30 * 2 ** 20, transcendentals=0),
        name='far_update' if made else 'near_update',
    )(*args)


def backward_kernel(limit_ref, rate_ref, act_ref, dout_ref, w1_ref, w2_ref, m1_ref, m2_ref, v1_ref, v2_ref, acc1_ref, acc2_ref,
                    g1_out, g2_out, clip_ref, b1_out, b2_out, g1_ref, g2_ref, b1_ref, b2_ref,
                    actv, grad, w1v, w2v, hid, slope, dpre, sent, accv, inbox,
                    norms, lsem, hsem, gsem, bsem, asem, csend, crecv, rsend, rrecv, nsend, nrecv):
    stage = lax.axis_index('stage')
    rep = lax.axis_index('data')
    far = 1 - rep
    n_rows, dim = actv.shape
    width = w1v.shape[1]
    n_chunks = n_rows // ROWS
    last = 3
    half1 = dim // 2
    half2 = width // 2
    n_parts = inbox.shape[0]
    n_cols = width // PART

    def chunk(idx):
        return pl.ds(pl.multiple_of(idx * ROWS, ROWS), ROWS)

    def peer(**where):
        return dict(device_id=where, device_id_type=pl.DeviceIdType.MESH)

    loads = [pltpu.make_async_copy(w1_ref, slope.at[2 * dim:3 * dim, :], lsem.at[0]), pltpu.make_async_copy(act_ref, actv, lsem.at[1])]
    loads += [pltpu.make_async_copy(w2_ref.at[idx * dim:(idx + 1) * dim, :], slope.at[3 * dim:4 * dim, idx * dim:(idx + 1) * dim], lsem.at[2 + idx]) for idx in range(4)]
    for copy in loads:
        copy.start()
    top = pltpu.make_async_copy(dout_ref, grad, lsem.at[6])

    @pl.when(stage == last)
    def _():
        top.start()

    def load_acc(idx, side, step):
        slot = step % accv.shape[0]
        if idx < n_cols:
            src = acc1_ref.at[pl.ds(pl.multiple_of(side * half1, half1), half1), pl.ds(idx * PART, PART)]
        else:
            src = acc2_ref.at[pl.ds(pl.multiple_of(side * half2 + (idx - n_cols) * half1, half1), half1), :]
        return pltpu.make_async_copy(src, accv.at[slot], asem.at[slot])

    steps = [(idx, far) for idx in range(n_parts)] + [(idx, rep) for idx in range(n_parts)]
    ahead = accv.shape[0]
    for step in range(ahead):
        load_acc(*steps[step], step).start()

    barrier = pltpu.get_barrier_semaphore()
    place = rep * 4 + stage
    others = [(place + hop) % 8 for hop in range(1, 8)]
    for other in others:
        pl.semaphore_signal(barrier, inc=1, **peer(data=other // 4, stage=other % 4))
    pl.semaphore_wait(barrier, 7)

    def hop(idx):
        return pltpu.make_async_remote_copy(src_ref=sent.at[chunk(idx)], dst_ref=grad.at[chunk(idx)], send_sem=csend.at[idx], recv_sem=crecv.at[idx],
                                            **peer(stage=(stage + 3) % 4))

    def prepare(idx):
        act = actv[chunk(idx), :]
        for first in range(0, width, COLS):
            cols = slice(first, first + COLS)
            z = jnp.dot(act, w1v[:, cols], preferred_element_type=jnp.float32)
            sq = z * z
            th = jnp.tanh(z * (0.7978845608028654 + 0.035677408136300125 * sq))
            gate = 0.5 + 0.5 * th
            hid[chunk(idx), cols] = (z * gate).astype(jnp.bfloat16)
            slope[chunk(idx), cols] = gate + (0.5 * z) * (1.0 - th * th) * (0.7978845608028654 + 0.10703222440890037 * sq)

    def descend(idx):
        grad_rows = grad[chunk(idx), :]
        total = None
        for first in range(0, width, COLS):
            cols = slice(first, first + COLS)
            d_hid = lax.dot_general(grad_rows, w2v[cols, :], TRANS_DIMS, preferred_element_type=jnp.float32)
            d_pre = (slope[chunk(idx), cols] * d_hid).astype(jnp.bfloat16)
            dpre[chunk(idx), cols] = d_pre
            part = lax.dot_general(d_pre, w1v[:, cols], TRANS_DIMS, preferred_element_type=jnp.float32)
            total = part if first == 0 else total + part
        sent[chunk(idx), :] = (grad_rows.astype(jnp.float32) + total).astype(jnp.bfloat16)

    loads[0].wait()

    @pl.loop(0, dim // 64)
    def _(idx):
        span = pl.ds(pl.multiple_of(idx * 64, 64), 64)
        w1v[span, :] = slope[pl.ds(pl.multiple_of(2 * dim + idx * 64, 64), 64), :].astype(jnp.bfloat16)

    loads[1].wait()
    prepare(0)
    for copy in loads[2:]:
        copy.wait()

    @pl.loop(0, dim // 64)
    def _(idx):
        for group in range(4):
            span = pl.ds(pl.multiple_of(group * dim + idx * 64, 64), 64)
            w2v[span, :] = slope[pl.ds(pl.multiple_of(3 * dim + idx * 64, 64), 64), group * dim:(group + 1) * dim].astype(jnp.bfloat16)

    @pl.when(stage == last)
    def _():
        top.wait()

    @pl.loop(0, n_chunks)
    def _(idx):
        @pl.when(stage < last)
        def _():
            hop(idx).wait_recv()

        descend(idx)

        @pl.when(stage > 0)
        def _():
            hop(idx).start()

        @pl.when(idx + 1 < n_chunks)
        def _():
            prepare(idx + 1)

    near = []
    for idx, ref in enumerate((w1_ref, m1_ref, v1_ref)):
        near.append(pltpu.make_async_copy(ref.at[pl.ds(pl.multiple_of(rep * half1, half1), half1), :], slope.at[dim + idx * half1:dim + (idx + 1) * half1, :], hsem.at[len(near)]))
    for idx, ref in enumerate((w2_ref, m2_ref, v2_ref)):
        for group in range(4):
            near.append(pltpu.make_async_copy(ref.at[pl.ds(pl.multiple_of(rep * half2 + group * half1, half1), half1), :],
                                              slope.at[dim + (3 + idx) * half1:dim + (4 + idx) * half1, group * dim:(group + 1) * dim], hsem.at[len(near)]))
    for copy in near:
        copy.start()

    def weight_grad(idx, side):
        if idx < n_cols:
            left = actv[:, pl.ds(pl.multiple_of(side * half1, half1), half1)]
            right = dpre[:, idx * PART:(idx + 1) * PART]
        else:
            left = hid[:, pl.ds(pl.multiple_of(side * half2 + (idx - n_cols) * half1, half1), half1)]
            right = grad[...]
        return lax.dot_general(left, right, FIRST_DIMS, preferred_element_type=jnp.float32)

    def own_part(idx):
        if idx < n_cols:
            return g1_ref, (slice(None), slice(idx * PART, (idx + 1) * PART))
        return g2_ref, (slice((idx - n_cols) * half1, (idx - n_cols + 1) * half1), slice(None))

    def outbox(idx):
        return slope.at[pl.ds((idx // n_cols) * half1, half1), pl.ds((idx % n_cols) * PART, PART)]

    def post(idx):
        return pltpu.make_async_remote_copy(src_ref=outbox(idx), dst_ref=inbox.at[idx], send_sem=rsend.at[idx], recv_sem=rrecv.at[idx], **peer(data=far))

    for step, (idx, side) in enumerate(steps):
        load_acc(idx, side, step).wait()
        value = accv[step % ahead] + weight_grad(idx, side)
        if step < n_parts:
            outbox(idx)[...] = value
            post(idx).start()
        else:
            ref, where = own_part(idx)
            ref[where] = value
        if step + ahead < len(steps):
            load_acc(*steps[step + ahead], step + ahead).start()

    for copy in near:
        copy.wait()
    mom_fix, sec_fix = 1.0 / (1.0 - BETA_ONE ** STEP_COUNT), 1.0 / (1.0 - BETA_TWO ** STEP_COUNT)
    kept = (1.0 - WEIGHT_DECAY * rate_ref[0], BETA_ONE * mom_fix, BETA_TWO * sec_fix)

    @pl.loop(0, half1 // ADAM_ROWS)
    def _(idx):
        for which in range(6):
            span = pl.ds(pl.multiple_of(dim + which * half1 + idx * ADAM_ROWS, ADAM_ROWS), ADAM_ROWS)
            slope[span, :] = kept[which % 3] * slope[span, :]

    def new_weight(which, coef, slope_rows, cols, grad_val):
        base, mom, sec = (slope[pl.ds(pl.multiple_of(dim + (which + idx) * half1 + slope_rows, ADAM_ROWS), ADAM_ROWS), cols] for idx in range(3))
        scaled = coef * grad_val
        top = mom + ((1.0 - BETA_ONE) * mom_fix) * scaled
        low = jnp.sqrt(sec + ((1.0 - BETA_TWO) * sec_fix) * (scaled * scaled)) + ADAM_EPS
        return base - rate_ref[0] * (top / low)

    def put_grad(idx):
        if idx < n_cols:
            where = (slice(None), slice(idx * PART, (idx + 1) * PART))
            return pltpu.make_async_copy(g1_ref.at[where], g1_out.at[where], gsem.at[idx])
        where = slice((idx - n_cols) * half1, (idx - n_cols + 1) * half1)
        return pltpu.make_async_copy(g2_ref.at[where], g2_out.at[where], gsem.at[idx])

    squares = jnp.zeros((8, PART), jnp.float32)
    for idx in range(n_parts):
        post(idx).wait_recv()
        ref, where = own_part(idx)
        mean = 0.5 * (ref[where] + inbox[idx])
        ref[where] = mean
        put_grad(idx).start()
        squares = squares + jnp.sum((mean * mean).reshape(half1 // 8, 8, PART), axis=0)
    norms[place] = squares

    def tell(idx):
        return pltpu.make_async_remote_copy(src_ref=norms.at[place], dst_ref=norms.at[place], send_sem=nsend.at[idx], recv_sem=nrecv.at[place],
                                            **peer(data=others[idx] // 4, stage=others[idx] % 4))

    def hear(idx):
        ref = norms.at[others[idx]]
        return pltpu.make_async_remote_copy(src_ref=ref, dst_ref=ref, send_sem=nsend.at[idx], recv_sem=nrecv.at[others[idx]],
                                            **peer(data=others[idx] // 4, stage=others[idx] % 4))

    for idx in range(7):
        tell(idx).start()
    for idx in range(7):
        hear(idx).wait_recv()
    total = norms[0]
    for idx in range(1, 8):
        total = total + norms[idx]
    total = jnp.sum(jnp.sum(total, axis=0, keepdims=True), axis=1, keepdims=True)
    clip = jnp.minimum(1.0, limit_ref[0] / (jnp.sqrt(total) + NORM_EPS))
    clip_ref[...] = jnp.broadcast_to(clip, clip_ref.shape)
    puts = [pltpu.make_async_copy(b1_ref, b1_out, bsem.at[0]), pltpu.make_async_copy(b2_ref, b2_out, bsem.at[1])]

    @pl.loop(0, half1 // ADAM_ROWS)
    def _(idx):
        span = pl.ds(pl.multiple_of(idx * ADAM_ROWS, ADAM_ROWS), ADAM_ROWS)
        new_w = new_weight(0, clip_ref[0:1, 0:1], idx * ADAM_ROWS, slice(0, width), g1_ref[span, :])
        b1_ref[span, :] = (0.5 * new_w).astype(jnp.bfloat16)

    puts[0].start()

    @pl.loop(0, half1 // ADAM_ROWS)
    def _(idx):
        for group in range(4):
            span = pl.ds(pl.multiple_of(group * half1 + idx * ADAM_ROWS, ADAM_ROWS), ADAM_ROWS)
            new_w = new_weight(3, clip_ref[0:1, 0:1], idx * ADAM_ROWS, slice(group * dim, (group + 1) * dim), g2_ref[span, :])
            b2_ref[span, :] = new_w.astype(jnp.bfloat16)

    puts[1].start()
    for idx in range(n_parts):
        put_grad(idx).wait()
    for copy in puts:
        copy.wait()
    for idx in range(7):
        tell(idx).wait_send()
    for idx in range(n_parts):
        post(idx).wait_send()

    @pl.when(stage > 0)
    def _():
        @pl.loop(0, n_chunks)
        def _(idx):
            hop(idx).wait_send()


def backward_all(limit, rate, act, d_out, first, second, acc_first, acc_second):
    n_rows, dim = act.shape
    width = first[0].shape[1]
    half1 = dim // 2
    n_chunks = n_rows // ROWS
    n_parts = 2 * (width // PART)
    dma = pltpu.SemaphoreType.DMA
    bf16, f32 = jnp.bfloat16, jnp.float32
    vmem = pl.BlockSpec(memory_space=pltpu.VMEM)
    return pl.pallas_call(
        backward_kernel,
        out_shape=(jax.ShapeDtypeStruct((half1, width), f32), jax.ShapeDtypeStruct((width // 2, dim), f32), jax.ShapeDtypeStruct((8, 128), f32),
                   jax.ShapeDtypeStruct((half1, width), bf16), jax.ShapeDtypeStruct((width // 2, dim), bf16)),
        in_specs=[pl.BlockSpec(memory_space=pltpu.SMEM)] * 2 + [pl.BlockSpec(memory_space=pl.ANY)] * 10,
        out_specs=(pl.BlockSpec(memory_space=pl.ANY),) * 2 + (vmem,) + (pl.BlockSpec(memory_space=pl.ANY),) * 2,
        scratch_shapes=[
            pltpu.VMEM((half1, width), f32), pltpu.VMEM((width // 2, dim), f32), pltpu.VMEM((half1, width), bf16), pltpu.VMEM((width // 2, dim), bf16),
            pltpu.VMEM((n_rows, dim), bf16), pltpu.VMEM((n_rows, dim), bf16),
            pltpu.VMEM((dim, width), bf16), pltpu.VMEM((width, dim), bf16),
            pltpu.VMEM((n_rows, width), bf16), pltpu.VMEM((n_rows, width), f32), pltpu.VMEM((n_rows, width), bf16),
            pltpu.VMEM((n_rows, dim), bf16), pltpu.VMEM((4, half1, PART), f32), pltpu.VMEM((n_parts, half1, PART), f32), pltpu.VMEM((8, 8, PART), f32),
            dma((7,)), dma((15,)), dma((n_parts,)), dma((2,)), dma((4,)), dma((n_chunks,)), dma((n_chunks,)), dma((n_parts,)), dma((n_parts,)), dma((7,)), dma((8,)),
        ],
        compiler_params=pltpu.CompilerParams(collective_id=1, has_side_effects=True, vmem_limit_bytes=63 * 2 ** 20),
        cost_estimate=pl.CostEstimate(flops=10 * n_rows * dim * width, bytes_accessed=40 * 2 ** 20, transcendentals=0),
        name='backward_all',
    )(limit, rate, act, d_out, first[0], second[0], first[1], second[1], first[2], second[2], acc_first, acc_second)


def solution(mesh):
    n_stage = mesh.shape['stage']
    w_spec = P('stage', None, None)
    acc_spec = P('data', 'stage', None, None)
    row_spec = P(None, 'data', None)

    def stage_program(w_in, w_out, mom_in, mom_out, var_in, var_out, acc_in, acc_out, stage_acts, d_out, next_x, learn_rate, max_norm):
        rep_idx = lax.axis_index('data')
        first = (w_in[0], mom_in[0], var_in[0])
        second = (w_out[0], mom_out[0], var_out[0])
        near_first, near_second, clip, half_first, half_second = backward_all(
            max_norm, learn_rate, stage_acts[0], d_out, first, second, acc_in[0, 0], acc_out[0, 0])
        own = (half_first, half_second)
        chip = tuple(lax.ppermute(arr, 'stage', [(src, (src + 2) % 4) for src in range(4)]) for arr in own)
        twin = tuple(lax.ppermute(arr, 'data', [(0, 1), (1, 0)]) for arr in own)
        near = half_update(rep_idx.reshape(1), learn_rate, clip, first, second, (near_first, near_second))
        n_micro, n_rows, dim = next_x.shape
        rows, far_first, far_second = forward_all(next_x.reshape(n_micro * n_rows, dim), own, chip, twin, near_first, near_second, n_stage, SHARED)
        *news, next_y = half_update((1 - rep_idx).reshape(1), learn_rate, clip, first, second, (far_first, far_second), near, rows)
        return (news[0][None], news[3][None], news[1][None], news[4][None], news[2][None], news[5][None], next_y.reshape(next_x.shape))

    return jax.shard_map(stage_program, mesh=mesh, in_specs=(w_spec, w_spec, w_spec, w_spec, w_spec, w_spec, acc_spec, acc_spec, P('stage', 'data', None), P('data', None), row_spec, P(None), P(None)), out_specs=(w_spec, w_spec, w_spec, w_spec, w_spec, w_spec, row_spec), check_vma=False)
```
